128 devices in a mesh: seq: 32 (over z, x, core), group: 4 (over y).
Axes of the slice: x: 4, y: 4, z: 4, core: 2. Of those that a mesh axis runs over, the one named last changes fastest.
Arguments:
- new_queries: bfloat16 [32, 8, 8, 128], P('seq', 'group'), may hold values from -6 to 6
- stored_keys: bfloat16 [32, 8, 16384, 128], P(None, 'group', 'seq'), may hold values from -6 to 6
- stored_values: bfloat16 [32, 8, 16384, 128], P(None, 'group', 'seq'), may hold values from -6 to 6
- used_length: int32 [32], replicated, may hold values from 8192 to 16384
- out_weight: bfloat16 [8, 8, 128, 5120], P('group'), may hold values from -0.0625 to 0.0625
Outputs:
- token_out: bfloat16 [32, 5120], P('seq', 'group')
The draws below stay inside these ranges and needn't reach their ends.
All inputs are finite; a program needn't handle non-finite values.
Results may differ from the reference program's by a relative error of at most 0.0025.
Values may be sent and summed in bfloat16 or wider, within the bound.
A program may use at most 128 MiB of HBM per device.

```python
import jax
import jax.numpy as jnp
from jax import lax

BATCH = 32
LENGTH = 16384
KV_HEADS = 8
GROUP = 8
HEAD_SIZE = 128
D_MODEL = 5120


def plant(drawn, key, smallest, largest):
    place = [jax.random.randint(jax.random.fold_in(key, axis), (), 0, length) for axis, length in enumerate(drawn.shape)]
    longest = drawn.shape.index(max(drawn.shape))
    neighbour = place[:longest] + [(place[longest] + 1) % drawn.shape[longest]] + place[longest + 1:]
    return drawn.at[tuple(place)].set(smallest).at[tuple(neighbour)].set(largest)


def steps_of(rng, extent, shards, smallest, top_value):
    def one(axis_at, shards_of):
        draws = jax.random.uniform(jax.random.fold_in(jax.random.fold_in(rng, 6), axis_at), (shards_of,), jnp.float32, smallest / len(shards), top_value / len(shards))
        return jnp.repeat(jnp.exp(draws), extent[axis_at] // shards_of).reshape((-1,) + (1,) * (len(extent) - axis_at - 1))

    gain = one(*shards[0])
    for cut in shards[1:]:
        gain = gain * one(*cut)
    return gain


def scatter_about(own_key, shape, deviation, reach, split=(), kind=jnp.bfloat16):
    array = jax.random.normal(own_key, shape, jnp.float32) * deviation
    if len(split) > 0:
        array = steps_of(own_key, shape, split, -0.22, 0.18) * array
    return jnp.clip(array, min=-reach, max=reach).astype(kind)


def setup_inputs(seed: int = 0) -> dict:
    arg_keys = jax.random.split(jax.random.key(seed), 6)
    new_queries = scatter_about(arg_keys[0], (BATCH, KV_HEADS, GROUP, HEAD_SIZE), 1.0, 6.0, ((0, 32), (1, 4)))
    stored_keys = scatter_about(arg_keys[1], (BATCH, KV_HEADS, LENGTH, HEAD_SIZE), 1.0, 6.0, ((1, 4), (2, 32)))
    stored_values = scatter_about(arg_keys[2], (BATCH, KV_HEADS, LENGTH, HEAD_SIZE), 1.0, 6.0, ((1, 4), (2, 32)))
    used_length = plant(jax.random.randint(arg_keys[3], (BATCH,), LENGTH // 2, LENGTH + 1), jax.random.fold_in(arg_keys[3], 1), LENGTH // 2, LENGTH).astype(jnp.int32)
    out_weight = scatter_about(arg_keys[4], (KV_HEADS, GROUP, HEAD_SIZE, D_MODEL), (KV_HEADS * GROUP * HEAD_SIZE) ** -0.5, 0.0625, ((0, 4),))
    return {"new_queries": new_queries, "stored_keys": stored_keys, "stored_values": stored_values, "used_length": used_length, "out_weight": out_weight}


def reference(new_queries, stored_keys, stored_values, used_length, out_weight):
    def one_sequence(item):
        query_one, keys_one, values_one, length_one = item
        logit = jnp.einsum("kgd,ktd->kgt", query_one.astype(jnp.float32), keys_one.astype(jnp.float32)) * HEAD_SIZE ** -0.5
        logit = jnp.where(jnp.arange(LENGTH) < length_one, logit, -1e30)
        share = jax.nn.softmax(logit, axis=-1)
        return jnp.einsum("kgt,ktd->kgd", share, values_one.astype(jnp.float32), precision=lax.Precision.HIGHEST)
    read = lax.map(one_sequence, (new_queries, stored_keys, stored_values, used_length)).astype(jnp.bfloat16)
    read = lax.optimization_barrier(read)
    token_out = jnp.einsum("bkgd,kgdm->bm", read.astype(jnp.float32), out_weight.astype(jnp.float32)).astype(jnp.bfloat16)
    return token_out
```

```python
import functools

import jax
import jax.numpy as jnp
from jax import lax
from jax.experimental import pallas as pl
from jax.experimental.pallas import tpu as pltpu
from jax.sharding import PartitionSpec as P

MESH = pl.DeviceIdType.MESH
SEQ, GRP = 32, 4
HEADS, GROUP, HEAD = 2, 8, 128
ROWS = HEADS * GROUP
STRETCH = 512
COLS = 1280
UNIT = 4
STEPS = SEQ // UNIT
TO_EXP2 = HEAD ** (-0.5) * 1.4426950408889634


def near_first(i):
    return i + (i // 2) * (5 - 2 * i)


def offset_of(me, dz, dx, dc):
    z, x, c = me // 8, (me // 2) % 4, me % 2
    return ((z + dz) % 4) * 8 + ((x + dx) % 4) * 2 + (c + dc) % 2


def sequence_of(me, step, u):
    dz = near_first(step // 2)
    dx = near_first(2 * (step % 2) + u // 2)
    return offset_of(me, dz, dx, u % 2)


def kernel(
    q_hbm, k_hbm, v_hbm, len_hbm, w_hbm, out_ref,
    kbuf, vbuf, wbuf, qbuf, lens, logits, psend, ssend, parts, stats, rows, ysend, ybuf,
    local_sem, k_sem, v_sem, w_sem, q_send, q_recv, p_send, p_recv, s_send, s_recv, y_send, y_recv,
):
    me = lax.axis_index("seq")
    grp = lax.axis_index("group")

    barrier = pltpu.get_barrier_semaphore()
    for i in range(1, SEQ):
        pl.semaphore_signal(barrier, 1, device_id={"seq": (me + i) % SEQ}, device_id_type=MESH)
    for i in range(1, GRP):
        pl.semaphore_signal(barrier, 1, device_id={"group": (grp + i) % GRP}, device_id_type=MESH)

    q_copy = pltpu.make_async_copy(q_hbm.at[0], qbuf.at[me], local_sem.at[0])
    len_copy = pltpu.make_async_copy(len_hbm, lens, local_sem.at[1])
    q_copy.start()
    len_copy.start()

    def k_copy(step, u):
        j = step * UNIT + u
        return pltpu.make_async_copy(k_hbm.at[sequence_of(me, step, u)], kbuf.at[j], k_sem.at[j])

    def v_copy(step, u):
        j = step * UNIT + u
        return pltpu.make_async_copy(v_hbm.at[sequence_of(me, step, u)], vbuf.at[j], v_sem.at[j])

    @pl.loop(0, STEPS)
    def _(step):
        for u in range(UNIT):
            k_copy(step, u).start()
        for u in range(UNIT):
            v_copy(step, u).start()

    def owner_of(quarter):
        return (grp + (2, 1, 3, 0)[quarter]) % GRP

    def w_copy(quarter):
        first = pl.multiple_of(owner_of(quarter) * COLS, 128)
        return pltpu.make_async_copy(
            w_hbm.at[:, :, :, pl.ds(first, COLS)], wbuf.at[quarter], w_sem.at[quarter]
        )

    for quarter in range(GRP):
        w_copy(quarter).start()

    def q_remote(source, i, peer):
        return pltpu.make_async_remote_copy(
            src_ref=qbuf.at[source], dst_ref=qbuf.at[source],
            send_sem=q_send.at[i], recv_sem=q_recv.at[source],
            device_id={"seq": peer}, device_id_type=MESH,
        )

    def peer_at(i):
        return sequence_of(me, i // UNIT, i % UNIT)

    q_copy.wait()
    len_copy.wait()
    pl.semaphore_wait(barrier, SEQ - 1 + GRP - 1)
    for i in range(SEQ - 1, 0, -1):
        q_remote(me, i, peer_at(i)).start()

    def scores(step, slot):
        for u in range(UNIT):
            b = sequence_of(me, step, u)
            if u == 0:

                @pl.when(step > 0)
                def _():
                    q_remote(b, 0, b).wait_recv()
            else:
                q_remote(b, 0, b).wait_recv()
            k_copy(step, u).wait()
        lane = lax.broadcasted_iota(jnp.int32, (ROWS, STRETCH), 1) + me * STRETCH
        for u in range(UNIT):
            j = step * UNIT + u
            b = sequence_of(me, step, u)
            zero = jnp.zeros((GROUP, HEAD), jnp.float32)
            q0 = qbuf[b, 0].astype(jnp.float32)
            q1 = qbuf[b, 1].astype(jnp.float32)
            q = jnp.concatenate(
                [jnp.concatenate([q0, zero], axis=1), jnp.concatenate([zero, q1], axis=1)], axis=0
            ).astype(jnp.bfloat16)
            k = jnp.concatenate([kbuf[j, 0], kbuf[j, 1]], axis=1)
            logit = lax.dot_general(
                q, k, (((1,), (1,)), ((), ())), preferred_element_type=jnp.float32
            )
            logits[slot, u] = jnp.where(lane < lens[b], logit, -1e30)

    def reads(step, slot):
        row = lax.broadcasted_iota(jnp.int32, (ROWS, HEAD), 0)
        lane = lax.broadcasted_iota(jnp.int32, (ROWS, HEAD), 1)
        for u in range(UNIT):
            v_copy(step, u).wait()
        for u in range(UNIT):
            j = step * UNIT + u
            logit = logits[slot, u]
            top = jnp.max(logit, axis=1, keepdims=True)
            part = jnp.exp2((logit - top) * TO_EXP2)
            total = jnp.sum(part, axis=1, keepdims=True)
            high = part.astype(jnp.bfloat16)
            low = (part - high.astype(jnp.float32)).astype(jnp.bfloat16)
            v = jnp.concatenate([vbuf[j, 0], vbuf[j, 1]], axis=1)
            both = jnp.dot(
                jnp.concatenate([high, low], axis=0), v, preferred_element_type=jnp.float32
            )
            both = both[:ROWS] + both[ROWS:]
            psend[j] = jnp.concatenate([both[:GROUP, :HEAD], both[GROUP:, HEAD:]], axis=0)
            pair = jnp.where(lane == row, top, jnp.where(lane == row + ROWS, total, 0.0))
            ssend[j] = jnp.sum(pair, axis=0, keepdims=True)

    def p_remote(source, j, peer):
        return pltpu.make_async_remote_copy(
            src_ref=psend.at[j], dst_ref=parts.at[source],
            send_sem=p_send.at[j], recv_sem=p_recv.at[source],
            device_id={"seq": peer}, device_id_type=MESH,
        )

    def s_remote(source, j, peer):
        return pltpu.make_async_remote_copy(
            src_ref=ssend.at[j], dst_ref=stats.at[source],
            send_sem=s_send.at[j], recv_sem=s_recv.at[source],
            device_id={"seq": peer}, device_id_type=MESH,
        )

    def send(step):
        for u in range(UNIT):
            j = step * UNIT + u

            def go():
                s_remote(me, j, sequence_of(me, step, u)).start()
                p_remote(me, j, sequence_of(me, step, u)).start()

            if u == 0:
                pl.when(step > 0)(go)
            else:
                go()

    scores(0, 0)

    @pl.loop(0, STEPS - 1)
    def _(step):
        scores(step + 1, (step + 1) % 2)
        reads(step, step % 2)
        send(step)

    reads(STEPS - 1, (STEPS - 1) % 2)
    send(STEPS - 1)
    parts[me] = psend[0]
    stats[me] = ssend[0]

    for i in range(1, SEQ):
        s_remote(peer_at(i), 0, me).wait_recv()
    stat = stats[:, 0, :]
    best = jnp.max(stat, axis=0, keepdims=True)
    scale = jnp.exp2((stat - best) * TO_EXP2)
    sums = pltpu.roll(stat, HEAD - ROWS, axis=1)
    weight = scale / jnp.sum(sums * scale, axis=0, keepdims=True)
    weight = weight.T[:ROWS]

    for i in range(1, SEQ):
        p_remote(peer_at(i), 0, me).wait_recv()
    read = jnp.zeros((ROWS, HEAD), jnp.float32)
    for i in range(SEQ):
        read = read + parts[i] * weight[:, i : i + 1]
    rows[...] = read.astype(jnp.bfloat16).astype(jnp.float32)
    spread = jnp.concatenate(
        [jnp.broadcast_to(rows[r : r + 1, :], (GROUP, HEAD)) for r in range(ROWS)], axis=1
    ).astype(jnp.bfloat16)

    def y_remote(source, quarter, peer):
        return pltpu.make_async_remote_copy(
            src_ref=ysend.at[quarter], dst_ref=ybuf.at[source],
            send_sem=y_send.at[quarter], recv_sem=y_recv.at[source],
            device_id={"group": peer}, device_id_type=MESH,
        )

    for quarter in range(GRP):
        w_copy(quarter).wait()
        term = jnp.dot(
            spread,
            wbuf[quarter].reshape(ROWS * HEAD, COLS),
            preferred_element_type=jnp.float32,
        )
        for n in range(COLS // 128):
            ysend[quarter, n : n + 1, :] = term[0:1, n * 128 : (n + 1) * 128]
        if quarter < GRP - 1:
            y_remote(grp, quarter, owner_of(quarter)).start()

    for i in range(1, GRP):
        y_remote((grp + i) % GRP, 0, grp).wait_recv()
    token = ysend[GRP - 1]
    for i in range(1, GRP):
        token = token + ybuf[(grp + i) % GRP]
    for n in range(COLS // 128):
        out_ref[0:1, n * 128 : (n + 1) * 128] = token[n : n + 1, :].astype(out_ref.dtype)

    for i in range(1, SEQ):
        q_remote(me, i, peer_at(i)).wait_send()
        p_remote(me, i, peer_at(i)).wait_send()
        s_remote(me, i, peer_at(i)).wait_send()
    for quarter in range(GRP - 1):
        y_remote(grp, quarter, owner_of(quarter)).wait_send()


def per_device(new_queries, stored_keys, stored_values, used_length, out_weight):
    hbm = pl.BlockSpec(memory_space=pl.ANY)
    dma = pltpu.SemaphoreType.DMA
    return pl.pallas_call(
        kernel,
        out_shape=jax.ShapeDtypeStruct((1, COLS), jnp.bfloat16),
        in_specs=[hbm] * 5,
        out_specs=pl.BlockSpec(memory_space=pltpu.VMEM),
        scratch_shapes=[
            pltpu.VMEM((SEQ, HEADS, STRETCH, HEAD), jnp.bfloat16),
            pltpu.VMEM((SEQ, HEADS, STRETCH, HEAD), jnp.bfloat16),
            pltpu.VMEM((GRP, HEADS, GROUP, HEAD, COLS), jnp.bfloat16),
            pltpu.VMEM((SEQ, HEADS, GROUP, HEAD), jnp.bfloat16),
            pltpu.SMEM((SEQ,), jnp.int32),
            pltpu.VMEM((2, UNIT, ROWS, STRETCH), jnp.float32),
            pltpu.VMEM((SEQ, ROWS, HEAD), jnp.float32),
            pltpu.VMEM((SEQ, 1, 128), jnp.float32),
            pltpu.VMEM((SEQ, ROWS, HEAD), jnp.float32),
            pltpu.VMEM((SEQ, 1, 128), jnp.float32),
            pltpu.VMEM((ROWS, HEAD), jnp.float32),
            pltpu.VMEM((GRP, COLS // 128, 128), jnp.float32),
            pltpu.VMEM((GRP, COLS // 128, 128), jnp.float32),
            dma((2,)), dma((SEQ,)), dma((SEQ,)), dma((GRP,)),
            dma((SEQ,)), dma((SEQ,)), dma((SEQ,)), dma((SEQ,)), dma((SEQ,)), dma((SEQ,)),
            dma((GRP,)), dma((GRP,)),
        ],
        compiler_params=pltpu.CompilerParams(
            collective_id=0, has_side_effects=True, vmem_limit_bytes=60 * 1024 * 1024
        ),
        name="decode",
    )(new_queries, stored_keys, stored_values, used_length, out_weight)


def solution(mesh):
    in_specs = (
        P("seq", "group", None, None),
        P(None, "group", "seq", None),
        P(None, "group", "seq", None),
        P(),
        P("group", None, None, None),
    )
    return jax.shard_map(
        per_device, mesh=mesh, in_specs=in_specs, out_specs=P("seq", "group"), check_vma=False
    )
```

```python
import jax
import jax.numpy as jnp
from jax import lax
from jax.experimental import pallas as pl
from jax.experimental.pallas import tpu as pltpu
from jax.sharding import PartitionSpec as P

MESH = pl.DeviceIdType.MESH
SEQ, GRP = 32, 4
LAYERS, ROW = 4, 8
HEADS, GROUP, HEAD = 2, 8, 128
ROWS = HEADS * GROUP
STRETCH = 512
COLS = 1280
UNIT = 4
STEPS = SEQ // UNIT
TO_EXP2 = HEAD ** (-0.5) * 1.4426950408889634


def kernel(
    q_hbm, k_hbm, v_hbm, len_hbm, w_hbm, out_ref,
    kbuf, vbuf, wbuf, qbuf, lens, logits, psend, ssend, parts, stats, rows, ysend, ybuf,
    local_sem, k_sem, v_sem, w_sem, q_send, q_recv, p_send, p_recv, s_send, s_recv, y_send, y_recv,
):
    me = lax.axis_index("seq")
    grp = lax.axis_index("group")
    layer, place = lax.div(me, ROW), lax.rem(me, ROW)
    first = layer * ROW

    def mate(i):
        return first + lax.rem(place + i, ROW)

    def column(i):
        return lax.rem(layer + i, LAYERS) * ROW + place

    def across(i):
        return lax.rem(grp + i, GRP)

    barrier = pltpu.get_barrier_semaphore()
    for i in range(1, LAYERS):
        pl.semaphore_signal(barrier, 1, device_id={"seq": column(i)}, device_id_type=MESH)
    for i in range(1, ROW):
        pl.semaphore_signal(barrier, 1, device_id={"seq": mate(i)}, device_id_type=MESH)
    for i in range(1, GRP):
        pl.semaphore_signal(barrier, 1, device_id={"group": across(i)}, device_id_type=MESH)

    q_copy = pltpu.make_async_copy(q_hbm.at[0], qbuf.at[me], local_sem.at[0])
    len_copy = pltpu.make_async_copy(len_hbm, lens, local_sem.at[1])
    q_copy.start()
    len_copy.start()

    def k_copy(step):
        some = pl.ds(step * UNIT, UNIT)
        return pltpu.make_async_copy(k_hbm.at[some], kbuf.at[some], k_sem.at[step])

    def v_copy(step):
        some = pl.ds(step * UNIT, UNIT)
        return pltpu.make_async_copy(v_hbm.at[some], vbuf.at[some], v_sem.at[step])

    def owner_of(quarter):
        return across((2, 1, 3, 0)[quarter])

    def w_copy(quarter):
        start = pl.multiple_of(owner_of(quarter) * COLS, 128)
        return pltpu.make_async_copy(
            w_hbm.at[:, :, :, pl.ds(start, COLS)], wbuf.at[quarter], w_sem.at[quarter]
        )

    for step in range(STEPS):
        k_copy(step).start()
        v_copy(step).start()
    for quarter in range(GRP):
        w_copy(quarter).start()

    def q_remote(source, peer):
        return pltpu.make_async_remote_copy(
            src_ref=qbuf.at[source], dst_ref=qbuf.at[source],
            send_sem=q_send, recv_sem=q_recv.at[source],
            device_id={"seq": peer}, device_id_type=MESH,
        )

    q_copy.wait()
    len_copy.wait()
    pl.semaphore_wait(barrier, LAYERS - 1 + ROW - 1 + GRP - 1)
    for i in range(1, ROW):
        q_remote(me, mate(i)).start()
    for i in range(1, LAYERS):
        q_remote(me, column(i)).start()

    @pl.loop(0, ROW)
    def _(i):
        source = first + i

        @pl.when(i != place)
        def _():
            q_remote(source, me).wait_recv()
            for other in range(1, LAYERS):
                q_remote(source, column(other)).start()

    def scores(step, slot):
        @pl.when(lax.div(step, ROW // UNIT) != layer)
        def _():
            for u in range(UNIT):
                q_remote(step * UNIT + u, me).wait_recv()

        k_copy(step).wait()
        lane = lax.broadcasted_iota(jnp.int32, (ROWS, STRETCH), 1) + me * STRETCH
        for u in range(UNIT):
            b = step * UNIT + u
            zero = jnp.zeros((GROUP, HEAD), jnp.float32)
            q0 = qbuf[b, 0].astype(jnp.float32)
            q1 = qbuf[b, 1].astype(jnp.float32)
            q = jnp.concatenate(
                [jnp.concatenate([q0, zero], axis=1), jnp.concatenate([zero, q1], axis=1)], axis=0
            ).astype(jnp.bfloat16)
            k = jnp.concatenate([kbuf[b, 0], kbuf[b, 1]], axis=1)
            logit = lax.dot_general(
                q, k, (((1,), (1,)), ((), ())), preferred_element_type=jnp.float32
            )
            logits[slot, u] = jnp.where(lane < lens[b], logit, -1e30)

    def reads(step, slot):
        row = lax.broadcasted_iota(jnp.int32, (ROWS, HEAD), 0)
        lane = lax.broadcasted_iota(jnp.int32, (ROWS, HEAD), 1)
        v_copy(step).wait()
        for u in range(UNIT):
            b = step * UNIT + u
            logit = logits[slot, u]
            top = jnp.max(logit, axis=1, keepdims=True)
            part = jnp.exp2((logit - top) * TO_EXP2)
            total = jnp.sum(part, axis=1, keepdims=True)
            high = part.astype(jnp.bfloat16)
            low = (part - high.astype(jnp.float32)).astype(jnp.bfloat16)
            v = jnp.concatenate([vbuf[b, 0], vbuf[b, 1]], axis=1)
            both = jnp.dot(
                jnp.concatenate([high, low], axis=0), v, preferred_element_type=jnp.float32
            )
            both = both[:ROWS] + both[ROWS:]
            psend[b] = jnp.concatenate([both[:GROUP, :HEAD], both[GROUP:, HEAD:]], axis=0)
            pair = jnp.where(lane == row, top, jnp.where(lane == row + ROWS, total, 0.0))
            ssend[b] = jnp.sum(pair, axis=0, keepdims=True)

    def p_remote(b):
        return pltpu.make_async_remote_copy(
            src_ref=psend.at[b], dst_ref=parts.at[me], send_sem=p_send, recv_sem=p_recv,
            device_id={"seq": b}, device_id_type=MESH,
        )

    def s_remote(b):
        return pltpu.make_async_remote_copy(
            src_ref=ssend.at[b], dst_ref=stats.at[me], send_sem=s_send, recv_sem=s_recv,
            device_id={"seq": b}, device_id_type=MESH,
        )

    def send(step):
        for u in range(UNIT):
            b = step * UNIT + u

            @pl.when(b != me)
            def _():
                s_remote(b).start()
                p_remote(b).start()

    scores(0, 0)

    @pl.loop(0, STEPS - 1)
    def _(step):
        scores(step + 1, lax.rem(step + 1, 2))
        reads(step, lax.rem(step, 2))
        send(step)

    reads(STEPS - 1, (STEPS - 1) % 2)
    send(STEPS - 1)
    parts[me] = psend[me]
    stats[me] = ssend[me]
    for quarter in range(GRP):
        w_copy(quarter).wait()

    def all_but_one(ref, send_sem, recv_sem):
        most = ref.at[pl.ds(0, SEQ - 1)]
        return pltpu.make_async_remote_copy(
            src_ref=most, dst_ref=most, send_sem=send_sem, recv_sem=recv_sem,
            device_id={"seq": me}, device_id_type=MESH,
        )

    all_but_one(stats, s_send, s_recv).wait_recv()
    stat = stats[:, 0, :]
    best = jnp.max(stat, axis=0, keepdims=True)
    scale = jnp.exp2((stat - best) * TO_EXP2)
    sums = pltpu.roll(stat, HEAD - ROWS, axis=1)
    weight = scale / jnp.sum(sums * scale, axis=0, keepdims=True)
    weight = weight.T[:ROWS]

    all_but_one(parts, p_send, p_recv).wait_recv()
    read = jnp.zeros((ROWS, HEAD), jnp.float32)
    for i in range(SEQ):
        read = read + parts[i] * weight[:, i : i + 1]
    rows[...] = read.astype(jnp.bfloat16).astype(jnp.float32)
    spread = jnp.concatenate(
        [jnp.broadcast_to(rows[r : r + 1, :], (GROUP, HEAD)) for r in range(ROWS)], axis=1
    ).astype(jnp.bfloat16)

    def y_remote(source, quarter, peer):
        return pltpu.make_async_remote_copy(
            src_ref=ysend.at[quarter], dst_ref=ybuf.at[source],
            send_sem=y_send.at[quarter], recv_sem=y_recv.at[source],
            device_id={"group": peer}, device_id_type=MESH,
        )

    for quarter in range(GRP):
        term = jnp.dot(
            spread,
            wbuf[quarter].reshape(ROWS * HEAD, COLS),
            preferred_element_type=jnp.float32,
        )
        for n in range(COLS // 128):
            ysend[quarter, n : n + 1, :] = term[0:1, n * 128 : (n + 1) * 128]
        if quarter < GRP - 1:
            y_remote(grp, quarter, owner_of(quarter)).start()

    for i in range(1, GRP):
        y_remote(across(i), 0, grp).wait_recv()
    token = ysend[GRP - 1]
    for i in range(1, GRP):
        token = token + ybuf[across(i)]
    for n in range(COLS // 128):
        out_ref[0:1, n * 128 : (n + 1) * 128] = token[n : n + 1, :].astype(out_ref.dtype)

    all_but_one(qbuf, q_send, q_recv.at[0]).wait_send()
    all_but_one(parts, p_send, p_recv).wait_send()
    all_but_one(stats, s_send, s_recv).wait_send()
    for quarter in range(GRP - 1):
        y_remote(grp, quarter, owner_of(quarter)).wait_send()


def per_device(new_queries, stored_keys, stored_values, used_length, out_weight):
    hbm = pl.BlockSpec(memory_space=pl.ANY)
    dma = pltpu.SemaphoreType.DMA
    return pl.pallas_call(
        kernel,
        out_shape=pltpu.VMEM((1, COLS), jnp.bfloat16),
        in_specs=[hbm] * 5,
        out_specs=pl.BlockSpec(memory_space=pltpu.VMEM),
        scratch_shapes=[
            pltpu.VMEM((SEQ, HEADS, STRETCH, HEAD), jnp.bfloat16),
            pltpu.VMEM((SEQ, HEADS, STRETCH, HEAD), jnp.bfloat16),
            pltpu.VMEM((GRP, HEADS, GROUP, HEAD, COLS), jnp.bfloat16),
            pltpu.VMEM((SEQ, HEADS, GROUP, HEAD), jnp.bfloat16),
            pltpu.SMEM((SEQ,), jnp.int32),
            pltpu.VMEM((2, UNIT, ROWS, STRETCH), jnp.float32),
            pltpu.VMEM((SEQ, ROWS, HEAD), jnp.float32),
            pltpu.VMEM((SEQ, 1, 128), jnp.float32),
            pltpu.VMEM((SEQ, ROWS, HEAD), jnp.float32),
            pltpu.VMEM((SEQ, 1, 128), jnp.float32),
            pltpu.VMEM((ROWS, HEAD), jnp.float32),
            pltpu.VMEM((GRP, COLS // 128, 128), jnp.float32),
            pltpu.VMEM((GRP, COLS // 128, 128), jnp.float32),
            dma((2,)), dma((STEPS,)), dma((STEPS,)), dma((GRP,)),
            dma(()), dma((SEQ,)), dma(()), dma(()), dma(()), dma(()),
            dma((GRP,)), dma((GRP,)),
        ],
        compiler_params=pltpu.CompilerParams(
            collective_id=0, has_side_effects=True, vmem_limit_bytes=60 * 1024 * 1024
        ),
        name="decode",
    )(new_queries, stored_keys, stored_values, used_length, out_weight)


def solution(mesh):
    in_specs = (
        P("seq", "group", None, None),
        P(None, "group", "seq", None),
        P(None, "group", "seq", None),
        P(),
        P("group", None, None, None),
    )
    return jax.shard_map(
        per_device, mesh=mesh, in_specs=in_specs, out_specs=P("seq", "group"), check_vma=False
    )
```

```python
import jax
import jax.numpy as jnp
from jax import lax
from jax.experimental import pallas as pl
from jax.experimental.pallas import tpu as pltpu
from jax.sharding import PartitionSpec as P

MESH = pl.DeviceIdType.MESH
SEQ, GRP = 32, 4
LAYERS, ROW, PAIR = 4, 8, 2
HEADS, GROUP, HEAD = 2, 8, 128
ROWS = HEADS * GROUP
STRETCH = 512
COLS = 1280
UNIT = 4
STEPS = SEQ // UNIT
TO_EXP2 = HEAD ** (-0.5) * 1.4426950408889634


def kernel(
    q_hbm, k_hbm, v_hbm, len_hbm, w_hbm, out_ref,
    kbuf, vbuf, wbuf, qbuf, lens, logits, psend, ssend, parts, stats, rows, ysend, ybuf,
    local_sem, k_sem, v_sem, w_sem, q_send, q_recv, p_send, p_recv, s_send, s_recv, y_send, y_recv,
):
    me = lax.axis_index("seq")
    grp = lax.axis_index("group")
    layer, place = lax.div(me, ROW), lax.rem(me, ROW)
    first = layer * ROW

    def mate(i):
        return first + lax.rem(place + i, ROW)

    def column(i):
        return lax.rem(layer + i, LAYERS) * ROW + place

    def across(i):
        return lax.rem(grp + i, GRP)

    core = lax.rem(me, PAIR)
    chip = me - core

    barrier = pltpu.get_barrier_semaphore()
    for i in range(1, LAYERS):
        pl.semaphore_signal(barrier, 1, device_id={"seq": column(i)}, device_id_type=MESH)
    for i in range(1, ROW):
        pl.semaphore_signal(barrier, 1, device_id={"seq": mate(i)}, device_id_type=MESH)
    for i in range(1, GRP):
        for other in range(PAIR):
            there = {"seq": chip + other, "group": across(i)}
            pl.semaphore_signal(barrier, 1, device_id=there, device_id_type=MESH)

    q_copy = pltpu.make_async_copy(q_hbm.at[0], qbuf.at[me], local_sem.at[0])
    len_copy = pltpu.make_async_copy(len_hbm, lens, local_sem.at[1])
    q_copy.start()
    len_copy.start()

    def k_copy(step):
        some = pl.ds(step * UNIT, UNIT)
        return pltpu.make_async_copy(k_hbm.at[some], kbuf.at[some], k_sem.at[step])

    def v_copy(step):
        some = pl.ds(step * UNIT, UNIT)
        return pltpu.make_async_copy(v_hbm.at[some], vbuf.at[some], v_sem.at[step])

    def owner_of(quarter):
        return across((2, 1, 3, 0)[quarter])

    def w_copy(quarter):
        start = pl.multiple_of(owner_of(quarter) * COLS, 128)
        return pltpu.make_async_copy(
            w_hbm.at[core, :, :, pl.ds(start, COLS)], wbuf.at[quarter], w_sem.at[quarter]
        )

    for step in range(STEPS):
        k_copy(step).start(priority=1)
        v_copy(step).start(priority=1)
    for quarter in range(GRP):
        w_copy(quarter).start(priority=1)

    def q_remote(source, peer):
        return pltpu.make_async_remote_copy(
            src_ref=qbuf.at[source], dst_ref=qbuf.at[source],
            send_sem=q_send, recv_sem=q_recv.at[source],
            device_id={"seq": peer}, device_id_type=MESH,
        )

    q_copy.wait()
    len_copy.wait()
    pl.semaphore_wait(barrier, LAYERS - 1 + ROW - 1 + PAIR * (GRP - 1))
    for i in range(1, LAYERS):
        q_remote(me, column(i)).start()
    for i in range(1, ROW):
        q_remote(me, mate(i)).start()

    @pl.loop(0, LAYERS)
    def _(i):
        source = i * ROW + place

        @pl.when(i != layer)
        def _():
            q_remote(source, me).wait_recv()
            for other in range(1, ROW):
                q_remote(source, mate(other)).start()

    def scores(step, slot):
        for u in range(UNIT):

            @pl.when(lax.rem(step * UNIT + u, ROW) != place)
            def _():
                q_remote(step * UNIT + u, me).wait_recv()

        k_copy(step).wait()
        lane = lax.broadcasted_iota(jnp.int32, (ROWS, STRETCH), 1) + me * STRETCH
        for u in range(UNIT):
            b = step * UNIT + u
            zero = jnp.zeros((GROUP, HEAD), jnp.float32)
            q0 = qbuf[b, 0].astype(jnp.float32)
            q1 = qbuf[b, 1].astype(jnp.float32)
            q = jnp.concatenate(
                [jnp.concatenate([q0, zero], axis=1), jnp.concatenate([zero, q1], axis=1)], axis=0
            ).astype(jnp.bfloat16)
            k = jnp.concatenate([kbuf[b, 0], kbuf[b, 1]], axis=1)
            logit = lax.dot_general(
                q, k, (((1,), (1,)), ((), ())), preferred_element_type=jnp.float32
            )
            logits[slot, u] = jnp.where(lane < lens[b], logit, -1e30)

    def reads(step, slot):
        row = lax.broadcasted_iota(jnp.int32, (ROWS, HEAD), 0)
        lane = lax.broadcasted_iota(jnp.int32, (ROWS, HEAD), 1)
        v_copy(step).wait()
        results = []
        for u in range(UNIT):
            b = step * UNIT + u
            logit = logits[slot, u]
            top = jnp.max(logit, axis=1, keepdims=True)
            part = jnp.exp2((logit - top) * TO_EXP2)
            total = jnp.sum(part, axis=1, keepdims=True)
            high = part.astype(jnp.bfloat16)
            low = (part - high.astype(jnp.float32)).astype(jnp.bfloat16)
            v = jnp.concatenate([vbuf[b, 0], vbuf[b, 1]], axis=1)
            both = jnp.dot(
                jnp.concatenate([high, low], axis=0), v, preferred_element_type=jnp.float32
            )
            results.append((both[:ROWS] + both[ROWS:], top, total))
        for u in range(0, UNIT, PAIR):
            for head in range(HEADS):
                own = slice(head * GROUP, (head + 1) * GROUP)
                here = slice(head * HEAD, (head + 1) * HEAD)
                two = results[u : u + PAIR]
                top = jnp.concatenate([r[1][own] for r in two], axis=0)
                total = jnp.concatenate([r[2][own] for r in two], axis=0)
                psend[step * UNIT + u + head] = jnp.concatenate([r[0][own, here] for r in two], axis=0)
                pair = jnp.where(lane == row, top, jnp.where(lane == row + ROWS, total, 0.0))
                ssend[step * UNIT + u + head] = jnp.sum(pair, axis=0, keepdims=True)

    def p_remote(b):
        return pltpu.make_async_remote_copy(
            src_ref=psend.at[b], dst_ref=parts.at[me], send_sem=p_send, recv_sem=p_recv,
            device_id={"seq": b}, device_id_type=MESH,
        )

    def s_remote(b):
        return pltpu.make_async_remote_copy(
            src_ref=ssend.at[b], dst_ref=stats.at[me], send_sem=s_send, recv_sem=s_recv,
            device_id={"seq": b}, device_id_type=MESH,
        )

    def send(step):
        for u in range(UNIT):
            b = step * UNIT + u

            @pl.when(b != me)
            def _():
                s_remote(b).start()
                p_remote(b).start()

    scores(0, 0)

    @pl.loop(0, STEPS - 1)
    def _(step):
        scores(step + 1, lax.rem(step + 1, 2))
        reads(step, lax.rem(step, 2))
        send(step)

    reads(STEPS - 1, (STEPS - 1) % 2)
    send(STEPS - 1)
    parts[me] = psend[me]
    stats[me] = ssend[me]
    for quarter in range(GRP):
        w_copy(quarter).wait()

    def all_but_one(ref, send_sem, recv_sem):
        most = ref.at[pl.ds(0, SEQ - 1)]
        return pltpu.make_async_remote_copy(
            src_ref=most, dst_ref=most, send_sem=send_sem, recv_sem=recv_sem,
            device_id={"seq": me}, device_id_type=MESH,
        )

    all_but_one(stats, s_send, s_recv).wait_recv()
    stat = stats[:, 0, :]
    best = jnp.max(stat, axis=0, keepdims=True)
    scale = jnp.exp2((stat - best) * TO_EXP2)
    sums = pltpu.roll(stat, HEAD - ROWS, axis=1)
    weight = scale / jnp.sum(sums * scale, axis=0, keepdims=True)
    weight = weight.T[:ROWS]

    all_but_one(parts, p_send, p_recv).wait_recv()
    read = jnp.zeros((ROWS, HEAD), jnp.float32)
    for i in range(SEQ):
        read = read + parts[i] * weight[:, i : i + 1]
    rows[...] = read.astype(jnp.bfloat16).astype(jnp.float32)
    even = lax.broadcasted_iota(jnp.int32, (GROUP, HEAD), 0) == 0
    spread = jnp.concatenate(
        [jnp.where(even, rows[r : r + 1, :], rows[GROUP + r : GROUP + r + 1, :]) for r in range(GROUP)],
        axis=1,
    ).astype(jnp.bfloat16)

    mine = grp * PAIR + core

    def y_remote(quarter, token, peer):
        return pltpu.make_async_remote_copy(
            src_ref=ysend.at[quarter, token], dst_ref=ybuf.at[mine], send_sem=y_send, recv_sem=y_recv,
            device_id={"seq": chip + token, "group": peer}, device_id_type=MESH,
        )

    for quarter in range(GRP):
        term = jnp.dot(
            spread, wbuf[quarter].reshape(GROUP * HEAD, COLS), preferred_element_type=jnp.float32
        )
        for token in range(PAIR):
            for n in range(COLS // 128):
                ysend[quarter, token, n : n + 1, :] = term[token : token + 1, n * 128 : (n + 1) * 128]
        if quarter < GRP - 1:
            for token in range(PAIR):
                y_remote(quarter, token, owner_of(quarter)).start()
    y_remote(GRP - 1, 1 - core, grp).start()
    ybuf[mine] = ysend[GRP - 1, core]

    def others(ref):
        most = ref.at[pl.ds(0, GRP * PAIR - 1)]
        return pltpu.make_async_remote_copy(
            src_ref=most, dst_ref=most, send_sem=y_send, recv_sem=y_recv,
            device_id={"seq": me}, device_id_type=MESH,
        )

    others(ybuf).wait_recv()
    token = ybuf[0]
    for i in range(1, GRP * PAIR):
        token = token + ybuf[i]
    for n in range(COLS // 128):
        out_ref[0:1, n * 128 : (n + 1) * 128] = token[n : n + 1, :].astype(out_ref.dtype)

    others(ybuf).wait_send()
    all_but_one(qbuf, q_send, q_recv.at[0]).wait_send()
    all_but_one(parts, p_send, p_recv).wait_send()
    all_but_one(stats, s_send, s_recv).wait_send()


def per_device(new_queries, stored_keys, stored_values, used_length, out_weight):
    hbm = pl.BlockSpec(memory_space=pl.ANY)
    dma = pltpu.SemaphoreType.DMA
    return pl.pallas_call(
        kernel,
        out_shape=pltpu.VMEM((1, COLS), jnp.bfloat16),
        in_specs=[hbm] * 5,
        out_specs=pl.BlockSpec(memory_space=pltpu.VMEM),
        scratch_shapes=[
            pltpu.VMEM((SEQ, HEADS, STRETCH, HEAD), jnp.bfloat16),
            pltpu.VMEM((SEQ, HEADS, STRETCH, HEAD), jnp.bfloat16),
            pltpu.VMEM((GRP, GROUP, HEAD, COLS), jnp.bfloat16),
            pltpu.VMEM((SEQ, HEADS, GROUP, HEAD), jnp.bfloat16),
            pltpu.SMEM((SEQ,), jnp.int32),
            pltpu.VMEM((2, UNIT, ROWS, STRETCH), jnp.float32),
            pltpu.VMEM((SEQ, ROWS, HEAD), jnp.float32),
            pltpu.VMEM((SEQ, 1, 128), jnp.float32),
            pltpu.VMEM((SEQ, ROWS, HEAD), jnp.float32),
            pltpu.VMEM((SEQ, 1, 128), jnp.float32),
            pltpu.VMEM((ROWS, HEAD), jnp.float32),
            pltpu.VMEM((GRP, PAIR, COLS // 128, 128), jnp.float32),
            pltpu.VMEM((GRP * PAIR, COLS // 128, 128), jnp.float32),
            dma((2,)), dma((STEPS,)), dma((STEPS,)), dma((GRP,)),
            dma(()), dma((SEQ,)), dma(()), dma(()), dma(()), dma(()),
            dma(()), dma(()),
        ],
        compiler_params=pltpu.CompilerParams(
            collective_id=0, has_side_effects=True, vmem_limit_bytes=60 * 1024 * 1024
        ),
        name="decode",
    )(new_queries, stored_keys, stored_values, used_length, out_weight)


def solution(mesh):
    in_specs = (
        P("seq", "group", None, None),
        P(None, "group", "seq", None),
        P(None, "group", "seq", None),
        P(),
        P("group", None, None, None),
    )
    return jax.shard_map(
        per_device, mesh=mesh, in_specs=in_specs, out_specs=P("seq", "group"), check_vma=False
    )
```

```python
import jax
import jax.numpy as jnp
from jax import lax
from jax.experimental import pallas as pl
from jax.experimental.pallas import tpu as pltpu
from jax.sharding import PartitionSpec as P

MESH = pl.DeviceIdType.MESH
SEQ, GRP = 32, 4
LAYERS, ROW, PAIR = 4, 8, 2
HEADS, GROUP, HEAD = 2, 8, 128
ROWS = HEADS * GROUP
STRETCH = 512
COLS = 1280
UNIT = 4
STEPS = SEQ // UNIT
TO_EXP2 = HEAD ** (-0.5) * 1.4426950408889634


def kernel(
    q_hbm, k_hbm, v_hbm, len_hbm, w_hbm, out_ref,
    kbuf, vbuf, wbuf, qbuf, lens, logits, psend, ssend, parts, stats, rows, ysend, ybuf,
    local_sem, k_sem, v_sem, w_sem, q_send, q_recv, p_send, p_recv, s_send, s_recv, y_send, y_recv,
):
    me = lax.axis_index("seq")
    grp = lax.axis_index("group")
    layer, place = lax.div(me, ROW), lax.rem(me, ROW)
    lane_x, core = lax.div(place, PAIR), lax.rem(place, PAIR)
    chip = me - core
    far_first = (2, 3, 1, 0)
    layers = {i: lax.rem(layer + i, LAYERS) * ROW for i in far_first}
    places = {i: lax.rem(lane_x + i, ROW // PAIR) * PAIR for i in far_first}
    peers = [layers[z] + places[x] + c for z in far_first for x in far_first if z or x for c in range(PAIR)]
    peers.append(chip + 1 - core)

    def across(i):
        return lax.rem(grp + i, GRP)

    barrier = pltpu.get_barrier_semaphore()
    for peer in peers:
        pl.semaphore_signal(barrier, 1, device_id={"seq": peer}, device_id_type=MESH)
    for i in range(1, GRP):
        for other in range(PAIR):
            there = {"seq": chip + other, "group": across(i)}
            pl.semaphore_signal(barrier, 1, device_id=there, device_id_type=MESH)

    q_copy = pltpu.make_async_copy(q_hbm.at[0], qbuf.at[me], local_sem.at[0])
    len_copy = pltpu.make_async_copy(len_hbm, lens, local_sem.at[1])
    q_copy.start()
    len_copy.start()

    def k_copy(step):
        some = pl.ds(step * UNIT, UNIT)
        return pltpu.make_async_copy(k_hbm.at[some], kbuf.at[some], k_sem.at[step])

    def v_copy(step):
        some = pl.ds(step * UNIT, UNIT)
        return pltpu.make_async_copy(v_hbm.at[some], vbuf.at[some], v_sem.at[step])

    def owner_of(quarter):
        return across((1, 2, 3, 0)[quarter])

    def w_copy(quarter):
        start = pl.multiple_of(owner_of(quarter) * COLS, 128)
        return pltpu.make_async_copy(
            w_hbm.at[core, :, :, pl.ds(start, COLS)], wbuf.at[quarter], w_sem.at[quarter]
        )

    for step in range(STEPS):
        k_copy(step).start(priority=1)
        v_copy(step).start(priority=1)
    for quarter in range(GRP):
        w_copy(quarter).start(priority=1)

    def q_remote(peer):
        return pltpu.make_async_remote_copy(
            src_ref=qbuf.at[me], dst_ref=qbuf.at[me],
            send_sem=q_send, recv_sem=q_recv.at[lax.div(me, UNIT)],
            device_id={"seq": peer}, device_id_type=MESH,
        )

    def q_wait(step, count):
        some = qbuf.at[pl.ds(step * UNIT, count)]
        return pltpu.make_async_remote_copy(
            src_ref=some, dst_ref=some, send_sem=q_send, recv_sem=q_recv.at[step],
            device_id={"seq": me}, device_id_type=MESH,
        )

    q_copy.wait()
    len_copy.wait()
    pl.semaphore_wait(barrier, SEQ - 1 + PAIR * (GRP - 1))
    for peer in peers:
        q_remote(peer).start()

    def arrived(step):
        own = lax.div(me, UNIT) == step

        @pl.when(own)
        def _():
            q_wait(step, UNIT - 1).wait_recv()

        @pl.when(jnp.logical_not(own))
        def _():
            q_wait(step, UNIT).wait_recv()

        k_copy(step).wait()

    def scores(step, slot):
        lane = lax.broadcasted_iota(jnp.int32, (ROWS, STRETCH), 1) + me * STRETCH
        for u in range(UNIT):
            b = step * UNIT + u
            zero = jnp.zeros((GROUP, HEAD), jnp.float32)
            q0 = qbuf[b, 0].astype(jnp.float32)
            q1 = qbuf[b, 1].astype(jnp.float32)
            q = jnp.concatenate(
                [jnp.concatenate([q0, zero], axis=1), jnp.concatenate([zero, q1], axis=1)], axis=0
            ).astype(jnp.bfloat16)
            k = jnp.concatenate([kbuf[b, 0], kbuf[b, 1]], axis=1)
            logit = lax.dot_general(
                q, k, (((1,), (1,)), ((), ())), preferred_element_type=jnp.float32
            )
            logits[slot, u] = jnp.where(lane < lens[b], logit, -1e30)

    def reads(step, slot):
        row = lax.broadcasted_iota(jnp.int32, (ROWS, HEAD), 0)
        lane = lax.broadcasted_iota(jnp.int32, (ROWS, HEAD), 1)
        results = []
        for u in range(UNIT):
            b = step * UNIT + u
            logit = logits[slot, u]
            top = jnp.max(logit, axis=1, keepdims=True)
            part = jnp.exp2((logit - top) * TO_EXP2)
            total = jnp.sum(part, axis=1, keepdims=True)
            high = part.astype(jnp.bfloat16)
            low = (part - high.astype(jnp.float32)).astype(jnp.bfloat16)
            v = jnp.concatenate([vbuf[b, 0], vbuf[b, 1]], axis=1)
            both = jnp.dot(
                jnp.concatenate([high, low], axis=0), v, preferred_element_type=jnp.float32
            )
            results.append((both[:ROWS] + both[ROWS:], top, total))
        for u in range(0, UNIT, PAIR):
            for head in range(HEADS):
                own = slice(head * GROUP, (head + 1) * GROUP)
                here = slice(head * HEAD, (head + 1) * HEAD)
                two = results[u : u + PAIR]
                top = jnp.concatenate([r[1][own] for r in two], axis=0)
                total = jnp.concatenate([r[2][own] for r in two], axis=0)
                psend[step * UNIT + u + head] = jnp.concatenate([r[0][own, here] for r in two], axis=0)
                pair = jnp.where(lane == row, top, jnp.where(lane == row + ROWS, total, 0.0))
                ssend[step * UNIT + u + head] = jnp.sum(pair, axis=0, keepdims=True)

    def p_remote(b):
        return pltpu.make_async_remote_copy(
            src_ref=psend.at[b], dst_ref=parts.at[me], send_sem=p_send, recv_sem=p_recv,
            device_id={"seq": b}, device_id_type=MESH,
        )

    def s_remote(b):
        return pltpu.make_async_remote_copy(
            src_ref=ssend.at[b], dst_ref=stats.at[me], send_sem=s_send, recv_sem=s_recv,
            device_id={"seq": b}, device_id_type=MESH,
        )

    def send(step):
        for u in range(UNIT):
            b = step * UNIT + u

            @pl.when(b != me)
            def _():
                s_remote(b).start()
                p_remote(b).start()

    def both(step, slot):
        arrived(step + 1)
        v_copy(step).wait()
        reads(step, slot)
        scores(step + 1, 1 - slot)
        send(step)

    arrived(0)
    scores(0, 0)

    @pl.loop(0, STEPS // 2 - 1)
    def _(i):
        both(2 * i, 0)
        both(2 * i + 1, 1)

    both(STEPS - 2, 0)
    v_copy(STEPS - 1).wait()
    reads(STEPS - 1, 1)
    send(STEPS - 1)
    parts[me] = psend[me]
    stats[me] = ssend[me]
    for quarter in range(GRP):
        w_copy(quarter).wait()

    def all_but_one(ref, send_sem, recv_sem):
        most = ref.at[pl.ds(0, SEQ - 1)]
        return pltpu.make_async_remote_copy(
            src_ref=most, dst_ref=most, send_sem=send_sem, recv_sem=recv_sem,
            device_id={"seq": me}, device_id_type=MESH,
        )

    all_but_one(stats, s_send, s_recv).wait_recv()
    stat = stats[:, 0, :]
    best = jnp.max(stat, axis=0, keepdims=True)
    scale = jnp.exp2((stat - best) * TO_EXP2)
    sums = pltpu.roll(stat, HEAD - ROWS, axis=1)
    weight = scale / jnp.sum(sums * scale, axis=0, keepdims=True)
    weight = weight.T[:ROWS]

    all_but_one(parts, p_send, p_recv).wait_recv()
    read = jnp.zeros((ROWS, HEAD), jnp.float32)
    for i in range(SEQ):
        read = read + parts[i] * weight[:, i : i + 1]
    rows[...] = read.astype(jnp.bfloat16).astype(jnp.float32)
    even = lax.broadcasted_iota(jnp.int32, (GROUP, HEAD), 0) == 0
    spread = jnp.concatenate(
        [jnp.where(even, rows[r : r + 1, :], rows[GROUP + r : GROUP + r + 1, :]) for r in range(GROUP)],
        axis=1,
    ).astype(jnp.bfloat16)

    mine = grp * PAIR + core

    def y_remote(quarter, token, peer):
        return pltpu.make_async_remote_copy(
            src_ref=ysend.at[quarter, token], dst_ref=ybuf.at[mine], send_sem=y_send, recv_sem=y_recv,
            device_id={"seq": chip + token, "group": peer}, device_id_type=MESH,
        )

    for quarter in range(GRP):
        term = jnp.dot(
            spread, wbuf[quarter].reshape(GROUP * HEAD, COLS), preferred_element_type=jnp.float32
        )
        for token in range(PAIR):
            for n in range(COLS // 128):
                ysend[quarter, token, n : n + 1, :] = term[token : token + 1, n * 128 : (n + 1) * 128]
        if quarter < GRP - 1:
            for token in range(PAIR):
                y_remote(quarter, token, owner_of(quarter)).start()
    y_remote(GRP - 1, 1 - core, grp).start()
    ybuf[mine] = ysend[GRP - 1, core]

    def others(ref):
        most = ref.at[pl.ds(0, GRP * PAIR - 1)]
        return pltpu.make_async_remote_copy(
            src_ref=most, dst_ref=most, send_sem=y_send, recv_sem=y_recv,
            device_id={"seq": me}, device_id_type=MESH,
        )

    others(ybuf).wait_recv()
    token = ybuf[0]
    for i in range(1, GRP * PAIR):
        token = token + ybuf[i]
    for n in range(COLS // 128):
        out_ref[0:1, n * 128 : (n + 1) * 128] = token[n : n + 1, :].astype(out_ref.dtype)

    others(ybuf).wait_send()
    all_but_one(qbuf, q_send, q_recv.at[0]).wait_send()
    all_but_one(parts, p_send, p_recv).wait_send()
    all_but_one(stats, s_send, s_recv).wait_send()


def per_device(new_queries, stored_keys, stored_values, used_length, out_weight):
    hbm = pl.BlockSpec(memory_space=pl.ANY)
    dma = pltpu.SemaphoreType.DMA
    return pl.pallas_call(
        kernel,
        out_shape=pltpu.VMEM((1, COLS), jnp.bfloat16),
        in_specs=[hbm] * 5,
        out_specs=pl.BlockSpec(memory_space=pltpu.VMEM),
        scratch_shapes=[
            pltpu.VMEM((SEQ, HEADS, STRETCH, HEAD), jnp.bfloat16),
            pltpu.VMEM((SEQ, HEADS, STRETCH, HEAD), jnp.bfloat16),
            pltpu.VMEM((GRP, GROUP, HEAD, COLS), jnp.bfloat16),
            pltpu.VMEM((SEQ, HEADS, GROUP, HEAD), jnp.bfloat16),
            pltpu.SMEM((SEQ,), jnp.int32),
            pltpu.VMEM((2, UNIT, ROWS, STRETCH), jnp.float32),
            pltpu.VMEM((SEQ, ROWS, HEAD), jnp.float32),
            pltpu.VMEM((SEQ, 1, 128), jnp.float32),
            pltpu.VMEM((SEQ, ROWS, HEAD), jnp.float32),
            pltpu.VMEM((SEQ, 1, 128), jnp.float32),
            pltpu.VMEM((ROWS, HEAD), jnp.float32),
            pltpu.VMEM((GRP, PAIR, COLS // 128, 128), jnp.float32),
            pltpu.VMEM((GRP * PAIR, COLS // 128, 128), jnp.float32),
            dma((2,)), dma((STEPS,)), dma((STEPS,)), dma((GRP,)),
            dma(()), dma((STEPS,)), dma(()), dma(()), dma(()), dma(()),
            dma(()), dma(()),
        ],
        compiler_params=pltpu.CompilerParams(
            collective_id=0, has_side_effects=True, vmem_limit_bytes=60 * 1024 * 1024
        ),
        name="decode",
    )(new_queries, stored_keys, stored_values, used_length, out_weight)


def solution(mesh):
    in_specs = (
        P("seq", "group", None, None),
        P(None, "group", "seq", None),
        P(None, "group", "seq", None),
        P(),
        P("group", None, None, None),
    )
    return jax.shard_map(
        per_device, mesh=mesh, in_specs=in_specs, out_specs=P("seq", "group"), check_vma=False
    )
```

```python
import jax
import jax.numpy as jnp
from jax import lax
from jax.experimental import pallas as pl
from jax.experimental.pallas import tpu as pltpu
from jax.sharding import PartitionSpec as P

MESH = pl.DeviceIdType.MESH
SEQ, GRP = 32, 4
ROW, PAIR = 8, 2
HEADS, GROUP, HEAD = 2, 8, 128
ROWS = HEADS * GROUP
STRETCH = 512
COLS = 1280
UNIT = 4
STEPS = SEQ // UNIT
TO_EXP2 = HEAD ** (-0.5) * 1.4426950408889634


def kernel(
    q_hbm, k_hbm, v_hbm, len_hbm, w_hbm, out_ref,
    kbuf, vbuf, wbuf, qbuf, lens, logits, psend, ssend, parts, stats, rows, ysend, ybuf,
    local_sem, k_sem, v_sem, w_sem, q_send, q_recv, p_send, p_recv, s_send, s_recv, y_send, y_recv,
):
    me = lax.axis_index("seq")
    grp = lax.axis_index("group")
    core = lax.rem(me, PAIR)
    chip = me - core

    def across(i):
        return lax.rem(grp + i, GRP)

    barrier = pltpu.get_barrier_semaphore()
    for peer in range(SEQ):

        @pl.when(peer != me)
        def _():
            pl.semaphore_signal(barrier, 1, device_id={"seq": peer}, device_id_type=MESH)

    for i in range(1, GRP):
        for other in range(PAIR):
            there = {"seq": chip + other, "group": across(i)}
            pl.semaphore_signal(barrier, 1, device_id=there, device_id_type=MESH)

    q_copy = pltpu.make_async_copy(q_hbm.at[0], qbuf.at[me], local_sem.at[0])
    len_copy = pltpu.make_async_copy(len_hbm, lens, local_sem.at[1])
    q_copy.start()
    len_copy.start()

    def k_copy(step):
        some = pl.ds(step * UNIT, UNIT)
        return pltpu.make_async_copy(k_hbm.at[some], kbuf.at[some], k_sem.at[step])

    def v_copy(step):
        some = pl.ds(step * UNIT, UNIT)
        return pltpu.make_async_copy(v_hbm.at[some], vbuf.at[some], v_sem.at[step])

    def owner_of(quarter):
        return across((1, 2, 3, 0)[quarter])

    def w_copy(quarter):
        start = pl.multiple_of(owner_of(quarter) * COLS, 128)
        return pltpu.make_async_copy(
            w_hbm.at[core, :, :, pl.ds(start, COLS)], wbuf.at[quarter], w_sem.at[quarter]
        )

    for step in range(STEPS):
        k_copy(step).start(priority=1)
        v_copy(step).start(priority=1)
    for quarter in range(GRP):
        w_copy(quarter).start(priority=1)

    def q_remote(peer):
        return pltpu.make_async_remote_copy(
            src_ref=qbuf.at[me], dst_ref=qbuf.at[me],
            send_sem=q_send, recv_sem=q_recv.at[lax.div(me, UNIT)],
            device_id={"seq": peer}, device_id_type=MESH,
        )

    def q_wait(step, count):
        some = qbuf.at[pl.ds(step * UNIT, count)]
        return pltpu.make_async_remote_copy(
            src_ref=some, dst_ref=some, send_sem=q_send, recv_sem=q_recv.at[step],
            device_id={"seq": me}, device_id_type=MESH,
        )

    q_copy.wait()
    len_copy.wait()
    pl.semaphore_wait(barrier, SEQ - 1 + PAIR * (GRP - 1))
    for z in (3, 2, 1, 0):
        for x in (2, 3, 1, 0):
            for peer in range(z * ROW + x * PAIR, z * ROW + x * PAIR + PAIR):

                @pl.when(peer != me)
                def _():
                    q_remote(peer).start()

    def arrived(step):
        own = lax.div(me, UNIT) == step

        @pl.when(own)
        def _():
            q_wait(step, UNIT - 1).wait_recv()

        @pl.when(jnp.logical_not(own))
        def _():
            q_wait(step, UNIT).wait_recv()

        k_copy(step).wait()

    def scores(step, slot):
        lane = lax.broadcasted_iota(jnp.int32, (ROWS, STRETCH), 1) + me * STRETCH
        for u in range(UNIT):
            b = step * UNIT + u
            zero = jnp.zeros((GROUP, HEAD), jnp.float32)
            q0 = qbuf[b, 0].astype(jnp.float32)
            q1 = qbuf[b, 1].astype(jnp.float32)
            q = jnp.concatenate(
                [jnp.concatenate([q0, zero], axis=1), jnp.concatenate([zero, q1], axis=1)], axis=0
            ).astype(jnp.bfloat16)
            k = jnp.concatenate([kbuf[b, 0], kbuf[b, 1]], axis=1)
            logit = lax.dot_general(
                q, k, (((1,), (1,)), ((), ())), preferred_element_type=jnp.float32
            )
            logits[slot, u] = jnp.where(lane < lens[b], logit, -1e30)

    def reads(step, slot):
        row = lax.broadcasted_iota(jnp.int32, (ROWS, HEAD), 0)
        lane = lax.broadcasted_iota(jnp.int32, (ROWS, HEAD), 1)
        results = []
        for u in range(UNIT):
            b = step * UNIT + u
            logit = logits[slot, u]
            top = jnp.max(logit, axis=1, keepdims=True)
            part = jnp.exp2((logit - top) * TO_EXP2)
            total = jnp.sum(part, axis=1, keepdims=True)
            high = part.astype(jnp.bfloat16)
            low = (part - high.astype(jnp.float32)).astype(jnp.bfloat16)
            v = jnp.concatenate([vbuf[b, 0], vbuf[b, 1]], axis=1)
            both = jnp.dot(
                jnp.concatenate([high, low], axis=0), v, preferred_element_type=jnp.float32
            )
            results.append((both[:ROWS] + both[ROWS:], top, total))
        for u in range(0, UNIT, PAIR):
            for head in range(HEADS):
                own = slice(head * GROUP, (head + 1) * GROUP)
                here = slice(head * HEAD, (head + 1) * HEAD)
                two = results[u : u + PAIR]
                top = jnp.concatenate([r[1][own] for r in two], axis=0)
                total = jnp.concatenate([r[2][own] for r in two], axis=0)
                psend[step * UNIT + u + head] = jnp.concatenate([r[0][own, here] for r in two], axis=0)
                pair = jnp.where(lane == row, top, jnp.where(lane == row + ROWS, total, 0.0))
                ssend[step * UNIT + u + head] = jnp.sum(pair, axis=0, keepdims=True)

    def p_remote(b):
        return pltpu.make_async_remote_copy(
            src_ref=psend.at[b], dst_ref=parts.at[me], send_sem=p_send, recv_sem=p_recv,
            device_id={"seq": b}, device_id_type=MESH,
        )

    def s_remote(b):
        return pltpu.make_async_remote_copy(
            src_ref=ssend.at[b], dst_ref=stats.at[me], send_sem=s_send, recv_sem=s_recv,
            device_id={"seq": b}, device_id_type=MESH,
        )

    def send(step):
        for u in range(UNIT):
            b = step * UNIT + u

            @pl.when(b != me)
            def _():
                s_remote(b).start()
                p_remote(b).start()

    arrived(0)
    scores(0, 0)
    arrived(1)
    v_copy(0).wait()
    scores(1, 1)
    reads(0, 0)
    send(0)

    @pl.loop(0, STEPS // 2 - 1)
    def _(i):
        step = 2 * i + 1
        for ahead in range(PAIR):
            arrived(step + 1 + ahead)
            v_copy(step + ahead).wait()
        scores(step + 1, 0)
        reads(step, 1)
        scores(step + 2, 1)
        reads(step + 1, 0)
        send(step)
        send(step + 1)

    v_copy(STEPS - 1).wait()
    for quarter in range(GRP):
        w_copy(quarter).wait()
    reads(STEPS - 1, 1)
    send(STEPS - 1)
    parts[me] = psend[me]
    stats[me] = ssend[me]

    def all_but_one(ref, send_sem, recv_sem):
        most = ref.at[pl.ds(0, SEQ - 1)]
        return pltpu.make_async_remote_copy(
            src_ref=most, dst_ref=most, send_sem=send_sem, recv_sem=recv_sem,
            device_id={"seq": me}, device_id_type=MESH,
        )

    all_but_one(stats, s_send, s_recv).wait_recv()
    stat = stats[:, 0, :]
    best = jnp.max(stat, axis=0, keepdims=True)
    scale = jnp.exp2((stat - best) * TO_EXP2)
    sums = pltpu.roll(stat, HEAD - ROWS, axis=1)
    weight = scale / jnp.sum(sums * scale, axis=0, keepdims=True)
    weight = weight.T[:ROWS]

    all_but_one(parts, p_send, p_recv).wait_recv()
    read = jnp.zeros((ROWS, HEAD), jnp.float32)
    for i in range(SEQ):
        read = read + parts[i] * weight[:, i : i + 1]
    rows[...] = read.astype(jnp.bfloat16).astype(jnp.float32)
    even = lax.broadcasted_iota(jnp.int32, (GROUP, HEAD), 0) == 0
    spread = jnp.concatenate(
        [jnp.where(even, rows[r : r + 1, :], rows[GROUP + r : GROUP + r + 1, :]) for r in range(GROUP)],
        axis=1,
    ).astype(jnp.bfloat16)

    mine = grp * PAIR + core

    def y_remote(quarter, token, peer):
        return pltpu.make_async_remote_copy(
            src_ref=ysend.at[quarter, token], dst_ref=ybuf.at[mine], send_sem=y_send, recv_sem=y_recv,
            device_id={"seq": chip + token, "group": peer}, device_id_type=MESH,
        )

    for quarter in range(GRP):
        term = jnp.dot(
            spread, wbuf[quarter].reshape(GROUP * HEAD, COLS), preferred_element_type=jnp.float32
        )
        for token in range(PAIR):
            for n in range(COLS // 128):
                ysend[quarter, token, n : n + 1, :] = term[token : token + 1, n * 128 : (n + 1) * 128]
        if quarter < GRP - 1:
            for token in range(PAIR):
                y_remote(quarter, token, owner_of(quarter)).start()
    y_remote(GRP - 1, 1 - core, grp).start()
    ybuf[mine] = ysend[GRP - 1, core]

    def others(ref):
        most = ref.at[pl.ds(0, GRP * PAIR - 1)]
        return pltpu.make_async_remote_copy(
            src_ref=most, dst_ref=most, send_sem=y_send, recv_sem=y_recv,
            device_id={"seq": me}, device_id_type=MESH,
        )

    others(ybuf).wait_recv()
    token = ybuf[0]
    for i in range(1, GRP * PAIR):
        token = token + ybuf[i]
    for n in range(COLS // 128):
        out_ref[0:1, n * 128 : (n + 1) * 128] = token[n : n + 1, :].astype(out_ref.dtype)

    others(ybuf).wait_send()
    all_but_one(qbuf, q_send, q_recv.at[0]).wait_send()
    all_but_one(parts, p_send, p_recv).wait_send()
    all_but_one(stats, s_send, s_recv).wait_send()


def per_device(new_queries, stored_keys, stored_values, used_length, out_weight):
    hbm = pl.BlockSpec(memory_space=pl.ANY)
    dma = pltpu.SemaphoreType.DMA
    return pl.pallas_call(
        kernel,
        out_shape=pltpu.VMEM((1, COLS), jnp.bfloat16),
        in_specs=[hbm] * 5,
        out_specs=pl.BlockSpec(memory_space=pltpu.VMEM),
        scratch_shapes=[
            pltpu.VMEM((SEQ, HEADS, STRETCH, HEAD), jnp.bfloat16),
            pltpu.VMEM((SEQ, HEADS, STRETCH, HEAD), jnp.bfloat16),
            pltpu.VMEM((GRP, GROUP, HEAD, COLS), jnp.bfloat16),
            pltpu.VMEM((SEQ, HEADS, GROUP, HEAD), jnp.bfloat16),
            pltpu.SMEM((SEQ,), jnp.int32),
            pltpu.VMEM((2, UNIT, ROWS, STRETCH), jnp.float32),
            pltpu.VMEM((SEQ, ROWS, HEAD), jnp.float32),
            pltpu.VMEM((SEQ, 1, 128), jnp.float32),
            pltpu.VMEM((SEQ, ROWS, HEAD), jnp.float32),
            pltpu.VMEM((SEQ, 1, 128), jnp.float32),
            pltpu.VMEM((ROWS, HEAD), jnp.float32),
            pltpu.VMEM((GRP, PAIR, COLS // 128, 128), jnp.float32),
            pltpu.VMEM((GRP * PAIR, COLS // 128, 128), jnp.float32),
            dma((2,)), dma((STEPS,)), dma((STEPS,)), dma((GRP,)),
            dma(()), dma((STEPS,)), dma(()), dma(()), dma(()), dma(()),
            dma(()), dma(()),
        ],
        compiler_params=pltpu.CompilerParams(
            collective_id=0, has_side_effects=True, vmem_limit_bytes=60 * 1024 * 1024
        ),
        name="decode",
    )(new_queries, stored_keys, stored_values, used_length, out_weight)


def solution(mesh):
    in_specs = (
        P("seq", "group", None, None),
        P(None, "group", "seq", None),
        P(None, "group", "seq", None),
        P(),
        P("group", None, None, None),
    )
    return jax.shard_map(
        per_device, mesh=mesh, in_specs=in_specs, out_specs=P("seq", "group"), check_vma=False
    )
```

```python
import jax
import jax.numpy as jnp
from jax import lax
from jax.experimental import pallas as pl
from jax.experimental.pallas import tpu as pltpu
from jax.sharding import PartitionSpec as P

MESH = pl.DeviceIdType.MESH
SEQ, GRP = 32, 4
ROW, PAIR = 8, 2
HEADS, GROUP, HEAD = 2, 8, 128
ROWS = HEADS * GROUP
STRETCH = 512
COLS = 1280
UNIT = 4
STEPS = SEQ // UNIT
TO_EXP2 = HEAD ** (-0.5) * 1.4426950408889634


def kernel(
    q_hbm, k_hbm, v_hbm, len_hbm, w_hbm, out_ref,
    kbuf, vbuf, wbuf, qbuf, lens, logits, psend, ssend, parts, stats, rows, ysend, ybuf,
    local_sem, k_sem, v_sem, w_sem, q_send, q_recv, p_send, p_recv, s_send, s_recv, y_send, y_recv,
):
    me = lax.axis_index("seq")
    grp = lax.axis_index("group")
    core = lax.rem(me, PAIR)
    chip = me - core

    def across(i):
        return lax.rem(grp + i, GRP)

    barrier = pltpu.get_barrier_semaphore()
    for peer in range(SEQ):

        @pl.when(peer != me)
        def _():
            pl.semaphore_signal(barrier, 1, device_id={"seq": peer}, device_id_type=MESH)

    for i in range(1, GRP):
        for other in range(PAIR):
            there = {"seq": chip + other, "group": across(i)}
            pl.semaphore_signal(barrier, 1, device_id=there, device_id_type=MESH)

    q_copy = pltpu.make_async_copy(q_hbm.at[0], qbuf.at[me], local_sem.at[0])
    len_copy = pltpu.make_async_copy(len_hbm, lens, local_sem.at[1])
    q_copy.start()
    len_copy.start()

    def k_copy(layer):
        some = pl.ds(layer * ROW, ROW)
        return pltpu.make_async_copy(k_hbm.at[some], kbuf.at[some], k_sem.at[layer])

    def v_copy(layer):
        some = pl.ds(layer * ROW, ROW)
        return pltpu.make_async_copy(v_hbm.at[some], vbuf.at[some], v_sem.at[layer])

    def owner_of(quarter):
        return quarter + (quarter >= grp).astype(jnp.int32) if quarter < GRP - 1 else grp

    def w_copy(quarter):
        start = pl.multiple_of(owner_of(quarter) * COLS, 128)
        return pltpu.make_async_copy(
            w_hbm.at[core, :, :, pl.ds(start, COLS)], wbuf.at[quarter], w_sem.at[0]
        )

    for layer in range(SEQ // ROW):
        k_copy(layer).start(priority=1)
        v_copy(layer).start(priority=1)
    for quarter in range(GRP):
        w_copy(quarter).start(priority=1)

    def q_remote(peer):
        return pltpu.make_async_remote_copy(
            src_ref=qbuf.at[me], dst_ref=qbuf.at[me],
            send_sem=q_send, recv_sem=q_recv.at[lax.div(me, PAIR)],
            device_id={"seq": peer}, device_id_type=MESH,
        )

    def q_wait(place, count):
        some = qbuf.at[pl.ds(place * PAIR, count)]
        return pltpu.make_async_remote_copy(
            src_ref=some, dst_ref=some, send_sem=q_send, recv_sem=q_recv.at[place],
            device_id={"seq": me}, device_id_type=MESH,
        )

    q_copy.wait()
    len_copy.wait()
    pl.semaphore_wait(barrier, SEQ - 1 + PAIR * (GRP - 1))
    for z in (3, 2, 1, 0):
        for x in (2, 3, 1, 0):
            for peer in range(z * ROW + x * PAIR, z * ROW + x * PAIR + PAIR):

                @pl.when(peer != me)
                def _():
                    q_remote(peer).start()

    def arrived(place):
        own = place * PAIR == chip

        @pl.when(own)
        def _():
            q_wait(place, PAIR - 1).wait_recv()

        @pl.when(jnp.logical_not(own))
        def _():
            q_wait(place, PAIR).wait_recv()

    def scores(step, slot, units=range(UNIT)):
        lane = lax.broadcasted_iota(jnp.int32, (ROWS, STRETCH), 1) + me * STRETCH
        for u in units:
            b = step * UNIT + u
            zero = jnp.zeros((GROUP, HEAD), jnp.float32)
            q0 = qbuf[b, 0].astype(jnp.float32)
            q1 = qbuf[b, 1].astype(jnp.float32)
            q = jnp.concatenate(
                [jnp.concatenate([q0, zero], axis=1), jnp.concatenate([zero, q1], axis=1)], axis=0
            ).astype(jnp.bfloat16)
            k = jnp.concatenate([kbuf[b, 0], kbuf[b, 1]], axis=1)
            logit = lax.dot_general(
                q, k, (((1,), (1,)), ((), ())), preferred_element_type=jnp.float32
            )
            logits[slot, u] = jnp.where(lane < lens[b], logit, -1e30)

    def reads(step, slot, units=range(UNIT)):
        row = lax.broadcasted_iota(jnp.int32, (ROWS, HEAD), 0)
        lane = lax.broadcasted_iota(jnp.int32, (ROWS, HEAD), 1)
        results = []
        for u in units:
            b = step * UNIT + u
            logit = logits[slot, u]
            top = jnp.max(logit, axis=1, keepdims=True)
            part = jnp.exp2((logit - top) * TO_EXP2)
            total = jnp.sum(part, axis=1, keepdims=True)
            high = part.astype(jnp.bfloat16)
            low = (part - high.astype(jnp.float32)).astype(jnp.bfloat16)
            v = jnp.concatenate([vbuf[b, 0], vbuf[b, 1]], axis=1)
            both = jnp.dot(
                jnp.concatenate([high, low], axis=0), v, preferred_element_type=jnp.float32
            )
            results.append((both[:ROWS] + both[ROWS:], top, total))
        for n, u in enumerate(units[::PAIR]):
            for head in range(HEADS):
                own = slice(head * GROUP, (head + 1) * GROUP)
                here = slice(head * HEAD, (head + 1) * HEAD)
                two = results[n * PAIR : (n + 1) * PAIR]
                top = jnp.concatenate([r[1][own] for r in two], axis=0)
                total = jnp.concatenate([r[2][own] for r in two], axis=0)
                psend[step * UNIT + u + head] = jnp.concatenate([r[0][own, here] for r in two], axis=0)
                pair = jnp.where(lane == row, top, jnp.where(lane == row + ROWS, total, 0.0))
                ssend[step * UNIT + u + head] = jnp.sum(pair, axis=0, keepdims=True)

    def p_remote(b):
        return pltpu.make_async_remote_copy(
            src_ref=psend.at[b], dst_ref=parts.at[me], send_sem=p_send, recv_sem=p_recv,
            device_id={"seq": b}, device_id_type=MESH,
        )

    def s_remote(b):
        return pltpu.make_async_remote_copy(
            src_ref=ssend.at[b], dst_ref=stats.at[me], send_sem=s_send, recv_sem=s_recv,
            device_id={"seq": b}, device_id_type=MESH,
        )

    def send(step, units=range(UNIT)):
        for u in units:
            b = step * UNIT + u

            @pl.when(b != me)
            def _():
                s_remote(b).start()
                p_remote(b).start()

    head, tail = range(PAIR), range(PAIR, UNIT)
    arrived(0)
    k_copy(0).wait()
    v_copy(0).wait()
    scores(0, 0, head)
    reads(0, 0, head)
    send(0, head)
    arrived(1)
    arrived(2)
    arrived(3)
    scores(0, 0, tail)
    scores(1, 1)
    reads(0, 0, tail)
    send(0, tail)

    @pl.loop(0, SEQ // ROW - 1)
    def _(layer):
        step = 2 * layer + 1
        for i in range(4):
            arrived(2 * (step + 1) + i)
        k_copy(layer + 1).wait()
        v_copy(layer + 1).wait()
        scores(step + 1, 0)
        reads(step, 1)
        scores(step + 2, 1)
        reads(step + 1, 0)
        send(step)
        send(step + 1)

    pltpu.make_async_copy(wbuf, wbuf, w_sem.at[0]).wait()
    reads(STEPS - 1, 1)
    send(STEPS - 1)
    parts[me] = psend[me]
    stats[me] = ssend[me]

    def all_but_one(ref, send_sem, recv_sem):
        most = ref.at[pl.ds(0, SEQ - 1)]
        return pltpu.make_async_remote_copy(
            src_ref=most, dst_ref=most, send_sem=send_sem, recv_sem=recv_sem,
            device_id={"seq": me}, device_id_type=MESH,
        )

    all_but_one(stats, s_send, s_recv).wait_recv()
    stat = stats[:, 0, :]
    best = jnp.max(stat, axis=0, keepdims=True)
    scale = jnp.exp2((stat - best) * TO_EXP2)
    sums = pltpu.roll(stat, HEAD - ROWS, axis=1)
    weight = scale / jnp.sum(sums * scale, axis=0, keepdims=True)
    weight = weight.T[:ROWS]

    all_but_one(parts, p_send, p_recv).wait_recv()
    read = jnp.zeros((ROWS, HEAD), jnp.float32)
    for i in range(SEQ):
        read = read + parts[i] * weight[:, i : i + 1]
    rows[...] = read.astype(jnp.bfloat16).astype(jnp.float32)
    even = lax.broadcasted_iota(jnp.int32, (GROUP, HEAD), 0) == 0
    spread = jnp.concatenate(
        [jnp.where(even, rows[r : r + 1, :], rows[GROUP + r : GROUP + r + 1, :]) for r in range(GROUP)],
        axis=1,
    ).astype(jnp.bfloat16)

    mine = grp * PAIR + core

    def y_remote(quarter, token, peer):
        return pltpu.make_async_remote_copy(
            src_ref=ysend.at[quarter, token], dst_ref=ybuf.at[mine], send_sem=y_send, recv_sem=y_recv,
            device_id={"seq": chip + token, "group": peer}, device_id_type=MESH,
        )

    def term(quarter, start, stop, top=0, bottom=GROUP):
        return jnp.dot(
            spread[:, top * HEAD : bottom * HEAD],
            wbuf[quarter, top:bottom, :, start:stop].reshape((bottom - top) * HEAD, stop - start),
            preferred_element_type=jnp.float32,
        )

    def rest(quarter):
        last = term(quarter, 1024, COLS, 0, GROUP // 2) + term(quarter, 1024, COLS, GROUP // 2)
        return [term(quarter, 512, 1024), last]

    terms = [term(0, 0, 512), *rest(0)]
    for quarter in range(GRP):
        ahead = [term(quarter + 1, 0, 512)] if quarter < GRP - 1 else []
        line = jnp.concatenate(terms, axis=1)
        for token in range(PAIR):
            for n in range(COLS // 128):
                ysend[quarter, token, n : n + 1, :] = line[token : token + 1, n * 128 : (n + 1) * 128]
        if quarter < GRP - 1:
            for token in range(PAIR):
                y_remote(quarter, token, owner_of(quarter)).start()
            terms = [*ahead, *rest(quarter + 1)]
    y_remote(GRP - 1, 1 - core, grp).start()
    ybuf[mine] = ysend[GRP - 1, core]

    def others(ref):
        most = ref.at[pl.ds(0, GRP * PAIR - 1)]
        return pltpu.make_async_remote_copy(
            src_ref=most, dst_ref=most, send_sem=y_send, recv_sem=y_recv,
            device_id={"seq": me}, device_id_type=MESH,
        )

    others(ybuf).wait_recv()
    token = ybuf[0]
    for i in range(1, GRP * PAIR):
        token = token + ybuf[i]
    for n in range(COLS // 128):
        out_ref[0:1, n * 128 : (n + 1) * 128] = token[n : n + 1, :].astype(out_ref.dtype)

    others(ybuf).wait_send()
    all_but_one(qbuf, q_send, q_recv.at[0]).wait_send()
    all_but_one(parts, p_send, p_recv).wait_send()
    all_but_one(stats, s_send, s_recv).wait_send()


def per_device(new_queries, stored_keys, stored_values, used_length, out_weight):
    hbm = pl.BlockSpec(memory_space=pl.ANY)
    dma = pltpu.SemaphoreType.DMA
    return pl.pallas_call(
        kernel,
        out_shape=pltpu.VMEM((1, COLS), jnp.bfloat16),
        in_specs=[hbm] * 5,
        out_specs=pl.BlockSpec(memory_space=pltpu.VMEM),
        scratch_shapes=[
            pltpu.VMEM((SEQ, HEADS, STRETCH, HEAD), jnp.bfloat16),
            pltpu.VMEM((SEQ, HEADS, STRETCH, HEAD), jnp.bfloat16),
            pltpu.VMEM((GRP, GROUP, HEAD, COLS), jnp.bfloat16),
            pltpu.VMEM((SEQ, HEADS, GROUP, HEAD), jnp.bfloat16),
            pltpu.SMEM((SEQ,), jnp.int32),
            pltpu.VMEM((2, UNIT, ROWS, STRETCH), jnp.float32),
            pltpu.VMEM((SEQ, ROWS, HEAD), jnp.float32),
            pltpu.VMEM((SEQ, 1, 128), jnp.float32),
            pltpu.VMEM((SEQ, ROWS, HEAD), jnp.float32),
            pltpu.VMEM((SEQ, 1, 128), jnp.float32),
            pltpu.VMEM((ROWS, HEAD), jnp.float32),
            pltpu.VMEM((GRP, PAIR, COLS // 128, 128), jnp.float32),
            pltpu.VMEM((GRP * PAIR, COLS // 128, 128), jnp.float32),
            dma((2,)), dma((SEQ // ROW,)), dma((SEQ // ROW,)), dma((1,)),
            dma(()), dma((SEQ // PAIR,)), dma(()), dma(()), dma(()), dma(()),
            dma(()), dma(()),
        ],
        compiler_params=pltpu.CompilerParams(
            collective_id=0, has_side_effects=True, vmem_limit_bytes=60 * 1024 * 1024
        ),
        name="decode",
    )(new_queries, stored_keys, stored_values, used_length, out_weight)


def solution(mesh):
    in_specs = (
        P("seq", "group", None, None),
        P(None, "group", "seq", None),
        P(None, "group", "seq", None),
        P(),
        P("group", None, None, None),
    )
    return jax.shard_map(
        per_device, mesh=mesh, in_specs=in_specs, out_specs=P("seq", "group"), check_vma=False
    )
```

```python
import jax
import jax.numpy as jnp
from jax import lax
from jax.experimental import pallas as pl
from jax.experimental.pallas import tpu as pltpu
from jax.sharding import PartitionSpec as P

MESH = pl.DeviceIdType.MESH
SEQ, GRP = 32, 4
ROW, PAIR = 8, 2
HEADS, GROUP, HEAD = 2, 8, 128
ROWS = HEADS * GROUP
STRETCH = 512
COLS = 1280
UNIT = 4
STEPS = SEQ // UNIT
TO_EXP2 = HEAD ** (-0.5) * 1.4426950408889634


def kernel(
    q_hbm, k_hbm, v_hbm, len_hbm, w_hbm, out_ref,
    kbuf, vbuf, wbuf, qbuf, lens, logits, psend, ssend, parts, stats, rows, ysend, ybuf,
    local_sem, kv_sem, w_sem, q_send, q_recv, p_send, p_recv, s_send, s_recv, y_send, y_recv,
):
    me = lax.axis_index("seq")
    grp = lax.axis_index("group")
    core = lax.rem(me, PAIR)
    chip = me - core

    def across(i):
        return lax.rem(grp + i, GRP)

    barrier = pltpu.get_barrier_semaphore()
    for peer in range(SEQ):

        @pl.when(peer != me)
        def _():
            pl.semaphore_signal(barrier, 1, device_id={"seq": peer}, device_id_type=MESH)

    for i in range(1, GRP):
        for other in range(PAIR):
            there = {"seq": chip + other, "group": across(i)}
            pl.semaphore_signal(barrier, 1, device_id=there, device_id_type=MESH)

    q_copy = pltpu.make_async_copy(q_hbm.at[0], qbuf.at[me], local_sem.at[0])
    len_copy = pltpu.make_async_copy(len_hbm, lens, local_sem.at[1])
    q_copy.start()
    len_copy.start()

    def nth(n):
        if isinstance(n, int):
            return {3: 6, 4: 3, 5: 4, 6: 5}.get(n, n)
        return n + jnp.where(n == 3, 3, 0) + jnp.where(n == 4, -1, 0) + jnp.where(n == 5, -1, 0) + jnp.where(n == 6, -1, 0)

    def load(n):
        some = pl.ds(nth(n) * UNIT, UNIT)
        pltpu.make_async_copy(k_hbm.at[some], kbuf.at[some], kv_sem.at[n]).start(priority=1)
        pltpu.make_async_copy(v_hbm.at[some], vbuf.at[some], kv_sem.at[n]).start(priority=1)

    def loaded(n):
        both = kbuf.at[pl.ds(0, 2 * UNIT)]
        pltpu.make_async_copy(both, both, kv_sem.at[n]).wait()

    def owner_of(quarter):
        return quarter + (quarter >= grp).astype(jnp.int32) if quarter < GRP - 1 else grp

    def w_copy(quarter):
        start = pl.multiple_of(owner_of(quarter) * COLS, 128)
        return pltpu.make_async_copy(
            w_hbm.at[core, :, :, pl.ds(start, COLS)], wbuf.at[quarter], w_sem.at[0]
        )

    for n in range(STEPS):
        load(n)
    for quarter in range(GRP):
        w_copy(quarter).start(priority=1)

    def q_remote(peer):
        return pltpu.make_async_remote_copy(
            src_ref=qbuf.at[me], dst_ref=qbuf.at[me],
            send_sem=q_send, recv_sem=q_recv.at[lax.div(me, PAIR)],
            device_id={"seq": peer}, device_id_type=MESH,
        )

    def q_wait(place, count):
        some = qbuf.at[pl.ds(place * PAIR, count)]
        return pltpu.make_async_remote_copy(
            src_ref=some, dst_ref=some, send_sem=q_send, recv_sem=q_recv.at[place],
            device_id={"seq": me}, device_id_type=MESH,
        )

    q_copy.wait()
    len_copy.wait()
    pl.semaphore_wait(barrier, SEQ - 1 + PAIR * (GRP - 1))
    for z in (3, 2, 1, 0):
        for x in (2, 3, 1, 0):
            for peer in range(z * ROW + x * PAIR, z * ROW + x * PAIR + PAIR):

                @pl.when(peer != me)
                def _():
                    q_remote(peer).start()

    def arrived(place):
        own = place * PAIR == chip

        @pl.when(own)
        def _():
            q_wait(place, PAIR - 1).wait_recv()

        @pl.when(jnp.logical_not(own))
        def _():
            q_wait(place, PAIR).wait_recv()

    def scores(step, slot, units=range(UNIT)):
        lane = lax.broadcasted_iota(jnp.int32, (ROWS, STRETCH), 1) + me * STRETCH
        for u in units:
            b = step * UNIT + u
            zero = jnp.zeros((GROUP, HEAD), jnp.float32)
            q0 = qbuf[b, 0].astype(jnp.float32)
            q1 = qbuf[b, 1].astype(jnp.float32)
            q = jnp.concatenate(
                [jnp.concatenate([q0, zero], axis=1), jnp.concatenate([zero, q1], axis=1)], axis=0
            ).astype(jnp.bfloat16)
            k = jnp.concatenate([kbuf[b, 0], kbuf[b, 1]], axis=1)
            logit = lax.dot_general(
                q, k, (((1,), (1,)), ((), ())), preferred_element_type=jnp.float32
            )
            logits[slot, u] = jnp.where(lane < lens[b], logit, -1e30)

    def reads(step, slot, units=range(UNIT)):
        row = lax.broadcasted_iota(jnp.int32, (ROWS, HEAD), 0)
        lane = lax.broadcasted_iota(jnp.int32, (ROWS, HEAD), 1)
        results = []
        for u in units:
            b = step * UNIT + u
            logit = logits[slot, u]
            top = jnp.max(logit, axis=1, keepdims=True)
            part = jnp.exp2((logit - top) * TO_EXP2)
            total = jnp.sum(part, axis=1, keepdims=True)
            high = part.astype(jnp.bfloat16)
            low = (part - high.astype(jnp.float32)).astype(jnp.bfloat16)
            v = jnp.concatenate([vbuf[b, 0], vbuf[b, 1]], axis=1)
            both = jnp.dot(
                jnp.concatenate([high, low], axis=0), v, preferred_element_type=jnp.float32
            )
            results.append((both[:ROWS] + both[ROWS:], top, total))
        for n, u in enumerate(units[::PAIR]):
            for head in range(HEADS):
                own = slice(head * GROUP, (head + 1) * GROUP)
                here = slice(head * HEAD, (head + 1) * HEAD)
                two = results[n * PAIR : (n + 1) * PAIR]
                top = jnp.concatenate([r[1][own] for r in two], axis=0)
                total = jnp.concatenate([r[2][own] for r in two], axis=0)
                psend[step * UNIT + u + head] = jnp.concatenate([r[0][own, here] for r in two], axis=0)
                pair = jnp.where(lane == row, top, jnp.where(lane == row + ROWS, total, 0.0))
                ssend[step * UNIT + u + head] = jnp.sum(pair, axis=0, keepdims=True)

    def p_remote(b):
        return pltpu.make_async_remote_copy(
            src_ref=psend.at[b], dst_ref=parts.at[me], send_sem=p_send, recv_sem=p_recv,
            device_id={"seq": b}, device_id_type=MESH,
        )

    def s_remote(b):
        return pltpu.make_async_remote_copy(
            src_ref=ssend.at[b], dst_ref=stats.at[me], send_sem=s_send, recv_sem=s_recv,
            device_id={"seq": b}, device_id_type=MESH,
        )

    def send(step, units=range(UNIT)):
        for u in units:
            b = step * UNIT + u

            @pl.when(b != me)
            def _():
                s_remote(b).start()
                p_remote(b).start()

    head, tail = range(PAIR), range(PAIR, UNIT)
    arrived(0)
    loaded(0)
    scores(0, 0, head)
    reads(0, 0, head)
    send(0, head)
    arrived(1)
    arrived(2 * nth(1))
    arrived(2 * nth(1) + 1)
    loaded(1)
    scores(0, 0, tail)
    scores(nth(1), 1)
    reads(0, 0, tail)
    send(0, tail)

    @pl.loop(0, STEPS // 2 - 1)
    def _(i):
        n = 2 * i + 1
        now, second, third = nth(n), nth(n + 1), nth(n + 2)
        for step in (second, third):
            arrived(2 * step)
            arrived(2 * step + 1)
        loaded(n + 1)
        loaded(n + 2)
        scores(second, 0)
        reads(now, 1)
        scores(third, 1)
        reads(second, 0)
        send(now)
        send(second)

    pltpu.make_async_copy(wbuf, wbuf, w_sem.at[0]).wait()
    reads(nth(STEPS - 1), 1)
    send(nth(STEPS - 1))
    parts[me] = psend[me]
    stats[me] = ssend[me]

    def all_but_one(ref, send_sem, recv_sem):
        most = ref.at[pl.ds(0, SEQ - 1)]
        return pltpu.make_async_remote_copy(
            src_ref=most, dst_ref=most, send_sem=send_sem, recv_sem=recv_sem,
            device_id={"seq": me}, device_id_type=MESH,
        )

    all_but_one(stats, s_send, s_recv).wait_recv()
    stat = stats[:, 0, :]
    best = jnp.max(stat, axis=0, keepdims=True)
    scale = jnp.exp2((stat - best) * TO_EXP2)
    sums = pltpu.roll(stat, HEAD - ROWS, axis=1)
    weight = scale / jnp.sum(sums * scale, axis=0, keepdims=True)
    weight = weight.T[:ROWS]

    all_but_one(parts, p_send, p_recv).wait_recv()
    read = jnp.zeros((ROWS, HEAD), jnp.float32)
    for i in range(SEQ):
        read = read + parts[i] * weight[:, i : i + 1]
    rows[...] = read.astype(jnp.bfloat16).astype(jnp.float32)
    even = lax.broadcasted_iota(jnp.int32, (GROUP, HEAD), 0) == 0
    spread = jnp.concatenate(
        [jnp.where(even, rows[r : r + 1, :], rows[GROUP + r : GROUP + r + 1, :]) for r in range(GROUP)],
        axis=1,
    ).astype(jnp.bfloat16)

    mine = grp * PAIR + core

    def y_remote(quarter, token, peer):
        return pltpu.make_async_remote_copy(
            src_ref=ysend.at[quarter, token], dst_ref=ybuf.at[mine], send_sem=y_send, recv_sem=y_recv,
            device_id={"seq": chip + token, "group": peer}, device_id_type=MESH,
        )

    def part(*where):
        w = [wbuf[q, :, :, 256 * a : 256 * b].reshape(GROUP * HEAD, 256 * (b - a)) for q, a, b in where]
        return jnp.dot(spread, jnp.concatenate(w, axis=1), preferred_element_type=jnp.float32)

    def ship(quarter, terms):
        line = jnp.concatenate(terms, axis=1)
        for token in range(PAIR):
            for n in range(COLS // 128):
                ysend[quarter, token, n : n + 1, :] = line[token : token + 1, n * 128 : (n + 1) * 128]
        if quarter < GRP - 1:
            for token in range(PAIR):
                y_remote(quarter, token, owner_of(quarter)).start()

    first, second, shared = part((0, 0, 2)), part((0, 2, 4)), part((0, 4, 5), (1, 0, 1))
    ahead = part((1, 1, 3))
    ship(0, [first, second, shared[:, :256]])
    third = part((1, 3, 5))
    first = part((2, 0, 2))
    ship(1, [shared[:, 256:], ahead, third])
    second, shared = part((2, 2, 4)), part((2, 4, 5), (3, 0, 1))
    ahead = part((3, 1, 3))
    ship(2, [first, second, shared[:, :256]])
    ship(3, [shared[:, 256:], ahead, part((3, 3, 5))])
    y_remote(GRP - 1, 1 - core, grp).start()
    ybuf[mine] = ysend[GRP - 1, core]

    def others(ref):
        most = ref.at[pl.ds(0, GRP * PAIR - 1)]
        return pltpu.make_async_remote_copy(
            src_ref=most, dst_ref=most, send_sem=y_send, recv_sem=y_recv,
            device_id={"seq": me}, device_id_type=MESH,
        )

    others(ybuf).wait_recv()
    token = ybuf[0]
    for i in range(1, GRP * PAIR):
        token = token + ybuf[i]
    for n in range(COLS // 128):
        out_ref[0:1, n * 128 : (n + 1) * 128] = token[n : n + 1, :].astype(out_ref.dtype)

    others(ybuf).wait_send()
    all_but_one(qbuf, q_send, q_recv.at[0]).wait_send()
    all_but_one(parts, p_send, p_recv).wait_send()
    all_but_one(stats, s_send, s_recv).wait_send()


def per_device(new_queries, stored_keys, stored_values, used_length, out_weight):
    hbm = pl.BlockSpec(memory_space=pl.ANY)
    dma = pltpu.SemaphoreType.DMA
    return pl.pallas_call(
        kernel,
        out_shape=pltpu.VMEM((1, COLS), jnp.bfloat16),
        in_specs=[hbm] * 5,
        out_specs=pl.BlockSpec(memory_space=pltpu.VMEM),
        scratch_shapes=[
            pltpu.VMEM((SEQ, HEADS, STRETCH, HEAD), jnp.bfloat16),
            pltpu.VMEM((SEQ, HEADS, STRETCH, HEAD), jnp.bfloat16),
            pltpu.VMEM((GRP, GROUP, HEAD, COLS), jnp.bfloat16),
            pltpu.VMEM((SEQ, HEADS, GROUP, HEAD), jnp.bfloat16),
            pltpu.SMEM((SEQ,), jnp.int32),
            pltpu.VMEM((2, UNIT, ROWS, STRETCH), jnp.float32),
            pltpu.VMEM((SEQ, ROWS, HEAD), jnp.float32),
            pltpu.VMEM((SEQ, 1, 128), jnp.float32),
            pltpu.VMEM((SEQ, ROWS, HEAD), jnp.float32),
            pltpu.VMEM((SEQ, 1, 128), jnp.float32),
            pltpu.VMEM((ROWS, HEAD), jnp.float32),
            pltpu.VMEM((GRP, PAIR, COLS // 128, 128), jnp.float32),
            pltpu.VMEM((GRP * PAIR, COLS // 128, 128), jnp.float32),
            dma((2,)), dma((STEPS,)), dma((1,)),
            dma(()), dma((SEQ // PAIR,)), dma(()), dma(()), dma(()), dma(()),
            dma(()), dma(()),
        ],
        compiler_params=pltpu.CompilerParams(
            collective_id=0, has_side_effects=True, vmem_limit_bytes=60 * 1024 * 1024
        ),
        name="decode",
    )(new_queries, stored_keys, stored_values, used_length, out_weight)


def solution(mesh):
    in_specs = (
        P("seq", "group", None, None),
        P(None, "group", "seq", None),
        P(None, "group", "seq", None),
        P(),
        P("group", None, None, None),
    )
    return jax.shard_map(
        per_device, mesh=mesh, in_specs=in_specs, out_specs=P("seq", "group"), check_vma=False
    )
```

```python
import jax
import jax.numpy as jnp
from jax import lax
from jax.experimental import pallas as pl
from jax.experimental.pallas import tpu as pltpu
from jax.sharding import PartitionSpec as P

MESH = pl.DeviceIdType.MESH
SEQ, GRP = 32, 4
ROW, PAIR = 8, 2
HEADS, GROUP, HEAD = 2, 8, 128
ROWS = HEADS * GROUP
STRETCH = 512
COLS = 1280
UNIT = 4
STEPS = SEQ // UNIT
TO_EXP2 = HEAD ** (-0.5) * 1.4426950408889634


def kernel(
    q_hbm, k_hbm, v_hbm, len_hbm, w_hbm, out_ref,
    kbuf, vbuf, wbuf, qbuf, lens, logits, psend, ssend, parts, stats, rows, ysend, ybuf,
    local_sem, kv_sem, w_sem, q_send, q_recv, p_send, p_recv, s_send, s_recv, y_send, y_recv,
):
    me = lax.axis_index("seq")
    grp = lax.axis_index("group")
    core = lax.rem(me, PAIR)
    chip = me - core

    def across(i):
        return lax.rem(grp + i, GRP)

    barrier = pltpu.get_barrier_semaphore()
    for peer in range(SEQ):

        @pl.when(peer != me)
        def _():
            pl.semaphore_signal(barrier, 1, device_id={"seq": peer}, device_id_type=MESH)

    for i in range(1, GRP):
        for other in range(PAIR):
            there = {"seq": chip + other, "group": across(i)}
            pl.semaphore_signal(barrier, 1, device_id=there, device_id_type=MESH)

    q_copy = pltpu.make_async_copy(q_hbm.at[0], qbuf.at[me], local_sem.at[0])
    len_copy = pltpu.make_async_copy(len_hbm, lens, local_sem.at[1])
    q_copy.start()
    len_copy.start()

    def nth(n):
        if isinstance(n, int):
            return {3: 6, 4: 3, 5: 4, 6: 5}.get(n, n)
        return n + jnp.where(n == 3, 3, 0) + jnp.where(n == 4, -1, 0) + jnp.where(n == 5, -1, 0) + jnp.where(n == 6, -1, 0)

    def load(n):
        some = pl.ds(nth(n) * UNIT, UNIT)
        pltpu.make_async_copy(k_hbm.at[some], kbuf.at[some], kv_sem.at[n]).start(priority=1)
        pltpu.make_async_copy(v_hbm.at[some], vbuf.at[some], kv_sem.at[n]).start(priority=1)

    def loaded(n):
        both = kbuf.at[pl.ds(0, 2 * UNIT)]
        pltpu.make_async_copy(both, both, kv_sem.at[n]).wait()

    def owner_of(quarter):
        return quarter + (quarter >= grp).astype(jnp.int32) if quarter < GRP - 1 else grp

    def w_copy(quarter):
        start = pl.multiple_of(owner_of(quarter) * COLS, 128)
        return pltpu.make_async_copy(
            w_hbm.at[core, :, :, pl.ds(start, COLS)], wbuf.at[quarter], w_sem.at[0]
        )

    for n in range(STEPS):
        load(n)
    for quarter in range(GRP):
        w_copy(quarter).start(priority=1)

    def q_remote(peer):
        return pltpu.make_async_remote_copy(
            src_ref=qbuf.at[me], dst_ref=qbuf.at[me],
            send_sem=q_send, recv_sem=q_recv.at[lax.div(me, PAIR)],
            device_id={"seq": peer}, device_id_type=MESH,
        )

    def q_wait(place, count):
        some = qbuf.at[pl.ds(place * PAIR, count)]
        return pltpu.make_async_remote_copy(
            src_ref=some, dst_ref=some, send_sem=q_send, recv_sem=q_recv.at[place],
            device_id={"seq": me}, device_id_type=MESH,
        )

    q_copy.wait()
    len_copy.wait()
    pl.semaphore_wait(barrier, SEQ - 1 + PAIR * (GRP - 1))
    for z in (3, 2, 1, 0):
        for x in (2, 3, 1, 0):
            for peer in range(z * ROW + x * PAIR, z * ROW + x * PAIR + PAIR):

                @pl.when(peer != me)
                def _():
                    q_remote(peer).start()

    def arrived(place):
        own = place * PAIR == chip

        @pl.when(own)
        def _():
            q_wait(place, PAIR - 1).wait_recv()

        @pl.when(jnp.logical_not(own))
        def _():
            q_wait(place, PAIR).wait_recv()

    def scores(step, slot, units=range(UNIT)):
        lane = lax.broadcasted_iota(jnp.int32, (ROWS, STRETCH), 1) + me * STRETCH
        for u in units:
            b = step * UNIT + u
            zero = jnp.zeros((GROUP, HEAD), jnp.float32)
            q0 = qbuf[b, 0].astype(jnp.float32)
            q1 = qbuf[b, 1].astype(jnp.float32)
            q = jnp.concatenate(
                [jnp.concatenate([q0, zero], axis=1), jnp.concatenate([zero, q1], axis=1)], axis=0
            ).astype(jnp.bfloat16)
            k = jnp.concatenate([kbuf[b, 0], kbuf[b, 1]], axis=1)
            logit = lax.dot_general(
                q, k, (((1,), (1,)), ((), ())), preferred_element_type=jnp.float32
            )
            logits[slot, u] = jnp.where(lane < lens[b], logit, -1e30)

    def reads(step, slot, units=range(UNIT)):
        row = lax.broadcasted_iota(jnp.int32, (ROWS, HEAD), 0)
        lane = lax.broadcasted_iota(jnp.int32, (ROWS, HEAD), 1)
        results = []
        for u in units:
            b = step * UNIT + u
            logit = logits[slot, u]
            top = jnp.max(logit, axis=1, keepdims=True)
            part = jnp.exp2((logit - top) * TO_EXP2)
            total = jnp.sum(part, axis=1, keepdims=True)
            high = part.astype(jnp.bfloat16)
            low = (part - high.astype(jnp.float32)).astype(jnp.bfloat16)
            v = jnp.concatenate([vbuf[b, 0], vbuf[b, 1]], axis=1)
            both = jnp.dot(
                jnp.concatenate([high, low], axis=0), v, preferred_element_type=jnp.float32
            )
            results.append((both[:ROWS] + both[ROWS:], top, total))
        for n, u in enumerate(units[::PAIR]):
            for head in range(HEADS):
                own = slice(head * GROUP, (head + 1) * GROUP)
                here = slice(head * HEAD, (head + 1) * HEAD)
                two = results[n * PAIR : (n + 1) * PAIR]
                top = jnp.concatenate([r[1][own] for r in two], axis=0)
                total = jnp.concatenate([r[2][own] for r in two], axis=0)
                psend[step * UNIT + u + head] = jnp.concatenate([r[0][own, here] for r in two], axis=0)
                pair = jnp.where(lane == row, top, jnp.where(lane == row + ROWS, total, 0.0))
                ssend[pl.ds(step * UNIT + u + head, 1)] = jnp.sum(pair, axis=0, keepdims=True)

    def p_remote(b):
        return pltpu.make_async_remote_copy(
            src_ref=psend.at[b], dst_ref=parts.at[me], send_sem=p_send, recv_sem=p_recv,
            device_id={"seq": b}, device_id_type=MESH,
        )

    def s_remote(b):
        return pltpu.make_async_remote_copy(
            src_ref=ssend.at[pl.ds(b, 1)], dst_ref=stats.at[pl.ds(me, 1)], send_sem=s_send, recv_sem=s_recv,
            device_id={"seq": b}, device_id_type=MESH,
        )

    def send(step, units=range(UNIT)):
        for u in units:
            b = step * UNIT + u

            @pl.when(b != me)
            def _():
                s_remote(b).start()
                p_remote(b).start()

    head, tail = range(PAIR), range(PAIR, UNIT)
    arrived(0)
    loaded(0)
    scores(0, 0, head)
    reads(0, 0, head)
    send(0, head)
    arrived(1)
    arrived(2 * nth(1))
    arrived(2 * nth(1) + 1)
    loaded(1)
    scores(0, 0, tail)
    scores(nth(1), 1)
    reads(0, 0, tail)
    send(0, tail)

    @pl.loop(0, STEPS // 2 - 1)
    def _(i):
        n = 2 * i + 1
        now, second, third = nth(n), nth(n + 1), nth(n + 2)
        for step in (second, third):
            arrived(2 * step)
            arrived(2 * step + 1)
        loaded(n + 1)
        loaded(n + 2)
        scores(second, 0)
        reads(now, 1)
        send(now)
        scores(third, 1)
        reads(second, 0)
        send(second)

    pltpu.make_async_copy(wbuf, wbuf, w_sem.at[0]).wait()
    reads(nth(STEPS - 1), 1)
    send(nth(STEPS - 1))
    parts[me] = psend[me]
    stats[pl.ds(me, 1)] = ssend[pl.ds(me, 1)]

    def all_but_one(ref, send_sem, recv_sem):
        most = ref.at[pl.ds(0, SEQ - 1)]
        return pltpu.make_async_remote_copy(
            src_ref=most, dst_ref=most, send_sem=send_sem, recv_sem=recv_sem,
            device_id={"seq": me}, device_id_type=MESH,
        )

    all_but_one(stats, s_send, s_recv).wait_recv()
    stat = stats[...]
    best = jnp.max(stat, axis=0, keepdims=True)
    scale = jnp.exp2((stat - best) * TO_EXP2)
    sums = pltpu.roll(stat, HEAD - ROWS, axis=1)
    weight = scale / jnp.sum(sums * scale, axis=0, keepdims=True)
    weight = weight.T[:ROWS]

    all_but_one(parts, p_send, p_recv).wait_recv()
    read = jnp.zeros((ROWS, HEAD), jnp.float32)
    for i in range(SEQ):
        read = read + parts[i] * weight[:, i : i + 1]
    rows[...] = read.astype(jnp.bfloat16).astype(jnp.float32)
    even = lax.broadcasted_iota(jnp.int32, (GROUP, HEAD), 0) == 0
    spread = jnp.concatenate(
        [jnp.where(even, rows[r : r + 1, :], rows[GROUP + r : GROUP + r + 1, :]) for r in range(GROUP)],
        axis=1,
    ).astype(jnp.bfloat16)

    mine = grp * PAIR + core

    def y_remote(quarter, token, peer):
        return pltpu.make_async_remote_copy(
            src_ref=ysend.at[quarter, token], dst_ref=ybuf.at[mine], send_sem=y_send, recv_sem=y_recv,
            device_id={"seq": chip + token, "group": peer}, device_id_type=MESH,
        )

    def part(*where):
        w = [wbuf[q, :, :, 256 * a : 256 * b].reshape(GROUP * HEAD, 256 * (b - a)) for q, a, b in where]
        return jnp.dot(spread, jnp.concatenate(w, axis=1), preferred_element_type=jnp.float32)

    def ship(quarter, terms):
        line = jnp.concatenate(terms, axis=1)
        for token in range(PAIR):
            for n in range(COLS // 128):
                ysend[quarter, token, n : n + 1, :] = line[token : token + 1, n * 128 : (n + 1) * 128]
        if quarter < GRP - 1:
            for token in range(PAIR):
                y_remote(quarter, token, owner_of(quarter)).start()

    first, second, shared = part((0, 0, 2)), part((0, 2, 4)), part((0, 4, 5), (1, 0, 1))
    ahead = part((1, 1, 3))
    ship(0, [first, second, shared[:, :256]])
    third = part((1, 3, 5))
    first = part((2, 0, 2))
    ship(1, [shared[:, 256:], ahead, third])
    second, shared = part((2, 2, 4)), part((2, 4, 5), (3, 0, 1))
    ahead = part((3, 1, 3))
    ship(2, [first, second, shared[:, :256]])
    ship(3, [shared[:, 256:], ahead, part((3, 3, 5))])
    y_remote(GRP - 1, 1 - core, grp).start()
    ybuf[mine] = ysend[GRP - 1, core]

    def others(ref):
        most = ref.at[pl.ds(0, GRP * PAIR - 1)]
        return pltpu.make_async_remote_copy(
            src_ref=most, dst_ref=most, send_sem=y_send, recv_sem=y_recv,
            device_id={"seq": me}, device_id_type=MESH,
        )

    all_but_one(qbuf, q_send, q_recv.at[0]).wait_send()
    all_but_one(stats, s_send, s_recv).wait_send()
    all_but_one(parts, p_send, p_recv).wait_send()
    others(ybuf).wait_send()
    others(ybuf).wait_recv()
    token = ybuf[0]
    for i in range(1, GRP * PAIR):
        token = token + ybuf[i]
    for n in range(COLS // 128):
        out_ref[0:1, n * 128 : (n + 1) * 128] = token[n : n + 1, :].astype(out_ref.dtype)


def per_device(new_queries, stored_keys, stored_values, used_length, out_weight):
    hbm = pl.BlockSpec(memory_space=pl.ANY)
    dma = pltpu.SemaphoreType.DMA
    return pl.pallas_call(
        kernel,
        out_shape=pltpu.VMEM((1, COLS), jnp.bfloat16),
        in_specs=[hbm] * 5,
        out_specs=pl.BlockSpec(memory_space=pltpu.VMEM),
        scratch_shapes=[
            pltpu.VMEM((SEQ, HEADS, STRETCH, HEAD), jnp.bfloat16),
            pltpu.VMEM((SEQ, HEADS, STRETCH, HEAD), jnp.bfloat16),
            pltpu.VMEM((GRP, GROUP, HEAD, COLS), jnp.bfloat16),
            pltpu.VMEM((SEQ, HEADS, GROUP, HEAD), jnp.bfloat16),
            pltpu.SMEM((SEQ,), jnp.int32),
            pltpu.VMEM((2, UNIT, ROWS, STRETCH), jnp.float32),
            pltpu.VMEM((SEQ, ROWS, HEAD), jnp.float32),
            pltpu.VMEM((SEQ, 128), jnp.float32),
            pltpu.VMEM((SEQ, ROWS, HEAD), jnp.float32),
            pltpu.VMEM((SEQ, 128), jnp.float32),
            pltpu.VMEM((ROWS, HEAD), jnp.float32),
            pltpu.VMEM((GRP, PAIR, COLS // 128, 128), jnp.float32),
            pltpu.VMEM((GRP * PAIR, COLS // 128, 128), jnp.float32),
            dma((2,)), dma((STEPS,)), dma((1,)),
            dma(()), dma((SEQ // PAIR,)), dma(()), dma(()), dma(()), dma(()),
            dma(()), dma(()),
        ],
        compiler_params=pltpu.CompilerParams(
            collective_id=0, has_side_effects=True, vmem_limit_bytes=60 * 1024 * 1024
        ),
        name="decode",
    )(new_queries, stored_keys, stored_values, used_length, out_weight)


def solution(mesh):
    in_specs = (
        P("seq", "group", None, None),
        P(None, "group", "seq", None),
        P(None, "group", "seq", None),
        P(),
        P("group", None, None, None),
    )
    return jax.shard_map(
        per_device, mesh=mesh, in_specs=in_specs, out_specs=P("seq", "group"), check_vma=False
    )
```

```python
import jax
import jax.numpy as jnp
from jax import lax
from jax.experimental import pallas as pl
from jax.experimental.pallas import tpu as pltpu
from jax.sharding import PartitionSpec as P

MESH = pl.DeviceIdType.MESH
SEQ, GRP = 32, 4
ROW, PAIR = 8, 2
HEADS, GROUP, HEAD = 2, 8, 128
ROWS = HEADS * GROUP
STRETCH = 512
COLS = 1280
UNIT = 4
STEPS = SEQ // UNIT
TO_EXP2 = HEAD ** (-0.5) * 1.4426950408889634


def kernel(
    q_hbm, k_hbm, v_hbm, len_hbm, w_hbm, out_ref,
    kbuf, vbuf, wbuf, qbuf, lens, logits, psend, ssend, parts, stats, rows, ysend, ybuf,
    local_sem, kv_sem, w_sem, q_send, q_recv, p_send, p_recv, s_send, s_recv, y_send, y_recv,
):
    me = lax.axis_index("seq")
    grp = lax.axis_index("group")
    core = lax.rem(me, PAIR)
    chip = me - core

    def across(i):
        return lax.rem(grp + i, GRP)

    barrier = pltpu.get_barrier_semaphore()
    for peer in range(SEQ):

        @pl.when(peer != me)
        def _():
            pl.semaphore_signal(barrier, 1, device_id={"seq": peer}, device_id_type=MESH)

    for i in range(1, GRP):
        for other in range(PAIR):
            there = {"seq": chip + other, "group": across(i)}
            pl.semaphore_signal(barrier, 1, device_id=there, device_id_type=MESH)

    q_copy = pltpu.make_async_copy(q_hbm.at[0], qbuf.at[me], local_sem.at[0])
    len_copy = pltpu.make_async_copy(len_hbm, lens, local_sem.at[1])
    q_copy.start()
    len_copy.start()

    def nth(n):
        if isinstance(n, int):
            return {3: 6, 4: 3, 5: 4, 6: 5}.get(n, n)
        return n + jnp.where(n == 3, 3, 0) + jnp.where(n == 4, -1, 0) + jnp.where(n == 5, -1, 0) + jnp.where(n == 6, -1, 0)

    def load(n):
        some = pl.ds(nth(n) * UNIT, UNIT)
        pltpu.make_async_copy(k_hbm.at[some], kbuf.at[some], kv_sem.at[n]).start(priority=1)
        pltpu.make_async_copy(v_hbm.at[some], vbuf.at[some], kv_sem.at[n]).start(priority=1)

    def loaded(n):
        both = kbuf.at[pl.ds(0, 2 * UNIT)]
        pltpu.make_async_copy(both, both, kv_sem.at[n]).wait()

    def owner_of(quarter):
        return quarter + (quarter >= grp).astype(jnp.int32) if quarter < GRP - 1 else grp

    def w_copy(quarter):
        start = pl.multiple_of(owner_of(quarter) * COLS, 128)
        return pltpu.make_async_copy(
            w_hbm.at[core, :, :, pl.ds(start, COLS)], wbuf.at[quarter], w_sem.at[0]
        )

    for n in range(STEPS):
        load(n)
    for quarter in range(GRP):
        w_copy(quarter).start(priority=1)

    def q_remote(peer):
        return pltpu.make_async_remote_copy(
            src_ref=qbuf.at[me], dst_ref=qbuf.at[me],
            send_sem=q_send, recv_sem=q_recv.at[lax.div(me, PAIR)],
            device_id={"seq": peer}, device_id_type=MESH,
        )

    def q_wait(place, count):
        some = qbuf.at[pl.ds(place * PAIR, count)]
        return pltpu.make_async_remote_copy(
            src_ref=some, dst_ref=some, send_sem=q_send, recv_sem=q_recv.at[place],
            device_id={"seq": me}, device_id_type=MESH,
        )

    q_copy.wait()
    len_copy.wait()
    pl.semaphore_wait(barrier, SEQ - 1 + PAIR * (GRP - 1))
    for z in (3, 2, 1, 0):
        for x in (2, 3, 1, 0):
            for peer in range(z * ROW + x * PAIR, z * ROW + x * PAIR + PAIR):

                @pl.when(peer != me)
                def _():
                    q_remote(peer).start()

    def arrived(place):
        own = place * PAIR == chip

        @pl.when(own)
        def _():
            q_wait(place, PAIR - 1).wait_recv()

        @pl.when(jnp.logical_not(own))
        def _():
            q_wait(place, PAIR).wait_recv()

    def scores(step, slot, units=range(UNIT)):
        lane = lax.broadcasted_iota(jnp.int32, (ROWS, STRETCH), 1) + me * STRETCH
        for u in units:
            b = step * UNIT + u
            zero = jnp.zeros((GROUP, HEAD), jnp.float32)
            q0 = qbuf[b, 0].astype(jnp.float32)
            q1 = qbuf[b, 1].astype(jnp.float32)
            q = jnp.concatenate(
                [jnp.concatenate([q0, zero], axis=1), jnp.concatenate([zero, q1], axis=1)], axis=0
            ).astype(jnp.bfloat16)
            k = jnp.concatenate([kbuf[b, 0], kbuf[b, 1]], axis=1)
            logit = lax.dot_general(
                q, k, (((1,), (1,)), ((), ())), preferred_element_type=jnp.float32
            )
            logits[slot, u] = jnp.where(lane < lens[b], logit, -1e30)

    def reads(step, slot, units=range(UNIT)):
        row = lax.broadcasted_iota(jnp.int32, (ROWS, HEAD), 0)
        lane = lax.broadcasted_iota(jnp.int32, (ROWS, HEAD), 1)
        results = []
        for u in units:
            b = step * UNIT + u
            logit = logits[slot, u]
            top = jnp.max(logit, axis=1, keepdims=True)
            part = jnp.exp2((logit - top) * TO_EXP2)
            total = jnp.sum(part, axis=1, keepdims=True)
            high = part.astype(jnp.bfloat16)
            low = (part - high.astype(jnp.float32)).astype(jnp.bfloat16)
            v = jnp.concatenate([vbuf[b, 0], vbuf[b, 1]], axis=1)
            both = jnp.dot(
                jnp.concatenate([high, low], axis=0), v, preferred_element_type=jnp.float32
            )
            results.append((both[:ROWS] + both[ROWS:], top, total))
        for n, u in enumerate(units[::PAIR]):
            for head in range(HEADS):
                own = slice(head * GROUP, (head + 1) * GROUP)
                here = slice(head * HEAD, (head + 1) * HEAD)
                two = results[n * PAIR : (n + 1) * PAIR]
                top = jnp.concatenate([r[1][own] for r in two], axis=0)
                total = jnp.concatenate([r[2][own] for r in two], axis=0)
                psend[step * UNIT + u + head] = jnp.concatenate([r[0][own, here] for r in two], axis=0)
                pair = jnp.where(lane == row, top, jnp.where(lane == row + ROWS, total, 0.0))
                ssend[pl.ds(step * UNIT + u + head, 1)] = jnp.sum(pair, axis=0, keepdims=True)

    def p_remote(b):
        return pltpu.make_async_remote_copy(
            src_ref=psend.at[b], dst_ref=parts.at[me], send_sem=p_send, recv_sem=p_recv,
            device_id={"seq": b}, device_id_type=MESH,
        )

    def s_remote(b):
        return pltpu.make_async_remote_copy(
            src_ref=ssend.at[pl.ds(b, 1)], dst_ref=stats.at[pl.ds(me, 1)], send_sem=s_send, recv_sem=s_recv,
            device_id={"seq": b}, device_id_type=MESH,
        )

    def send(step, units=range(UNIT)):
        for u in units:
            b = step * UNIT + u

            @pl.when(b != me)
            def _():
                s_remote(b).start()
                p_remote(b).start()

    head, tail = range(PAIR), range(PAIR, UNIT)
    arrived(0)
    loaded(0)
    scores(0, 0, head)
    reads(0, 0, head)
    send(0, head)
    arrived(1)
    arrived(2 * nth(1))
    arrived(2 * nth(1) + 1)
    loaded(1)
    scores(0, 0, tail)
    scores(nth(1), 1)
    reads(0, 0, tail)
    send(0, tail)

    @pl.loop(0, STEPS // 2 - 1)
    def _(i):
        n = 2 * i + 1
        now, second, third = nth(n), nth(n + 1), nth(n + 2)
        for step in (second, third):
            arrived(2 * step)
            arrived(2 * step + 1)
        loaded(n + 1)
        loaded(n + 2)
        scores(second, 0)
        reads(now, 1)
        send(now)
        scores(third, 1)
        reads(second, 0)
        send(second)

    pltpu.make_async_copy(wbuf, wbuf, w_sem.at[0]).wait()
    reads(nth(STEPS - 1), 1)
    send(nth(STEPS - 1))
    parts[me] = psend[me]
    stats[pl.ds(me, 1)] = ssend[pl.ds(me, 1)]

    def all_but_one(ref, send_sem, recv_sem):
        most = ref.at[pl.ds(0, SEQ - 1)]
        return pltpu.make_async_remote_copy(
            src_ref=most, dst_ref=most, send_sem=send_sem, recv_sem=recv_sem,
            device_id={"seq": me}, device_id_type=MESH,
        )

    all_but_one(stats, s_send, s_recv).wait_recv()
    stat = stats[...]
    best = jnp.max(stat, axis=0, keepdims=True)
    scale = jnp.exp2((stat - best) * TO_EXP2)
    sums = pltpu.roll(stat, HEAD - ROWS, axis=1)
    weight = scale / jnp.sum(sums * scale, axis=0, keepdims=True)
    weight = weight.T[:ROWS]

    all_but_one(parts, p_send, p_recv).wait_recv()
    read = jnp.zeros((ROWS, HEAD), jnp.float32)
    for i in range(SEQ):
        read = read + parts[i] * weight[:, i : i + 1]
    rows[...] = read.astype(jnp.bfloat16).astype(jnp.float32)
    even = lax.broadcasted_iota(jnp.int32, (GROUP, HEAD), 0) == 0
    wide = jnp.concatenate(
        [jnp.where(even, rows[r : r + 1, :], rows[GROUP + r : GROUP + r + 1, :]) for r in range(GROUP)],
        axis=1,
    )
    spread = wide.astype(jnp.bfloat16)
    deep = GROUP * HEAD // 2
    folded = jnp.concatenate([wide[:, :deep], wide[:, deep:]], axis=0).astype(jnp.bfloat16)

    mine = grp * PAIR + core

    def y_remote(quarter, token, peer):
        return pltpu.make_async_remote_copy(
            src_ref=ysend.at[quarter, token], dst_ref=ybuf.at[mine], send_sem=y_send, recv_sem=y_recv,
            device_id={"seq": chip + token, "group": peer}, device_id_type=MESH,
        )

    def pair(quarter, start):
        w = wbuf[quarter, :, :, start : start + 512].reshape(GROUP * HEAD, 512)
        return jnp.dot(spread, w, preferred_element_type=jnp.float32)

    def single(quarter):
        w = wbuf[quarter, :, :, 1024:COLS]
        w = jnp.concatenate(
            [w[: GROUP // 2].reshape(deep, 256), w[GROUP // 2 :].reshape(deep, 256)], axis=1
        )
        both = jnp.dot(folded, w, preferred_element_type=jnp.float32)
        return both[:GROUP, :256] + both[GROUP:, 256:]

    def ship(quarter, terms):
        line = jnp.concatenate(terms, axis=1)
        for token in range(PAIR):
            for n in range(COLS // 128):
                ysend[quarter, token, n : n + 1, :] = line[token : token + 1, n * 128 : (n + 1) * 128]
        if quarter < GRP - 1:
            for token in range(PAIR):
                y_remote(quarter, token, owner_of(quarter)).start()

    ahead = pair(0, 0)
    for quarter in range(GRP):
        terms = [ahead, pair(quarter, 512), single(quarter)]
        if quarter < GRP - 1:
            ahead = pair(quarter + 1, 0)
        ship(quarter, terms)
    y_remote(GRP - 1, 1 - core, grp).start()
    ybuf[mine] = ysend[GRP - 1, core]

    def others(ref):
        most = ref.at[pl.ds(0, GRP * PAIR - 1)]
        return pltpu.make_async_remote_copy(
            src_ref=most, dst_ref=most, send_sem=y_send, recv_sem=y_recv,
            device_id={"seq": me}, device_id_type=MESH,
        )

    all_but_one(qbuf, q_send, q_recv.at[0]).wait_send()
    all_but_one(stats, s_send, s_recv).wait_send()
    all_but_one(parts, p_send, p_recv).wait_send()
    others(ybuf).wait_send()
    others(ybuf).wait_recv()
    token = ybuf[0]
    for i in range(1, GRP * PAIR):
        token = token + ybuf[i]
    for n in range(COLS // 128):
        out_ref[0:1, n * 128 : (n + 1) * 128] = token[n : n + 1, :].astype(out_ref.dtype)


def per_device(new_queries, stored_keys, stored_values, used_length, out_weight):
    hbm = pl.BlockSpec(memory_space=pl.ANY)
    dma = pltpu.SemaphoreType.DMA
    return pl.pallas_call(
        kernel,
        out_shape=pltpu.VMEM((1, COLS), jnp.bfloat16),
        in_specs=[hbm] * 5,
        out_specs=pl.BlockSpec(memory_space=pltpu.VMEM),
        scratch_shapes=[
            pltpu.VMEM((SEQ, HEADS, STRETCH, HEAD), jnp.bfloat16),
            pltpu.VMEM((SEQ, HEADS, STRETCH, HEAD), jnp.bfloat16),
            pltpu.VMEM((GRP, GROUP, HEAD, COLS), jnp.bfloat16),
            pltpu.VMEM((SEQ, HEADS, GROUP, HEAD), jnp.bfloat16),
            pltpu.SMEM((SEQ,), jnp.int32),
            pltpu.VMEM((2, UNIT, ROWS, STRETCH), jnp.float32),
            pltpu.VMEM((SEQ, ROWS, HEAD), jnp.float32),
            pltpu.VMEM((SEQ, 128), jnp.float32),
            pltpu.VMEM((SEQ, ROWS, HEAD), jnp.float32),
            pltpu.VMEM((SEQ, 128), jnp.float32),
            pltpu.VMEM((ROWS, HEAD), jnp.float32),
            pltpu.VMEM((GRP, PAIR, COLS // 128, 128), jnp.float32),
            pltpu.VMEM((GRP * PAIR, COLS // 128, 128), jnp.float32),
            dma((2,)), dma((STEPS,)), dma((1,)),
            dma(()), dma((SEQ // PAIR,)), dma(()), dma(()), dma(()), dma(()),
            dma(()), dma(()),
        ],
        compiler_params=pltpu.CompilerParams(
            collective_id=0, has_side_effects=True, vmem_limit_bytes=60 * 1024 * 1024
        ),
        name="decode",
    )(new_queries, stored_keys, stored_values, used_length, out_weight)


def solution(mesh):
    in_specs = (
        P("seq", "group", None, None),
        P(None, "group", "seq", None),
        P(None, "group", "seq", None),
        P(),
        P("group", None, None, None),
    )
    return jax.shard_map(
        per_device, mesh=mesh, in_specs=in_specs, out_specs=P("seq", "group"), check_vma=False
    )
```

```python
import jax
import jax.numpy as jnp
from jax import lax
from jax.experimental import pallas as pl
from jax.experimental.pallas import tpu as pltpu
from jax.sharding import PartitionSpec as P

MESH = pl.DeviceIdType.MESH
SEQ, GRP = 32, 4
ROW, PAIR = 8, 2
HEADS, GROUP, HEAD = 2, 8, 128
ROWS = HEADS * GROUP
STRETCH = 512
COLS = 1280
UNIT = 4
STEPS = SEQ // UNIT
KINDS = 2
TO_EXP2 = HEAD ** (-0.5) * 1.4426950408889634


def kernel(
    q_hbm, k_hbm, v_hbm, len_hbm, w_hbm, out_ref,
    kbuf, vbuf, wbuf, qbuf, lens, logits, psend, ssend, parts, stats, rows, ysend, ybuf,
    local_sem, kv_sem, w_sem, q_send, q_recv, p_send, p_recv, s_send, s_recv, y_send, y_recv,
):
    me = lax.axis_index("seq")
    grp = lax.axis_index("group")
    core = lax.rem(me, PAIR)
    chip = me - core

    def across(i):
        return lax.rem(grp + i, GRP)

    barrier = pltpu.get_barrier_semaphore()
    for peer in range(SEQ):

        @pl.when(peer != me)
        def _():
            pl.semaphore_signal(barrier, 1, device_id={"seq": peer}, device_id_type=MESH)

    for i in range(1, GRP):
        for other in range(PAIR):
            there = {"seq": chip + other, "group": across(i)}
            pl.semaphore_signal(barrier, 1, device_id=there, device_id_type=MESH)

    q_copy = pltpu.make_async_copy(q_hbm.at[0], qbuf.at[me], local_sem.at[0])
    len_copy = pltpu.make_async_copy(len_hbm, lens, local_sem.at[1])
    q_copy.start()
    len_copy.start()

    def nth(n):
        if isinstance(n, int):
            return {3: 6, 4: 3, 5: 4, 6: 5}.get(n, n)
        return n + jnp.where(n == 3, 3, 0) + jnp.where(n == 4, -1, 0) + jnp.where(n == 5, -1, 0) + jnp.where(n == 6, -1, 0)

    def load(n):
        some = pl.ds(nth(n) * UNIT, UNIT)
        pltpu.make_async_copy(k_hbm.at[some], kbuf.at[some], kv_sem.at[n]).start(priority=1)
        pltpu.make_async_copy(v_hbm.at[some], vbuf.at[some], kv_sem.at[n]).start(priority=1)

    def loaded(n):
        both = kbuf.at[pl.ds(0, 2 * UNIT)]
        pltpu.make_async_copy(both, both, kv_sem.at[n]).wait()

    def owner_of(quarter):
        return quarter + (quarter >= grp).astype(jnp.int32) if quarter < GRP - 1 else grp

    def w_copy(quarter):
        start = pl.multiple_of(owner_of(quarter) * COLS, 128)
        return pltpu.make_async_copy(
            w_hbm.at[core, :, :, pl.ds(start, COLS)], wbuf.at[quarter], w_sem.at[0]
        )

    for n in range(STEPS):
        load(n)
    for quarter in range(GRP):
        w_copy(quarter).start(priority=1)

    def q_remote(peer):
        return pltpu.make_async_remote_copy(
            src_ref=qbuf.at[me], dst_ref=qbuf.at[me],
            send_sem=q_send, recv_sem=q_recv.at[lax.div(me, PAIR)],
            device_id={"seq": peer}, device_id_type=MESH,
        )

    def q_wait(place, count):
        some = qbuf.at[pl.ds(place * PAIR, count)]
        return pltpu.make_async_remote_copy(
            src_ref=some, dst_ref=some, send_sem=q_send, recv_sem=q_recv.at[place],
            device_id={"seq": me}, device_id_type=MESH,
        )

    q_copy.wait()
    len_copy.wait()
    pl.semaphore_wait(barrier, SEQ - 1 + PAIR * (GRP - 1))
    for z in (3, 2, 1, 0):
        for x in (2, 3, 1, 0):
            for peer in range(z * ROW + x * PAIR, z * ROW + x * PAIR + PAIR):

                @pl.when(peer != me)
                def _():
                    q_remote(peer).start()

    def arrived(place):
        own = place * PAIR == chip

        @pl.when(own)
        def _():
            q_wait(place, PAIR - 1).wait_recv()

        @pl.when(jnp.logical_not(own))
        def _():
            q_wait(place, PAIR).wait_recv()

    def scores(step, slot, units=range(UNIT)):
        lane = lax.broadcasted_iota(jnp.int32, (ROWS, STRETCH), 1) + me * STRETCH
        for u in units:
            b = step * UNIT + u
            zero = jnp.zeros((GROUP, HEAD), jnp.float32)
            q0 = qbuf[b, 0].astype(jnp.float32)
            q1 = qbuf[b, 1].astype(jnp.float32)
            q = jnp.concatenate(
                [jnp.concatenate([q0, zero], axis=1), jnp.concatenate([zero, q1], axis=1)], axis=0
            ).astype(jnp.bfloat16)
            k = jnp.concatenate([kbuf[b, 0], kbuf[b, 1]], axis=1)
            logit = lax.dot_general(
                q, k, (((1,), (1,)), ((), ())), preferred_element_type=jnp.float32
            )
            logits[slot, u] = jnp.where(lane < lens[b], logit, -1e30)

    def reads(step, slot, units=range(UNIT)):
        row = lax.broadcasted_iota(jnp.int32, (ROWS, HEAD), 0)
        lane = lax.broadcasted_iota(jnp.int32, (ROWS, HEAD), 1)
        results = []
        for u in units:
            b = step * UNIT + u
            logit = logits[slot, u]
            top = jnp.max(logit, axis=1, keepdims=True)
            part = jnp.exp2((logit - top) * TO_EXP2)
            total = jnp.sum(part, axis=1, keepdims=True)
            high = part.astype(jnp.bfloat16)
            low = (part - high.astype(jnp.float32)).astype(jnp.bfloat16)
            v = jnp.concatenate([vbuf[b, 0], vbuf[b, 1]], axis=1)
            both = jnp.dot(
                jnp.concatenate([high, low], axis=0), v, preferred_element_type=jnp.float32
            )
            results.append((both[:ROWS] + both[ROWS:], top, total))
        for n, u in enumerate(units[::PAIR]):
            for head in range(HEADS):
                own = slice(head * GROUP, (head + 1) * GROUP)
                here = slice(head * HEAD, (head + 1) * HEAD)
                two = results[n * PAIR : (n + 1) * PAIR]
                top = jnp.concatenate([r[1][own] for r in two], axis=0)
                total = jnp.concatenate([r[2][own] for r in two], axis=0)
                psend[step * UNIT + u + head] = jnp.concatenate([r[0][own, here] for r in two], axis=0)
                for n_of, kind in enumerate((top, total)):
                    line = jnp.sum(jnp.where(lane == row, kind, 0.0), axis=0, keepdims=True)
                    ssend[pl.ds(KINDS * (step * UNIT + u + head) + n_of, 1)] = line

    def p_remote(b):
        return pltpu.make_async_remote_copy(
            src_ref=psend.at[b], dst_ref=parts.at[me], send_sem=p_send, recv_sem=p_recv,
            device_id={"seq": b}, device_id_type=MESH,
        )

    def s_remote(b):
        return pltpu.make_async_remote_copy(
            src_ref=ssend.at[pl.ds(KINDS * b, KINDS)], dst_ref=stats.at[pl.ds(KINDS * me, KINDS)], send_sem=s_send, recv_sem=s_recv,
            device_id={"seq": b}, device_id_type=MESH,
        )

    def send(step, units=range(UNIT)):
        for u in units:
            b = step * UNIT + u

            @pl.when(b != me)
            def _():
                s_remote(b).start()
                p_remote(b).start()

    head, tail = range(PAIR), range(PAIR, UNIT)
    arrived(0)
    loaded(0)
    scores(0, 0, head)
    reads(0, 0, head)
    send(0, head)
    arrived(1)
    arrived(2 * nth(1))
    arrived(2 * nth(1) + 1)
    loaded(1)
    scores(0, 0, tail)
    scores(nth(1), 1)
    reads(0, 0, tail)
    send(0, tail)

    @pl.loop(0, STEPS // 2 - 1)
    def _(i):
        n = 2 * i + 1
        now, second, third = nth(n), nth(n + 1), nth(n + 2)
        for step in (second, third):
            arrived(2 * step)
            arrived(2 * step + 1)
        loaded(n + 1)
        loaded(n + 2)
        scores(second, 0)
        reads(now, 1)
        send(now)
        scores(third, 1)
        reads(second, 0)
        send(second)

    pltpu.make_async_copy(wbuf, wbuf, w_sem.at[0]).wait()
    reads(nth(STEPS - 1), 1)
    send(nth(STEPS - 1))
    parts[me] = psend[me]
    for kind in range(KINDS):
        stats[pl.ds(KINDS * me + kind, 1)] = ssend[pl.ds(KINDS * me + kind, 1)]

    def all_but_one(ref, send_sem, recv_sem, each=1):
        most = ref.at[pl.ds(0, each * (SEQ - 1))]
        return pltpu.make_async_remote_copy(
            src_ref=most, dst_ref=most, send_sem=send_sem, recv_sem=recv_sem,
            device_id={"seq": me}, device_id_type=MESH,
        )

    all_but_one(stats, s_send, s_recv, KINDS).wait_recv()
    tops, sums = (stats[pl.ds(kind, SEQ, stride=KINDS)] for kind in range(KINDS))
    scale = jnp.exp2((tops - jnp.max(tops, axis=0, keepdims=True)) * TO_EXP2)
    weight = scale / jnp.sum(sums * scale, axis=0, keepdims=True)
    weight = weight.T[:ROWS]

    all_but_one(parts, p_send, p_recv).wait_recv()
    read = jnp.zeros((ROWS, HEAD), jnp.float32)
    for i in range(SEQ):
        read = read + parts[i] * weight[:, i : i + 1]
    rows[...] = read.astype(jnp.bfloat16).astype(jnp.float32)
    even = lax.broadcasted_iota(jnp.int32, (GROUP, HEAD), 0) == 0
    wide = jnp.concatenate(
        [jnp.where(even, rows[r : r + 1, :], rows[GROUP + r : GROUP + r + 1, :]) for r in range(GROUP)],
        axis=1,
    )
    spread = wide.astype(jnp.bfloat16)
    deep = GROUP * HEAD // 2
    folded = jnp.concatenate([wide[:, :deep], wide[:, deep:]], axis=0).astype(jnp.bfloat16)

    mine = grp * PAIR + core

    def y_remote(quarter, token, peer):
        return pltpu.make_async_remote_copy(
            src_ref=ysend.at[quarter, token], dst_ref=ybuf.at[mine], send_sem=y_send, recv_sem=y_recv,
            device_id={"seq": chip + token, "group": peer}, device_id_type=MESH,
        )

    def pair(quarter, start):
        w = wbuf[quarter, :, :, start : start + 512].reshape(GROUP * HEAD, 512)
        return jnp.dot(spread, w, preferred_element_type=jnp.float32)

    def single(quarter):
        w = wbuf[quarter, :, :, 1024:COLS]
        w = jnp.concatenate(
            [w[: GROUP // 2].reshape(deep, 256), w[GROUP // 2 :].reshape(deep, 256)], axis=1
        )
        both = jnp.dot(folded, w, preferred_element_type=jnp.float32)
        return both[:GROUP, :256] + both[GROUP:, 256:]

    def ship(quarter, terms):
        line = jnp.concatenate(terms, axis=1)
        for token in range(PAIR):
            for n in range(COLS // 128):
                ysend[quarter, token, n : n + 1, :] = line[token : token + 1, n * 128 : (n + 1) * 128]
        if quarter < GRP - 1:
            for token in range(PAIR):
                y_remote(quarter, token, owner_of(quarter)).start()

    ahead = pair(0, 0)
    for quarter in range(GRP):
        terms = [ahead, pair(quarter, 512), single(quarter)]
        if quarter < GRP - 1:
            ahead = pair(quarter + 1, 0)
        ship(quarter, terms)
    y_remote(GRP - 1, 1 - core, grp).start()
    ybuf[mine] = ysend[GRP - 1, core]

    def others(ref):
        most = ref.at[pl.ds(0, GRP * PAIR - 1)]
        return pltpu.make_async_remote_copy(
            src_ref=most, dst_ref=most, send_sem=y_send, recv_sem=y_recv,
            device_id={"seq": me}, device_id_type=MESH,
        )

    all_but_one(qbuf, q_send, q_recv.at[0]).wait_send()
    all_but_one(stats, s_send, s_recv, KINDS).wait_send()
    all_but_one(parts, p_send, p_recv).wait_send()
    others(ybuf).wait_send()
    others(ybuf).wait_recv()
    token = ybuf[0]
    for i in range(1, GRP * PAIR):
        token = token + ybuf[i]
    for n in range(COLS // 128):
        out_ref[0:1, n * 128 : (n + 1) * 128] = token[n : n + 1, :].astype(out_ref.dtype)


def per_device(new_queries, stored_keys, stored_values, used_length, out_weight):
    hbm = pl.BlockSpec(memory_space=pl.ANY)
    dma = pltpu.SemaphoreType.DMA
    return pl.pallas_call(
        kernel,
        out_shape=pltpu.VMEM((1, COLS), jnp.bfloat16),
        in_specs=[hbm] * 5,
        out_specs=pl.BlockSpec(memory_space=pltpu.VMEM),
        scratch_shapes=[
            pltpu.VMEM((SEQ, HEADS, STRETCH, HEAD), jnp.bfloat16),
            pltpu.VMEM((SEQ, HEADS, STRETCH, HEAD), jnp.bfloat16),
            pltpu.VMEM((GRP, GROUP, HEAD, COLS), jnp.bfloat16),
            pltpu.VMEM((SEQ, HEADS, GROUP, HEAD), jnp.bfloat16),
            pltpu.SMEM((SEQ,), jnp.int32),
            pltpu.VMEM((2, UNIT, ROWS, STRETCH), jnp.float32),
            pltpu.VMEM((SEQ, ROWS, HEAD), jnp.float32),
            pltpu.VMEM((KINDS * SEQ, 128), jnp.float32),
            pltpu.VMEM((SEQ, ROWS, HEAD), jnp.float32),
            pltpu.VMEM((KINDS * SEQ, 128), jnp.float32),
            pltpu.VMEM((ROWS, HEAD), jnp.float32),
            pltpu.VMEM((GRP, PAIR, COLS // 128, 128), jnp.float32),
            pltpu.VMEM((GRP * PAIR, COLS // 128, 128), jnp.float32),
            dma((2,)), dma((STEPS,)), dma((1,)),
            dma(()), dma((SEQ // PAIR,)), dma(()), dma(()), dma(()), dma(()),
            dma(()), dma(()),
        ],
        compiler_params=pltpu.CompilerParams(
            collective_id=0, has_side_effects=True, vmem_limit_bytes=60 * 1024 * 1024
        ),
        name="decode",
    )(new_queries, stored_keys, stored_values, used_length, out_weight)


def solution(mesh):
    in_specs = (
        P("seq", "group", None, None),
        P(None, "group", "seq", None),
        P(None, "group", "seq", None),
        P(),
        P("group", None, None, None),
    )
    return jax.shard_map(
        per_device, mesh=mesh, in_specs=in_specs, out_specs=P("seq", "group"), check_vma=False
    )
```

```python
import jax
import jax.numpy as jnp
from jax import lax
from jax.experimental import pallas as pl
from jax.experimental.pallas import tpu as pltpu
from jax.sharding import PartitionSpec as P

MESH = pl.DeviceIdType.MESH
SEQ, GRP = 32, 4
ROW, PAIR = 8, 2
HEADS, GROUP, HEAD = 2, 8, 128
ROWS = HEADS * GROUP
STRETCH = 512
COLS = 1280
UNIT = 4
STEPS = SEQ // UNIT
KINDS = 2
TO_EXP2 = HEAD ** (-0.5) * 1.4426950408889634


def kernel(
    q_hbm, k_hbm, v_hbm, len_hbm, w_hbm, out_ref,
    kbuf, vbuf, wbuf, qbuf, lens, logits, psend, ssend, parts, stats, rows, ysend, ybuf,
    local_sem, kv_sem, w_sem, q_send, q_recv, p_send, p_recv, s_send, s_recv, y_send, y_recv,
):
    me = lax.axis_index("seq")
    grp = lax.axis_index("group")
    core = lax.rem(me, PAIR)
    chip = me - core

    def across(i):
        return lax.rem(grp + i, GRP)

    barrier = pltpu.get_barrier_semaphore()
    for peer in range(SEQ):

        @pl.when(peer != me)
        def _():
            pl.semaphore_signal(barrier, 1, device_id={"seq": peer}, device_id_type=MESH)

    for i in range(1, GRP):
        for other in range(PAIR):
            there = {"seq": chip + other, "group": across(i)}
            pl.semaphore_signal(barrier, 1, device_id=there, device_id_type=MESH)

    q_copy = pltpu.make_async_copy(q_hbm.at[0], qbuf.at[me], local_sem.at[0])
    len_copy = pltpu.make_async_copy(len_hbm, lens, local_sem.at[1])
    q_copy.start()
    len_copy.start()

    def nth(n):
        if isinstance(n, int):
            return {3: 6, 4: 3, 5: 4, 6: 5}.get(n, n)
        return n + jnp.where(n == 3, 3, 0) + jnp.where(n == 4, -1, 0) + jnp.where(n == 5, -1, 0) + jnp.where(n == 6, -1, 0)

    def load(n):
        some = pl.ds(nth(n) * UNIT, UNIT)
        pltpu.make_async_copy(k_hbm.at[some], kbuf.at[some], kv_sem.at[n]).start(priority=1)
        pltpu.make_async_copy(v_hbm.at[some], vbuf.at[some], kv_sem.at[n]).start(priority=1)

    def loaded(n):
        both = kbuf.at[pl.ds(0, 2 * UNIT)]
        pltpu.make_async_copy(both, both, kv_sem.at[n]).wait()

    def owner_of(quarter):
        return quarter + (quarter >= grp).astype(jnp.int32) if quarter < GRP - 1 else grp

    def w_copy(quarter):
        start = pl.multiple_of(owner_of(quarter) * COLS, 128)
        return pltpu.make_async_copy(
            w_hbm.at[core, :, :, pl.ds(start, COLS)], wbuf.at[quarter], w_sem.at[0]
        )

    for n in range(STEPS):
        load(n)
    for quarter in range(GRP):
        w_copy(quarter).start(priority=1)

    def q_remote(peer):
        return pltpu.make_async_remote_copy(
            src_ref=qbuf.at[me], dst_ref=qbuf.at[me],
            send_sem=q_send, recv_sem=q_recv.at[lax.div(me, PAIR)],
            device_id={"seq": peer}, device_id_type=MESH,
        )

    def q_wait(place, count):
        some = qbuf.at[pl.ds(place * PAIR, count)]
        return pltpu.make_async_remote_copy(
            src_ref=some, dst_ref=some, send_sem=q_send, recv_sem=q_recv.at[place],
            device_id={"seq": me}, device_id_type=MESH,
        )

    q_copy.wait()
    len_copy.wait()
    pl.semaphore_wait(barrier, SEQ - 1 + PAIR * (GRP - 1))
    for z in (3, 2, 1, 0):
        for x in (2, 3, 1, 0):
            for peer in range(z * ROW + x * PAIR, z * ROW + x * PAIR + PAIR):

                @pl.when(peer != me)
                def _():
                    q_remote(peer).start()

    def arrived(place):
        own = place * PAIR == chip

        @pl.when(own)
        def _():
            q_wait(place, PAIR - 1).wait_recv()

        @pl.when(jnp.logical_not(own))
        def _():
            q_wait(place, PAIR).wait_recv()

    def scores(step, slot, units=range(UNIT)):
        lane = lax.broadcasted_iota(jnp.int32, (ROWS, STRETCH), 1) + me * STRETCH
        for u in units:
            b = step * UNIT + u
            zero = jnp.zeros((GROUP, HEAD), jnp.float32)
            q0 = qbuf[b, 0].astype(jnp.float32)
            q1 = qbuf[b, 1].astype(jnp.float32)
            q = jnp.concatenate(
                [jnp.concatenate([q0, zero], axis=1), jnp.concatenate([zero, q1], axis=1)], axis=0
            ).astype(jnp.bfloat16)
            k = jnp.concatenate([kbuf[b, 0], kbuf[b, 1]], axis=1)
            logit = lax.dot_general(
                q, k, (((1,), (1,)), ((), ())), preferred_element_type=jnp.float32
            )
            logits[slot, u] = jnp.where(lane < lens[b], logit, -1e30)

    def reads(step, slot, units=range(UNIT)):
        row = lax.broadcasted_iota(jnp.int32, (ROWS, HEAD), 0)
        lane = lax.broadcasted_iota(jnp.int32, (ROWS, HEAD), 1)
        results = []
        for u in units:
            b = step * UNIT + u
            logit = logits[slot, u]
            top = jnp.max(logit, axis=1, keepdims=True)
            part = jnp.exp2((logit - top) * TO_EXP2)
            total = jnp.sum(part, axis=1, keepdims=True)
            high = part.astype(jnp.bfloat16)
            low = (part - high.astype(jnp.float32)).astype(jnp.bfloat16)
            v = jnp.concatenate([vbuf[b, 0], vbuf[b, 1]], axis=1)
            both = jnp.dot(
                jnp.concatenate([high, low], axis=0), v, preferred_element_type=jnp.float32
            )
            results.append((both[:ROWS] + both[ROWS:], top, total))
        for n, u in enumerate(units[::PAIR]):
            for head in range(HEADS):
                own = slice(head * GROUP, (head + 1) * GROUP)
                here = slice(head * HEAD, (head + 1) * HEAD)
                two = results[n * PAIR : (n + 1) * PAIR]
                top = jnp.concatenate([r[1][own] for r in two], axis=0)
                total = jnp.concatenate([r[2][own] for r in two], axis=0)
                psend[step * UNIT + u + head] = jnp.concatenate([r[0][own, here] for r in two], axis=0)
                for n_of, kind in enumerate((top, total)):
                    line = jnp.sum(jnp.where(lane == row, kind, 0.0), axis=0, keepdims=True)
                    ssend[pl.ds(KINDS * (step * UNIT + u + head) + n_of, 1)] = line

    def p_remote(b):
        return pltpu.make_async_remote_copy(
            src_ref=psend.at[b], dst_ref=parts.at[me], send_sem=p_send, recv_sem=p_recv,
            device_id={"seq": b}, device_id_type=MESH,
        )

    def s_remote(b):
        return pltpu.make_async_remote_copy(
            src_ref=ssend.at[pl.ds(KINDS * b, KINDS)], dst_ref=stats.at[pl.ds(KINDS * me, KINDS)], send_sem=s_send, recv_sem=s_recv,
            device_id={"seq": b}, device_id_type=MESH,
        )

    def send(step, units=range(UNIT)):
        for u in units:
            b = step * UNIT + u

            @pl.when(b != me)
            def _():
                s_remote(b).start()
                p_remote(b).start()

    head, tail = range(PAIR), range(PAIR, UNIT)
    arrived(0)
    loaded(0)
    scores(0, 0, head)
    reads(0, 0, head)
    send(0, head)
    arrived(1)
    arrived(2 * nth(1))
    arrived(2 * nth(1) + 1)
    loaded(1)
    scores(0, 0, tail)
    scores(nth(1), 1)
    reads(0, 0, tail)
    send(0, tail)

    @pl.loop(0, STEPS // 2 - 2)
    def _(i):
        n = 2 * i + 1
        now, second, third = nth(n), nth(n + 1), nth(n + 2)
        for step in (second, third):
            arrived(2 * step)
            arrived(2 * step + 1)
        loaded(n + 1)
        loaded(n + 2)
        scores(second, 0)
        reads(now, 1)
        send(now)
        scores(third, 1)
        reads(second, 0)
        send(second)

    for n in (STEPS - 2, STEPS - 1):
        arrived(2 * nth(n))
        arrived(2 * nth(n) + 1)
        loaded(n)
    pltpu.make_async_copy(wbuf, wbuf, w_sem.at[0]).wait()
    scores(nth(STEPS - 2), 0)
    reads(nth(STEPS - 3), 1)
    send(nth(STEPS - 3))
    scores(nth(STEPS - 1), 1)
    reads(nth(STEPS - 2), 0)
    reads(nth(STEPS - 1), 1)
    send(nth(STEPS - 2))
    send(nth(STEPS - 1))
    parts[me] = psend[me]
    for kind in range(KINDS):
        stats[pl.ds(KINDS * me + kind, 1)] = ssend[pl.ds(KINDS * me + kind, 1)]

    def all_but_one(ref, send_sem, recv_sem, each=1):
        most = ref.at[pl.ds(0, each * (SEQ - 1))]
        return pltpu.make_async_remote_copy(
            src_ref=most, dst_ref=most, send_sem=send_sem, recv_sem=recv_sem,
            device_id={"seq": me}, device_id_type=MESH,
        )

    all_but_one(stats, s_send, s_recv, KINDS).wait_recv()
    tops, sums = (stats[pl.ds(kind, SEQ, stride=KINDS)] for kind in range(KINDS))
    scale = jnp.exp2((tops - jnp.max(tops, axis=0, keepdims=True)) * TO_EXP2)
    weight = scale / jnp.sum(sums * scale, axis=0, keepdims=True)
    weight = weight.T[:ROWS]

    all_but_one(parts, p_send, p_recv).wait_recv()
    read = jnp.zeros((ROWS, HEAD), jnp.float32)
    for i in range(SEQ):
        read = read + parts[i] * weight[:, i : i + 1]
    rows[...] = read.astype(jnp.bfloat16).astype(jnp.float32)
    even = lax.broadcasted_iota(jnp.int32, (GROUP, HEAD), 0) == 0
    wide = jnp.concatenate(
        [jnp.where(even, rows[r : r + 1, :], rows[GROUP + r : GROUP + r + 1, :]) for r in range(GROUP)],
        axis=1,
    )
    spread = wide.astype(jnp.bfloat16)
    deep = GROUP * HEAD // 2
    folded = jnp.concatenate([wide[:, :deep], wide[:, deep:]], axis=0).astype(jnp.bfloat16)

    mine = grp * PAIR + core

    def y_remote(quarter, token, peer):
        return pltpu.make_async_remote_copy(
            src_ref=ysend.at[quarter, token], dst_ref=ybuf.at[mine], send_sem=y_send, recv_sem=y_recv,
            device_id={"seq": chip + token, "group": peer}, device_id_type=MESH,
        )

    def pair(quarter, start):
        w = wbuf[quarter, :, :, start : start + 512].reshape(GROUP * HEAD, 512)
        return jnp.dot(spread, w, preferred_element_type=jnp.float32)

    def single(quarter):
        w = wbuf[quarter, :, :, 1024:COLS]
        w = jnp.concatenate(
            [w[: GROUP // 2].reshape(deep, 256), w[GROUP // 2 :].reshape(deep, 256)], axis=1
        )
        both = jnp.dot(folded, w, preferred_element_type=jnp.float32)
        return both[:GROUP, :256] + both[GROUP:, 256:]

    def ship(quarter, terms):
        line = jnp.concatenate(terms, axis=1)
        for token in range(PAIR):
            for n in range(COLS // 128):
                ysend[quarter, token, n : n + 1, :] = line[token : token + 1, n * 128 : (n + 1) * 128]
        if quarter < GRP - 1:
            for token in range(PAIR):
                y_remote(quarter, token, owner_of(quarter)).start()

    ahead = pair(0, 0)
    for quarter in range(GRP):
        terms = [ahead, pair(quarter, 512), single(quarter)]
        if quarter < GRP - 1:
            ahead = pair(quarter + 1, 0)
        ship(quarter, terms)
    y_remote(GRP - 1, 1 - core, grp).start()
    ybuf[mine] = ysend[GRP - 1, core]

    def others(ref):
        most = ref.at[pl.ds(0, GRP * PAIR - 1)]
        return pltpu.make_async_remote_copy(
            src_ref=most, dst_ref=most, send_sem=y_send, recv_sem=y_recv,
            device_id={"seq": me}, device_id_type=MESH,
        )

    all_but_one(qbuf, q_send, q_recv.at[0]).wait_send()
    all_but_one(stats, s_send, s_recv, KINDS).wait_send()
    all_but_one(parts, p_send, p_recv).wait_send()
    others(ybuf).wait_send()
    others(ybuf).wait_recv()
    token = ybuf[0]
    for i in range(1, GRP * PAIR):
        token = token + ybuf[i]
    for n in range(COLS // 128):
        out_ref[0:1, n * 128 : (n + 1) * 128] = token[n : n + 1, :].astype(out_ref.dtype)


def per_device(new_queries, stored_keys, stored_values, used_length, out_weight):
    hbm = pl.BlockSpec(memory_space=pl.ANY)
    dma = pltpu.SemaphoreType.DMA
    return pl.pallas_call(
        kernel,
        out_shape=pltpu.VMEM((1, COLS), jnp.bfloat16),
        in_specs=[hbm] * 5,
        out_specs=pl.BlockSpec(memory_space=pltpu.VMEM),
        scratch_shapes=[
            pltpu.VMEM((SEQ, HEADS, STRETCH, HEAD), jnp.bfloat16),
            pltpu.VMEM((SEQ, HEADS, STRETCH, HEAD), jnp.bfloat16),
            pltpu.VMEM((GRP, GROUP, HEAD, COLS), jnp.bfloat16),
            pltpu.VMEM((SEQ, HEADS, GROUP, HEAD), jnp.bfloat16),
            pltpu.SMEM((SEQ,), jnp.int32),
            pltpu.VMEM((2, UNIT, ROWS, STRETCH), jnp.float32),
            pltpu.VMEM((SEQ, ROWS, HEAD), jnp.float32),
            pltpu.VMEM((KINDS * SEQ, 128), jnp.float32),
            pltpu.VMEM((SEQ, ROWS, HEAD), jnp.float32),
            pltpu.VMEM((KINDS * SEQ, 128), jnp.float32),
            pltpu.VMEM((ROWS, HEAD), jnp.float32),
            pltpu.VMEM((GRP, PAIR, COLS // 128, 128), jnp.float32),
            pltpu.VMEM((GRP * PAIR, COLS // 128, 128), jnp.float32),
            dma((2,)), dma((STEPS,)), dma((1,)),
            dma(()), dma((SEQ // PAIR,)), dma(()), dma(()), dma(()), dma(()),
            dma(()), dma(()),
        ],
        compiler_params=pltpu.CompilerParams(
            collective_id=0, has_side_effects=True, vmem_limit_bytes=60 * 1024 * 1024
        ),
        name="decode",
    )(new_queries, stored_keys, stored_values, used_length, out_weight)


def solution(mesh):
    in_specs = (
        P("seq", "group", None, None),
        P(None, "group", "seq", None),
        P(None, "group", "seq", None),
        P(),
        P("group", None, None, None),
    )
    return jax.shard_map(
        per_device, mesh=mesh, in_specs=in_specs, out_specs=P("seq", "group"), check_vma=False
    )
```

```python
import jax
import jax.numpy as jnp
from jax import lax
from jax.experimental import pallas as pl
from jax.experimental.pallas import tpu as pltpu
from jax.sharding import PartitionSpec as P

MESH = pl.DeviceIdType.MESH
SEQ, GRP = 32, 4
ROW, PAIR = 8, 2
HEADS, GROUP, HEAD = 2, 8, 128
ROWS = HEADS * GROUP
STRETCH = 512
COLS = 1280
UNIT = 4
STEPS = SEQ // UNIT
TO_EXP2 = HEAD ** (-0.5) * 1.4426950408889634


def kernel(
    q_hbm, k_hbm, v_hbm, len_hbm, w_hbm, out_ref,
    kbuf, vbuf, wbuf, qbuf, lens, logits, psend, ssend, parts, stats, rows, ysend, ybuf,
    local_sem, kv_sem, w_sem, q_send, q_recv, p_send, p_recv, s_send, s_recv, y_send, y_recv,
):
    me = lax.axis_index("seq")
    grp = lax.axis_index("group")
    core = lax.rem(me, PAIR)
    chip = me - core

    def across(i):
        return lax.rem(grp + i, GRP)

    barrier = pltpu.get_barrier_semaphore()
    for peer in range(SEQ):

        @pl.when(peer != me)
        def _():
            pl.semaphore_signal(barrier, 1, device_id={"seq": peer}, device_id_type=MESH)

    for i in range(1, GRP):
        for other in range(PAIR):
            there = {"seq": chip + other, "group": across(i)}
            pl.semaphore_signal(barrier, 1, device_id=there, device_id_type=MESH)

    q_copy = pltpu.make_async_copy(q_hbm.at[0], qbuf.at[me], local_sem.at[0])
    len_copy = pltpu.make_async_copy(len_hbm, lens, local_sem.at[1])
    q_copy.start()
    len_copy.start()

    def nth(n):
        if isinstance(n, int):
            return {3: 6, 4: 3, 5: 4, 6: 5}.get(n, n)
        return n + jnp.where(n == 3, 3, 0) + jnp.where(n == 4, -1, 0) + jnp.where(n == 5, -1, 0) + jnp.where(n == 6, -1, 0)

    def load(n):
        some = pl.ds(nth(n) * UNIT, UNIT)
        pltpu.make_async_copy(k_hbm.at[some], kbuf.at[some], kv_sem.at[n]).start(priority=1)
        pltpu.make_async_copy(v_hbm.at[some], vbuf.at[some], kv_sem.at[n]).start(priority=1)

    def loaded(n):
        both = kbuf.at[pl.ds(0, 2 * UNIT)]
        pltpu.make_async_copy(both, both, kv_sem.at[n]).wait()

    def owner_of(quarter):
        return quarter + (quarter >= grp).astype(jnp.int32) if quarter < GRP - 1 else grp

    def w_copy(quarter):
        start = pl.multiple_of(owner_of(quarter) * COLS, 128)
        return pltpu.make_async_copy(
            w_hbm.at[core, :, :, pl.ds(start, COLS)], wbuf.at[quarter], w_sem.at[0]
        )

    for n in range(STEPS):
        load(n)
    for quarter in range(GRP):
        w_copy(quarter).start(priority=1)

    def q_remote(peer):
        return pltpu.make_async_remote_copy(
            src_ref=qbuf.at[me], dst_ref=qbuf.at[me],
            send_sem=q_send, recv_sem=q_recv.at[lax.div(me, PAIR)],
            device_id={"seq": peer}, device_id_type=MESH,
        )

    def q_wait(place, count):
        some = qbuf.at[pl.ds(place * PAIR, count)]
        return pltpu.make_async_remote_copy(
            src_ref=some, dst_ref=some, send_sem=q_send, recv_sem=q_recv.at[place],
            device_id={"seq": me}, device_id_type=MESH,
        )

    q_copy.wait()
    len_copy.wait()
    pl.semaphore_wait(barrier, SEQ - 1 + PAIR * (GRP - 1))
    for z in (3, 2, 1, 0):
        for x in (2, 3, 1, 0):
            for peer in range(z * ROW + x * PAIR, z * ROW + x * PAIR + PAIR):

                @pl.when(peer != me)
                def _():
                    q_remote(peer).start()

    def arrived(place):
        own = place * PAIR == chip

        @pl.when(own)
        def _():
            q_wait(place, PAIR - 1).wait_recv()

        @pl.when(jnp.logical_not(own))
        def _():
            q_wait(place, PAIR).wait_recv()

    def scores(step, slot, units=range(UNIT)):
        lane = lax.broadcasted_iota(jnp.int32, (ROWS, STRETCH), 1) + me * STRETCH
        for u in units:
            b = step * UNIT + u
            zero = jnp.zeros((GROUP, HEAD), jnp.float32)
            q0 = qbuf[b, 0].astype(jnp.float32)
            q1 = qbuf[b, 1].astype(jnp.float32)
            q = jnp.concatenate(
                [jnp.concatenate([q0, zero], axis=1), jnp.concatenate([zero, q1], axis=1)], axis=0
            ).astype(jnp.bfloat16)
            k = jnp.concatenate([kbuf[b, 0], kbuf[b, 1]], axis=1)
            logit = lax.dot_general(
                q, k, (((1,), (1,)), ((), ())), preferred_element_type=jnp.float32
            )
            logits[slot, u] = jnp.where(lane < lens[b], logit, -1e30)

    def reads(step, slot, units=range(UNIT)):
        row = lax.broadcasted_iota(jnp.int32, (ROWS, HEAD), 0)
        lane = lax.broadcasted_iota(jnp.int32, (ROWS, HEAD), 1)
        results = []
        for u in units:
            b = step * UNIT + u
            logit = logits[slot, u]
            top = jnp.max(logit, axis=1, keepdims=True)
            part = jnp.exp2((logit - top) * TO_EXP2)
            total = jnp.sum(part, axis=1, keepdims=True)
            high = part.astype(jnp.bfloat16)
            low = (part - high.astype(jnp.float32)).astype(jnp.bfloat16)
            v = jnp.concatenate([vbuf[b, 0], vbuf[b, 1]], axis=1)
            both = jnp.dot(
                jnp.concatenate([high, low], axis=0), v, preferred_element_type=jnp.float32
            )
            results.append((both[:ROWS] + both[ROWS:], top, total))
        for n, u in enumerate(units[::PAIR]):
            for head in range(HEADS):
                own = slice(head * GROUP, (head + 1) * GROUP)
                here = slice(head * HEAD, (head + 1) * HEAD)
                two = results[n * PAIR : (n + 1) * PAIR]
                top = jnp.concatenate([r[1][own] for r in two], axis=0)
                total = jnp.concatenate([r[2][own] for r in two], axis=0)
                psend[step * UNIT + u + head] = jnp.concatenate([r[0][own, here] for r in two], axis=0)
                pair = jnp.where(lane == row, top, jnp.where(lane == row + ROWS, total, 0.0))
                ssend[pl.ds(step * UNIT + u + head, 1)] = jnp.sum(pair, axis=0, keepdims=True)

    def p_remote(b):
        return pltpu.make_async_remote_copy(
            src_ref=psend.at[b], dst_ref=parts.at[me], send_sem=p_send, recv_sem=p_recv,
            device_id={"seq": b}, device_id_type=MESH,
        )

    def s_remote(b):
        return pltpu.make_async_remote_copy(
            src_ref=ssend.at[pl.ds(b, 1)], dst_ref=stats.at[pl.ds(me, 1)], send_sem=s_send, recv_sem=s_recv,
            device_id={"seq": b}, device_id_type=MESH,
        )

    def send(step, units=range(UNIT)):
        for u in units:
            b = step * UNIT + u

            @pl.when(b != me)
            def _():
                s_remote(b).start()
                p_remote(b).start()

    head, tail = range(PAIR), range(PAIR, UNIT)
    arrived(0)
    loaded(0)
    scores(0, 0, head)
    reads(0, 0, head)
    send(0, head)
    arrived(1)
    arrived(2 * nth(1))
    arrived(2 * nth(1) + 1)
    loaded(1)
    scores(0, 0, tail)
    scores(nth(1), 1)
    reads(0, 0, tail)
    send(0, tail)

    @pl.loop(0, STEPS // 2 - 1)
    def _(i):
        n = 2 * i + 1
        now, second, third = nth(n), nth(n + 1), nth(n + 2)
        arrived(2 * second)
        arrived(2 * second + 1)
        loaded(n + 1)
        scores(second, 0)
        reads(now, 1)
        send(now)
        arrived(2 * third)
        arrived(2 * third + 1)
        loaded(n + 2)
        scores(third, 1)
        reads(second, 0)
        send(second)

    pltpu.make_async_copy(wbuf, wbuf, w_sem.at[0]).wait()
    reads(nth(STEPS - 1), 1)
    send(nth(STEPS - 1))
    parts[me] = psend[me]
    stats[pl.ds(me, 1)] = ssend[pl.ds(me, 1)]

    def all_but_one(ref, send_sem, recv_sem):
        most = ref.at[pl.ds(0, SEQ - 1)]
        return pltpu.make_async_remote_copy(
            src_ref=most, dst_ref=most, send_sem=send_sem, recv_sem=recv_sem,
            device_id={"seq": me}, device_id_type=MESH,
        )

    all_but_one(stats, s_send, s_recv).wait_recv()
    stat = stats[...]
    best = jnp.max(stat, axis=0, keepdims=True)
    scale = jnp.exp2((stat - best) * TO_EXP2)
    sums = pltpu.roll(stat, HEAD - ROWS, axis=1)
    weight = scale / jnp.sum(sums * scale, axis=0, keepdims=True)
    weight = weight.T[:ROWS]

    all_but_one(parts, p_send, p_recv).wait_recv()
    read = jnp.zeros((ROWS, HEAD), jnp.float32)
    for i in range(SEQ):
        read = read + parts[i] * weight[:, i : i + 1]
    rows[...] = read.astype(jnp.bfloat16).astype(jnp.float32)
    even = lax.broadcasted_iota(jnp.int32, (GROUP, HEAD), 0) == 0
    wide = jnp.concatenate(
        [jnp.where(even, rows[r : r + 1, :], rows[GROUP + r : GROUP + r + 1, :]) for r in range(GROUP)],
        axis=1,
    )
    spread = wide.astype(jnp.bfloat16)
    deep = GROUP * HEAD // 2
    folded = jnp.concatenate([wide[:, :deep], wide[:, deep:]], axis=0).astype(jnp.bfloat16)

    mine = grp * PAIR + core

    def y_remote(quarter, token, peer):
        return pltpu.make_async_remote_copy(
            src_ref=ysend.at[quarter, token], dst_ref=ybuf.at[mine], send_sem=y_send, recv_sem=y_recv,
            device_id={"seq": chip + token, "group": peer}, device_id_type=MESH,
        )

    def pair(quarter, start):
        w = wbuf[quarter, :, :, start : start + 512].reshape(GROUP * HEAD, 512)
        return jnp.dot(spread, w, preferred_element_type=jnp.float32)

    def single(quarter):
        w = wbuf[quarter, :, :, 1024:COLS]
        w = jnp.concatenate(
            [w[: GROUP // 2].reshape(deep, 256), w[GROUP // 2 :].reshape(deep, 256)], axis=1
        )
        both = jnp.dot(folded, w, preferred_element_type=jnp.float32)
        return both[:GROUP, :256] + both[GROUP:, 256:]

    def ship(quarter, terms):
        line = jnp.concatenate(terms, axis=1)
        for token in range(PAIR):
            for n in range(COLS // 128):
                ysend[quarter, token, n : n + 1, :] = line[token : token + 1, n * 128 : (n + 1) * 128]
        if quarter < GRP - 1:
            for token in range(PAIR):
                y_remote(quarter, token, owner_of(quarter)).start()

    ahead = pair(0, 0)
    for quarter in range(GRP):
        terms = [ahead, pair(quarter, 512), single(quarter)]
        if quarter < GRP - 1:
            ahead = pair(quarter + 1, 0)
        ship(quarter, terms)
    y_remote(GRP - 1, 1 - core, grp).start()
    ybuf[mine] = ysend[GRP - 1, core]

    def others(ref):
        most = ref.at[pl.ds(0, GRP * PAIR - 1)]
        return pltpu.make_async_remote_copy(
            src_ref=most, dst_ref=most, send_sem=y_send, recv_sem=y_recv,
            device_id={"seq": me}, device_id_type=MESH,
        )

    all_but_one(qbuf, q_send, q_recv.at[0]).wait_send()
    all_but_one(stats, s_send, s_recv).wait_send()
    all_but_one(parts, p_send, p_recv).wait_send()
    others(ybuf).wait_send()
    others(ybuf).wait_recv()
    token = ybuf[0]
    for i in range(1, GRP * PAIR):
        token = token + ybuf[i]
    for n in range(COLS // 128):
        out_ref[0:1, n * 128 : (n + 1) * 128] = token[n : n + 1, :].astype(out_ref.dtype)


def per_device(new_queries, stored_keys, stored_values, used_length, out_weight):
    hbm = pl.BlockSpec(memory_space=pl.ANY)
    dma = pltpu.SemaphoreType.DMA
    return pl.pallas_call(
        kernel,
        out_shape=pltpu.VMEM((1, COLS), jnp.bfloat16),
        in_specs=[hbm] * 5,
        out_specs=pl.BlockSpec(memory_space=pltpu.VMEM),
        scratch_shapes=[
            pltpu.VMEM((SEQ, HEADS, STRETCH, HEAD), jnp.bfloat16),
            pltpu.VMEM((SEQ, HEADS, STRETCH, HEAD), jnp.bfloat16),
            pltpu.VMEM((GRP, GROUP, HEAD, COLS), jnp.bfloat16),
            pltpu.VMEM((SEQ, HEADS, GROUP, HEAD), jnp.bfloat16),
            pltpu.SMEM((SEQ,), jnp.int32),
            pltpu.VMEM((2, UNIT, ROWS, STRETCH), jnp.float32),
            pltpu.VMEM((SEQ, ROWS, HEAD), jnp.float32),
            pltpu.VMEM((SEQ, 128), jnp.float32),
            pltpu.VMEM((SEQ, ROWS, HEAD), jnp.float32),
            pltpu.VMEM((SEQ, 128), jnp.float32),
            pltpu.VMEM((ROWS, HEAD), jnp.float32),
            pltpu.VMEM((GRP, PAIR, COLS // 128, 128), jnp.float32),
            pltpu.VMEM((GRP * PAIR, COLS // 128, 128), jnp.float32),
            dma((2,)), dma((STEPS,)), dma((1,)),
            dma(()), dma((SEQ // PAIR,)), dma(()), dma(()), dma(()), dma(()),
            dma(()), dma(()),
        ],
        compiler_params=pltpu.CompilerParams(
            collective_id=0, has_side_effects=True, vmem_limit_bytes=60 * 1024 * 1024
        ),
        name="decode",
    )(new_queries, stored_keys, stored_values, used_length, out_weight)


def solution(mesh):
    in_specs = (
        P("seq", "group", None, None),
        P(None, "group", "seq", None),
        P(None, "group", "seq", None),
        P(),
        P("group", None, None, None),
    )
    return jax.shard_map(
        per_device, mesh=mesh, in_specs=in_specs, out_specs=P("seq", "group"), check_vma=False
    )
```

```python
import jax
import jax.numpy as jnp
from jax import lax
from jax.experimental import pallas as pl
from jax.experimental.pallas import tpu as pltpu
from jax.sharding import PartitionSpec as P

MESH = pl.DeviceIdType.MESH
SEQ, GRP = 32, 4
ROW, PAIR = 8, 2
HEADS, GROUP, HEAD = 2, 8, 128
ROWS = HEADS * GROUP
STRETCH = 512
COLS = 1280
UNIT = 4
STEPS = SEQ // UNIT
TO_EXP2 = HEAD ** (-0.5) * 1.4426950408889634


def kernel(
    q_hbm, k_hbm, v_hbm, len_hbm, w_hbm, out_ref,
    kbuf, vbuf, wbuf, qbuf, lens, logits, psend, ssend, parts, stats, rows, ysend, ybuf,
    local_sem, kv_sem, w_sem, q_send, q_recv, p_send, p_recv, s_send, s_recv, y_send, y_recv,
):
    me = lax.axis_index("seq")
    grp = lax.axis_index("group")
    core = lax.rem(me, PAIR)
    chip = me - core

    def across(i):
        return lax.rem(grp + i, GRP)

    barrier = pltpu.get_barrier_semaphore()
    for peer in range(SEQ):

        @pl.when(peer != me)
        def _():
            pl.semaphore_signal(barrier, 1, device_id={"seq": peer}, device_id_type=MESH)

    for i in range(1, GRP):
        for other in range(PAIR):
            there = {"seq": chip + other, "group": across(i)}
            pl.semaphore_signal(barrier, 1, device_id=there, device_id_type=MESH)

    q_copy = pltpu.make_async_copy(q_hbm.at[0], qbuf.at[me], local_sem.at[0])
    len_copy = pltpu.make_async_copy(len_hbm, lens, local_sem.at[1])
    q_copy.start()
    len_copy.start()

    def nth(n):
        if isinstance(n, int):
            return {3: 6, 4: 3, 5: 4, 6: 5}.get(n, n)
        return n + jnp.where(n == 3, 3, 0) + jnp.where(n == 4, -1, 0) + jnp.where(n == 5, -1, 0) + jnp.where(n == 6, -1, 0)

    def load(n):
        some = pl.ds(nth(n) * UNIT, UNIT)
        pltpu.make_async_copy(k_hbm.at[some], kbuf.at[some], kv_sem.at[n]).start(priority=1)
        pltpu.make_async_copy(v_hbm.at[some], vbuf.at[some], kv_sem.at[n]).start(priority=1)

    def loaded(n):
        both = kbuf.at[pl.ds(0, 2 * UNIT)]
        pltpu.make_async_copy(both, both, kv_sem.at[n]).wait()

    def owner_of(quarter):
        return quarter + (quarter >= grp).astype(jnp.int32) if quarter < GRP - 1 else grp

    def w_copy(quarter):
        start = pl.multiple_of(owner_of(quarter) * COLS, 128)
        return pltpu.make_async_copy(
            w_hbm.at[core, :, :, pl.ds(start, COLS)], wbuf.at[quarter], w_sem.at[0]
        )

    for n in range(STEPS):
        load(n)
    for quarter in range(GRP):
        w_copy(quarter).start(priority=1)

    def q_remote(peer):
        return pltpu.make_async_remote_copy(
            src_ref=qbuf.at[me], dst_ref=qbuf.at[me],
            send_sem=q_send, recv_sem=q_recv.at[lax.div(me, PAIR)],
            device_id={"seq": peer}, device_id_type=MESH,
        )

    def q_wait(place, count):
        some = qbuf.at[pl.ds(place * PAIR, count)]
        return pltpu.make_async_remote_copy(
            src_ref=some, dst_ref=some, send_sem=q_send, recv_sem=q_recv.at[place],
            device_id={"seq": me}, device_id_type=MESH,
        )

    q_copy.wait()
    len_copy.wait()
    pl.semaphore_wait(barrier, SEQ - 1 + PAIR * (GRP - 1))
    for z in (3, 2, 1, 0):
        for x in (2, 3, 1, 0):
            for peer in range(z * ROW + x * PAIR, z * ROW + x * PAIR + PAIR):

                @pl.when(peer != me)
                def _():
                    q_remote(peer).start()

    def arrived(place):
        own = place * PAIR == chip

        @pl.when(own)
        def _():
            q_wait(place, PAIR - 1).wait_recv()

        @pl.when(jnp.logical_not(own))
        def _():
            q_wait(place, PAIR).wait_recv()

    def scores(step, slot, units=range(UNIT)):
        lane = lax.broadcasted_iota(jnp.int32, (ROWS, STRETCH), 1) + me * STRETCH
        for u in units:
            b = step * UNIT + u
            zero = jnp.zeros((GROUP, HEAD), jnp.float32)
            q0 = qbuf[b, 0].astype(jnp.float32)
            q1 = qbuf[b, 1].astype(jnp.float32)
            q = jnp.concatenate(
                [jnp.concatenate([q0, zero], axis=1), jnp.concatenate([zero, q1], axis=1)], axis=0
            ).astype(jnp.bfloat16)
            k = jnp.concatenate([kbuf[b, 0], kbuf[b, 1]], axis=1)
            logit = lax.dot_general(
                q, k, (((1,), (1,)), ((), ())), preferred_element_type=jnp.float32
            )
            logits[slot, u] = jnp.where(lane < lens[b], logit, -1e30)

    def reads(step, slot, units=range(UNIT)):
        row = lax.broadcasted_iota(jnp.int32, (ROWS, HEAD), 0)
        lane = lax.broadcasted_iota(jnp.int32, (ROWS, HEAD), 1)
        results = []
        for u in units:
            b = step * UNIT + u
            logit = logits[slot, u]
            top = jnp.max(logit, axis=1, keepdims=True)
            part = jnp.exp2((logit - top) * TO_EXP2)
            total = jnp.sum(part, axis=1, keepdims=True)
            high = part.astype(jnp.bfloat16)
            low = (part - high.astype(jnp.float32)).astype(jnp.bfloat16)
            v = jnp.concatenate([vbuf[b, 0], vbuf[b, 1]], axis=1)
            both = jnp.dot(
                jnp.concatenate([high, low], axis=0), v, preferred_element_type=jnp.float32
            )
            results.append((both[:ROWS] + both[ROWS:], top, total))
        for n, u in enumerate(units[::PAIR]):
            for head in range(HEADS):
                own = slice(head * GROUP, (head + 1) * GROUP)
                here = slice(head * HEAD, (head + 1) * HEAD)
                two = results[n * PAIR : (n + 1) * PAIR]
                top = jnp.concatenate([r[1][own] for r in two], axis=0)
                total = jnp.concatenate([r[2][own] for r in two], axis=0)
                psend[step * UNIT + u + head] = jnp.concatenate([r[0][own, here] for r in two], axis=0)
                pair = jnp.where(lane == row, top, jnp.where(lane == row + ROWS, total, 0.0))
                ssend[pl.ds(step * UNIT + u + head, 1)] = jnp.sum(pair, axis=0, keepdims=True)

    def p_remote(b):
        return pltpu.make_async_remote_copy(
            src_ref=psend.at[b], dst_ref=parts.at[me], send_sem=p_send, recv_sem=p_recv,
            device_id={"seq": b}, device_id_type=MESH,
        )

    def s_remote(b):
        return pltpu.make_async_remote_copy(
            src_ref=ssend.at[pl.ds(b, 1)], dst_ref=stats.at[pl.ds(me, 1)], send_sem=s_send, recv_sem=s_recv,
            device_id={"seq": b}, device_id_type=MESH,
        )

    def send(step, units=range(UNIT)):
        for u in units:
            b = step * UNIT + u

            @pl.when(b != me)
            def _():
                s_remote(b).start()
                p_remote(b).start()

    head, tail = range(PAIR), range(PAIR, UNIT)
    arrived(0)
    loaded(0)
    scores(0, 0, head)
    reads(0, 0, head)
    send(0, head)
    arrived(1)
    arrived(2 * nth(1))
    arrived(2 * nth(1) + 1)
    loaded(1)
    scores(0, 0, tail)
    scores(nth(1), 1)
    reads(0, 0, tail)
    send(0, tail)

    @pl.loop(0, STEPS // 2 - 1)
    def _(i):
        n = 2 * i + 1
        now, second, third = nth(n), nth(n + 1), nth(n + 2)
        for step in (second, third):
            arrived(2 * step)
            arrived(2 * step + 1)
        loaded(n + 1)
        loaded(n + 2)
        scores(second, 0)
        reads(now, 1)
        send(now)
        scores(third, 1)
        reads(second, 0)
        send(second)

    pltpu.make_async_copy(wbuf, wbuf, w_sem.at[0]).wait()
    for units in (head, tail):
        reads(nth(STEPS - 1), 1, units)
        send(nth(STEPS - 1), units)
    parts[me] = psend[me]
    stats[pl.ds(me, 1)] = ssend[pl.ds(me, 1)]

    def all_but_one(ref, send_sem, recv_sem):
        most = ref.at[pl.ds(0, SEQ - 1)]
        return pltpu.make_async_remote_copy(
            src_ref=most, dst_ref=most, send_sem=send_sem, recv_sem=recv_sem,
            device_id={"seq": me}, device_id_type=MESH,
        )

    all_but_one(stats, s_send, s_recv).wait_recv()
    stat = stats[...]
    best = jnp.max(stat, axis=0, keepdims=True)
    scale = jnp.exp2((stat - best) * TO_EXP2)
    sums = pltpu.roll(stat, HEAD - ROWS, axis=1)
    weight = scale / jnp.sum(sums * scale, axis=0, keepdims=True)
    weight = weight.T[:ROWS]

    all_but_one(parts, p_send, p_recv).wait_recv()
    read = jnp.zeros((ROWS, HEAD), jnp.float32)
    for i in range(SEQ):
        read = read + parts[i] * weight[:, i : i + 1]
    rows[...] = read.astype(jnp.bfloat16).astype(jnp.float32)
    even = lax.broadcasted_iota(jnp.int32, (GROUP, HEAD), 0) == 0
    wide = jnp.concatenate(
        [jnp.where(even, rows[r : r + 1, :], rows[GROUP + r : GROUP + r + 1, :]) for r in range(GROUP)],
        axis=1,
    )
    spread = wide.astype(jnp.bfloat16)
    deep = GROUP * HEAD // 2
    folded = jnp.concatenate([wide[:, :deep], wide[:, deep:]], axis=0).astype(jnp.bfloat16)

    mine = grp * PAIR + core

    def y_remote(quarter, token, peer):
        return pltpu.make_async_remote_copy(
            src_ref=ysend.at[quarter, token], dst_ref=ybuf.at[mine], send_sem=y_send, recv_sem=y_recv,
            device_id={"seq": chip + token, "group": peer}, device_id_type=MESH,
        )

    def pair(quarter, start):
        w = wbuf[quarter, :, :, start : start + 512].reshape(GROUP * HEAD, 512)
        return jnp.dot(spread, w, preferred_element_type=jnp.float32)

    def single(quarter):
        w = wbuf[quarter, :, :, 1024:COLS]
        w = jnp.concatenate(
            [w[: GROUP // 2].reshape(deep, 256), w[GROUP // 2 :].reshape(deep, 256)], axis=1
        )
        both = jnp.dot(folded, w, preferred_element_type=jnp.float32)
        return both[:GROUP, :256] + both[GROUP:, 256:]

    def ship(quarter, terms):
        line = jnp.concatenate(terms, axis=1)
        for token in range(PAIR):
            for n in range(COLS // 128):
                ysend[quarter, token, n : n + 1, :] = line[token : token + 1, n * 128 : (n + 1) * 128]
        if quarter < GRP - 1:
            for token in range(PAIR):
                y_remote(quarter, token, owner_of(quarter)).start()

    ahead = pair(0, 0)
    for quarter in range(GRP):
        terms = [ahead, pair(quarter, 512), single(quarter)]
        if quarter < GRP - 1:
            ahead = pair(quarter + 1, 0)
        ship(quarter, terms)
    y_remote(GRP - 1, 1 - core, grp).start()
    ybuf[mine] = ysend[GRP - 1, core]

    def others(ref):
        most = ref.at[pl.ds(0, GRP * PAIR - 1)]
        return pltpu.make_async_remote_copy(
            src_ref=most, dst_ref=most, send_sem=y_send, recv_sem=y_recv,
            device_id={"seq": me}, device_id_type=MESH,
        )

    all_but_one(qbuf, q_send, q_recv.at[0]).wait_send()
    all_but_one(stats, s_send, s_recv).wait_send()
    all_but_one(parts, p_send, p_recv).wait_send()
    others(ybuf).wait_send()
    others(ybuf).wait_recv()
    token = ybuf[0]
    for i in range(1, GRP * PAIR):
        token = token + ybuf[i]
    for n in range(COLS // 128):
        out_ref[0:1, n * 128 : (n + 1) * 128] = token[n : n + 1, :].astype(out_ref.dtype)


def per_device(new_queries, stored_keys, stored_values, used_length, out_weight):
    hbm = pl.BlockSpec(memory_space=pl.ANY)
    dma = pltpu.SemaphoreType.DMA
    return pl.pallas_call(
        kernel,
        out_shape=pltpu.VMEM((1, COLS), jnp.bfloat16),
        in_specs=[hbm] * 5,
        out_specs=pl.BlockSpec(memory_space=pltpu.VMEM),
        scratch_shapes=[
            pltpu.VMEM((SEQ, HEADS, STRETCH, HEAD), jnp.bfloat16),
            pltpu.VMEM((SEQ, HEADS, STRETCH, HEAD), jnp.bfloat16),
            pltpu.VMEM((GRP, GROUP, HEAD, COLS), jnp.bfloat16),
            pltpu.VMEM((SEQ, HEADS, GROUP, HEAD), jnp.bfloat16),
            pltpu.SMEM((SEQ,), jnp.int32),
            pltpu.VMEM((2, UNIT, ROWS, STRETCH), jnp.float32),
            pltpu.VMEM((SEQ, ROWS, HEAD), jnp.float32),
            pltpu.VMEM((SEQ, 128), jnp.float32),
            pltpu.VMEM((SEQ, ROWS, HEAD), jnp.float32),
            pltpu.VMEM((SEQ, 128), jnp.float32),
            pltpu.VMEM((ROWS, HEAD), jnp.float32),
            pltpu.VMEM((GRP, PAIR, COLS // 128, 128), jnp.float32),
            pltpu.VMEM((GRP * PAIR, COLS // 128, 128), jnp.float32),
            dma((2,)), dma((STEPS,)), dma((1,)),
            dma(()), dma((SEQ // PAIR,)), dma(()), dma(()), dma(()), dma(()),
            dma(()), dma(()),
        ],
        compiler_params=pltpu.CompilerParams(
            collective_id=0, has_side_effects=True, vmem_limit_bytes=60 * 1024 * 1024
        ),
        name="decode",
    )(new_queries, stored_keys, stored_values, used_length, out_weight)


def solution(mesh):
    in_specs = (
        P("seq", "group", None, None),
        P(None, "group", "seq", None),
        P(None, "group", "seq", None),
        P(),
        P("group", None, None, None),
    )
    return jax.shard_map(
        per_device, mesh=mesh, in_specs=in_specs, out_specs=P("seq", "group"), check_vma=False
    )
```

```python
import jax
import jax.numpy as jnp
from jax import lax
from jax.experimental import pallas as pl
from jax.experimental.pallas import tpu as pltpu
from jax.sharding import PartitionSpec as P

MESH = pl.DeviceIdType.MESH
SEQ, GRP = 32, 4
ROW, PAIR = 8, 2
HEADS, GROUP, HEAD = 2, 8, 128
ROWS = HEADS * GROUP
STRETCH = 512
COLS = 1280
UNIT = 4
STEPS = SEQ // UNIT
TO_EXP2 = HEAD ** (-0.5) * 1.4426950408889634


def kernel(
    q_hbm, k_hbm, v_hbm, len_hbm, w_hbm, out_ref,
    kbuf, vbuf, wbuf, qbuf, lens, logits, psend, ssend, parts, stats, rows, ysend, ybuf,
    local_sem, kv_sem, w_sem, q_send, q_recv, p_send, p_recv, s_send, s_recv, y_send, y_recv,
):
    me = lax.axis_index("seq")
    grp = lax.axis_index("group")
    core = lax.rem(me, PAIR)
    chip = me - core

    def across(i):
        return lax.rem(grp + i, GRP)

    barrier = pltpu.get_barrier_semaphore()
    for peer in range(SEQ):

        @pl.when(peer != me)
        def _():
            pl.semaphore_signal(barrier, 1, device_id={"seq": peer}, device_id_type=MESH)

    for i in range(1, GRP):
        for other in range(PAIR):
            there = {"seq": chip + other, "group": across(i)}
            pl.semaphore_signal(barrier, 1, device_id=there, device_id_type=MESH)

    q_copy = pltpu.make_async_copy(q_hbm.at[0], qbuf.at[me], local_sem.at[0])
    len_copy = pltpu.make_async_copy(len_hbm, lens, local_sem.at[1])
    q_copy.start()
    len_copy.start()

    def nth(n):
        if isinstance(n, int):
            return {3: 6, 4: 3, 5: 4, 6: 5}.get(n, n)
        return n + jnp.where(n == 3, 3, 0) + jnp.where(n == 4, -1, 0) + jnp.where(n == 5, -1, 0) + jnp.where(n == 6, -1, 0)

    def load(n):
        some = pl.ds(nth(n) * UNIT, UNIT)
        pltpu.make_async_copy(k_hbm.at[some], kbuf.at[some], kv_sem.at[n]).start(priority=1)
        pltpu.make_async_copy(v_hbm.at[some], vbuf.at[some], kv_sem.at[n]).start(priority=1)

    def loaded(n):
        both = kbuf.at[pl.ds(0, 2 * UNIT)]
        pltpu.make_async_copy(both, both, kv_sem.at[n]).wait()

    def owner_of(quarter):
        return quarter + (quarter >= grp).astype(jnp.int32) if quarter < GRP - 1 else grp

    def w_copy(quarter):
        start = pl.multiple_of(owner_of(quarter) * COLS, 128)
        return pltpu.make_async_copy(
            w_hbm.at[core, :, :, pl.ds(start, COLS)], wbuf.at[quarter], w_sem.at[0]
        )

    for n in range(STEPS):
        load(n)
    for quarter in range(GRP):
        w_copy(quarter).start(priority=1)

    def q_remote(peer):
        return pltpu.make_async_remote_copy(
            src_ref=qbuf.at[me], dst_ref=qbuf.at[me],
            send_sem=q_send, recv_sem=q_recv.at[lax.div(me, PAIR)],
            device_id={"seq": peer}, device_id_type=MESH,
        )

    def q_wait(place, count):
        some = qbuf.at[pl.ds(place * PAIR, count)]
        return pltpu.make_async_remote_copy(
            src_ref=some, dst_ref=some, send_sem=q_send, recv_sem=q_recv.at[place],
            device_id={"seq": me}, device_id_type=MESH,
        )

    q_copy.wait()
    len_copy.wait()
    pl.semaphore_wait(barrier, SEQ - 1 + PAIR * (GRP - 1))
    for z in (3, 2, 1, 0):
        for x in (2, 3, 1, 0):
            for peer in range(z * ROW + x * PAIR, z * ROW + x * PAIR + PAIR):

                @pl.when(peer != me)
                def _():
                    q_remote(peer).start()

    def arrived(place):
        own = place * PAIR == chip

        @pl.when(own)
        def _():
            q_wait(place, PAIR - 1).wait_recv()

        @pl.when(jnp.logical_not(own))
        def _():
            q_wait(place, PAIR).wait_recv()

    def scores(step, slot, units=range(UNIT)):
        lane = lax.broadcasted_iota(jnp.int32, (ROWS, STRETCH), 1) + me * STRETCH
        for u in units:
            b = step * UNIT + u
            zero = jnp.zeros((GROUP, HEAD), jnp.float32)
            q0 = qbuf[b, 0].astype(jnp.float32)
            q1 = qbuf[b, 1].astype(jnp.float32)
            q = jnp.concatenate(
                [jnp.concatenate([q0, zero], axis=1), jnp.concatenate([zero, q1], axis=1)], axis=0
            ).astype(jnp.bfloat16)
            k = jnp.concatenate([kbuf[b, 0], kbuf[b, 1]], axis=1)
            logit = lax.dot_general(
                q, k, (((1,), (1,)), ((), ())), preferred_element_type=jnp.float32
            )
            logits[slot, u] = jnp.where(lane < lens[b], logit, -1e30)

    def reads(step, slot, units=range(UNIT)):
        row = lax.broadcasted_iota(jnp.int32, (ROWS, HEAD), 0)
        lane = lax.broadcasted_iota(jnp.int32, (ROWS, HEAD), 1)
        results = []
        for u in units:
            b = step * UNIT + u
            logit = logits[slot, u]
            top = jnp.max(logit, axis=1, keepdims=True)
            part = jnp.exp2((logit - top) * TO_EXP2)
            total = jnp.sum(part, axis=1, keepdims=True)
            high = part.astype(jnp.bfloat16)
            low = (part - high.astype(jnp.float32)).astype(jnp.bfloat16)
            v = jnp.concatenate([vbuf[b, 0], vbuf[b, 1]], axis=1)
            both = jnp.dot(
                jnp.concatenate([high, low], axis=0), v, preferred_element_type=jnp.float32
            )
            results.append((both[:ROWS] + both[ROWS:], top, total))
        for n, u in enumerate(units[::PAIR]):
            for head in range(HEADS):
                own = slice(head * GROUP, (head + 1) * GROUP)
                here = slice(head * HEAD, (head + 1) * HEAD)
                two = results[n * PAIR : (n + 1) * PAIR]
                top = jnp.concatenate([r[1][own] for r in two], axis=0)
                total = jnp.concatenate([r[2][own] for r in two], axis=0)
                psend[step * UNIT + u + head] = jnp.concatenate([r[0][own, here] for r in two], axis=0)
                pair = jnp.where(lane == row, top, jnp.where(lane == row + ROWS, total, 0.0))
                ssend[pl.ds(step * UNIT + u + head, 1)] = jnp.sum(pair, axis=0, keepdims=True)

    def p_remote(b):
        return pltpu.make_async_remote_copy(
            src_ref=psend.at[b], dst_ref=parts.at[me], send_sem=p_send, recv_sem=p_recv,
            device_id={"seq": b}, device_id_type=MESH,
        )

    def s_remote(b):
        return pltpu.make_async_remote_copy(
            src_ref=ssend.at[pl.ds(b, 1)], dst_ref=stats.at[pl.ds(me, 1)], send_sem=s_send, recv_sem=s_recv,
            device_id={"seq": b}, device_id_type=MESH,
        )

    def send(step, units=range(UNIT)):
        for u in units:
            b = step * UNIT + u

            @pl.when(b != me)
            def _():
                p_remote(b).start()
                s_remote(b).start()

    head, tail = range(PAIR), range(PAIR, UNIT)
    arrived(0)
    loaded(0)
    scores(0, 0, head)
    reads(0, 0, head)
    send(0, head)
    arrived(1)
    arrived(2 * nth(1))
    arrived(2 * nth(1) + 1)
    loaded(1)
    scores(0, 0, tail)
    scores(nth(1), 1)
    reads(0, 0, tail)
    send(0, tail)

    @pl.loop(0, STEPS // 2 - 1)
    def _(i):
        n = 2 * i + 1
        now, second, third = nth(n), nth(n + 1), nth(n + 2)
        for step in (second, third):
            arrived(2 * step)
            arrived(2 * step + 1)
        loaded(n + 1)
        loaded(n + 2)
        scores(second, 0)
        reads(now, 1)
        send(now)
        scores(third, 1)
        reads(second, 0)
        send(second)

    pltpu.make_async_copy(wbuf, wbuf, w_sem.at[0]).wait()
    reads(nth(STEPS - 1), 1)
    send(nth(STEPS - 1))
    parts[me] = psend[me]
    stats[pl.ds(me, 1)] = ssend[pl.ds(me, 1)]

    def all_but_one(ref, send_sem, recv_sem):
        most = ref.at[pl.ds(0, SEQ - 1)]
        return pltpu.make_async_remote_copy(
            src_ref=most, dst_ref=most, send_sem=send_sem, recv_sem=recv_sem,
            device_id={"seq": me}, device_id_type=MESH,
        )

    all_but_one(stats, s_send, s_recv).wait_recv()
    stat = stats[...]
    best = jnp.max(stat, axis=0, keepdims=True)
    scale = jnp.exp2((stat - best) * TO_EXP2)
    sums = pltpu.roll(stat, HEAD - ROWS, axis=1)
    weight = scale / jnp.sum(sums * scale, axis=0, keepdims=True)
    weight = weight.T[:ROWS]

    all_but_one(parts, p_send, p_recv).wait_recv()
    read = jnp.zeros((ROWS, HEAD), jnp.float32)
    for i in range(SEQ):
        read = read + parts[i] * weight[:, i : i + 1]
    rows[...] = read.astype(jnp.bfloat16).astype(jnp.float32)
    even = lax.broadcasted_iota(jnp.int32, (GROUP, HEAD), 0) == 0
    wide = jnp.concatenate(
        [jnp.where(even, rows[r : r + 1, :], rows[GROUP + r : GROUP + r + 1, :]) for r in range(GROUP)],
        axis=1,
    )
    spread = wide.astype(jnp.bfloat16)
    deep = GROUP * HEAD // 2
    folded = jnp.concatenate([wide[:, :deep], wide[:, deep:]], axis=0).astype(jnp.bfloat16)

    mine = grp * PAIR + core

    def y_remote(quarter, token, peer):
        return pltpu.make_async_remote_copy(
            src_ref=ysend.at[quarter, token], dst_ref=ybuf.at[mine], send_sem=y_send, recv_sem=y_recv,
            device_id={"seq": chip + token, "group": peer}, device_id_type=MESH,
        )

    def pair(quarter, start):
        w = wbuf[quarter, :, :, start : start + 512].reshape(GROUP * HEAD, 512)
        return jnp.dot(spread, w, preferred_element_type=jnp.float32)

    def single(quarter):
        w = wbuf[quarter, :, :, 1024:COLS]
        w = jnp.concatenate(
            [w[: GROUP // 2].reshape(deep, 256), w[GROUP // 2 :].reshape(deep, 256)], axis=1
        )
        both = jnp.dot(folded, w, preferred_element_type=jnp.float32)
        return both[:GROUP, :256] + both[GROUP:, 256:]

    def ship(quarter, terms):
        line = jnp.concatenate(terms, axis=1)
        for token in range(PAIR):
            for n in range(COLS // 128):
                ysend[quarter, token, n : n + 1, :] = line[token : token + 1, n * 128 : (n + 1) * 128]
        if quarter < GRP - 1:
            for token in range(PAIR):
                y_remote(quarter, token, owner_of(quarter)).start()

    ahead = pair(0, 0)
    for quarter in range(GRP):
        terms = [ahead, pair(quarter, 512), single(quarter)]
        if quarter < GRP - 1:
            ahead = pair(quarter + 1, 0)
        ship(quarter, terms)
    y_remote(GRP - 1, 1 - core, grp).start()
    ybuf[mine] = ysend[GRP - 1, core]

    def others(ref):
        most = ref.at[pl.ds(0, GRP * PAIR - 1)]
        return pltpu.make_async_remote_copy(
            src_ref=most, dst_ref=most, send_sem=y_send, recv_sem=y_recv,
            device_id={"seq": me}, device_id_type=MESH,
        )

    all_but_one(qbuf, q_send, q_recv.at[0]).wait_send()
    all_but_one(stats, s_send, s_recv).wait_send()
    all_but_one(parts, p_send, p_recv).wait_send()
    others(ybuf).wait_send()
    others(ybuf).wait_recv()
    token = ybuf[0]
    for i in range(1, GRP * PAIR):
        token = token + ybuf[i]
    for n in range(COLS // 128):
        out_ref[0:1, n * 128 : (n + 1) * 128] = token[n : n + 1, :].astype(out_ref.dtype)


def per_device(new_queries, stored_keys, stored_values, used_length, out_weight):
    hbm = pl.BlockSpec(memory_space=pl.ANY)
    dma = pltpu.SemaphoreType.DMA
    return pl.pallas_call(
        kernel,
        out_shape=pltpu.VMEM((1, COLS), jnp.bfloat16),
        in_specs=[hbm] * 5,
        out_specs=pl.BlockSpec(memory_space=pltpu.VMEM),
        scratch_shapes=[
            pltpu.VMEM((SEQ, HEADS, STRETCH, HEAD), jnp.bfloat16),
            pltpu.VMEM((SEQ, HEADS, STRETCH, HEAD), jnp.bfloat16),
            pltpu.VMEM((GRP, GROUP, HEAD, COLS), jnp.bfloat16),
            pltpu.VMEM((SEQ, HEADS, GROUP, HEAD), jnp.bfloat16),
            pltpu.SMEM((SEQ,), jnp.int32),
            pltpu.VMEM((2, UNIT, ROWS, STRETCH), jnp.float32),
            pltpu.VMEM((SEQ, ROWS, HEAD), jnp.float32),
            pltpu.VMEM((SEQ, 128), jnp.float32),
            pltpu.VMEM((SEQ, ROWS, HEAD), jnp.float32),
            pltpu.VMEM((SEQ, 128), jnp.float32),
            pltpu.VMEM((ROWS, HEAD), jnp.float32),
            pltpu.VMEM((GRP, PAIR, COLS // 128, 128), jnp.float32),
            pltpu.VMEM((GRP * PAIR, COLS // 128, 128), jnp.float32),
            dma((2,)), dma((STEPS,)), dma((1,)),
            dma(()), dma((SEQ // PAIR,)), dma(()), dma(()), dma(()), dma(()),
            dma(()), dma(()),
        ],
        compiler_params=pltpu.CompilerParams(
            collective_id=0, has_side_effects=True, vmem_limit_bytes=60 * 1024 * 1024
        ),
        name="decode",
    )(new_queries, stored_keys, stored_values, used_length, out_weight)


def solution(mesh):
    in_specs = (
        P("seq", "group", None, None),
        P(None, "group", "seq", None),
        P(None, "group", "seq", None),
        P(),
        P("group", None, None, None),
    )
    return jax.shard_map(
        per_device, mesh=mesh, in_specs=in_specs, out_specs=P("seq", "group"), check_vma=False
    )
```

```python
import jax
import jax.numpy as jnp
from jax import lax
from jax.experimental import pallas as pl
from jax.experimental.pallas import tpu as pltpu
from jax.sharding import PartitionSpec as P

MESH = pl.DeviceIdType.MESH
SEQ, GRP = 32, 4
ROW, PAIR = 8, 2
HEADS, GROUP, HEAD = 2, 8, 128
ROWS = HEADS * GROUP
STRETCH = 512
COLS = 1280
UNIT = 4
STEPS = SEQ // UNIT
TO_EXP2 = HEAD ** (-0.5) * 1.4426950408889634


def kernel(
    q_hbm, k_hbm, v_hbm, len_hbm, w_hbm, out_ref,
    kbuf, vbuf, wbuf, qbuf, lens, logits, psend, ssend, parts, stats, rows, ysend, ybuf,
    local_sem, kv_sem, w_sem, q_send, q_recv, p_send, p_recv, s_send, s_recv, y_send, y_recv,
):
    me = lax.axis_index("seq")
    grp = lax.axis_index("group")
    core = lax.rem(me, PAIR)
    chip = me - core

    def across(i):
        return lax.rem(grp + i, GRP)

    barrier = pltpu.get_barrier_semaphore()
    for peer in range(SEQ):

        @pl.when(peer != me)
        def _():
            pl.semaphore_signal(barrier, 1, device_id={"seq": peer}, device_id_type=MESH)

    for i in range(1, GRP):
        for other in range(PAIR):
            there = {"seq": chip + other, "group": across(i)}
            pl.semaphore_signal(barrier, 1, device_id=there, device_id_type=MESH)

    q_copy = pltpu.make_async_copy(q_hbm.at[0], qbuf.at[me], local_sem.at[0])
    len_copy = pltpu.make_async_copy(len_hbm, lens, local_sem.at[1])
    q_copy.start()
    len_copy.start()

    def nth(n):
        if isinstance(n, int):
            return {3: 6, 4: 3, 5: 4, 6: 5}.get(n, n)
        return n + jnp.where(n == 3, 3, 0) + jnp.where(n == 4, -1, 0) + jnp.where(n == 5, -1, 0) + jnp.where(n == 6, -1, 0)

    def load(n):
        some = pl.ds(nth(n) * UNIT, UNIT)
        pltpu.make_async_copy(k_hbm.at[some], kbuf.at[some], kv_sem.at[n]).start(priority=1)
        pltpu.make_async_copy(v_hbm.at[some], vbuf.at[some], kv_sem.at[n]).start(priority=1)

    def loaded(n):
        both = kbuf.at[pl.ds(0, 2 * UNIT)]
        pltpu.make_async_copy(both, both, kv_sem.at[n]).wait()

    def owner_of(quarter):
        return quarter + (quarter >= grp).astype(jnp.int32) if quarter < GRP - 1 else grp

    def w_copy(quarter):
        start = pl.multiple_of(owner_of(quarter) * COLS, 128)
        return pltpu.make_async_copy(
            w_hbm.at[core, :, :, pl.ds(start, COLS)], wbuf.at[quarter], w_sem.at[0]
        )

    for n in range(STEPS):
        load(n)
    for quarter in range(GRP):
        w_copy(quarter).start(priority=1)

    def q_remote(peer):
        return pltpu.make_async_remote_copy(
            src_ref=qbuf.at[me], dst_ref=qbuf.at[me],
            send_sem=q_send, recv_sem=q_recv.at[lax.div(me, PAIR)],
            device_id={"seq": peer}, device_id_type=MESH,
        )

    def q_wait(place, count):
        some = qbuf.at[pl.ds(place * PAIR, count)]
        return pltpu.make_async_remote_copy(
            src_ref=some, dst_ref=some, send_sem=q_send, recv_sem=q_recv.at[place],
            device_id={"seq": me}, device_id_type=MESH,
        )

    q_copy.wait()
    len_copy.wait()
    pl.semaphore_wait(barrier, SEQ - 1 + PAIR * (GRP - 1))
    for z in (3, 1, 2, 0):
        for x in (2, 3, 1, 0):
            for peer in range(z * ROW + x * PAIR, z * ROW + x * PAIR + PAIR):

                @pl.when(peer != me)
                def _():
                    q_remote(peer).start()

    def arrived(place):
        own = place * PAIR == chip

        @pl.when(own)
        def _():
            q_wait(place, PAIR - 1).wait_recv()

        @pl.when(jnp.logical_not(own))
        def _():
            q_wait(place, PAIR).wait_recv()

    def scores(step, slot, units=range(UNIT)):
        lane = lax.broadcasted_iota(jnp.int32, (ROWS, STRETCH), 1) + me * STRETCH
        for u in units:
            b = step * UNIT + u
            zero = jnp.zeros((GROUP, HEAD), jnp.float32)
            q0 = qbuf[b, 0].astype(jnp.float32)
            q1 = qbuf[b, 1].astype(jnp.float32)
            q = jnp.concatenate(
                [jnp.concatenate([q0, zero], axis=1), jnp.concatenate([zero, q1], axis=1)], axis=0
            ).astype(jnp.bfloat16)
            k = jnp.concatenate([kbuf[b, 0], kbuf[b, 1]], axis=1)
            logit = lax.dot_general(
                q, k, (((1,), (1,)), ((), ())), preferred_element_type=jnp.float32
            )
            logits[slot, u] = jnp.where(lane < lens[b], logit, -1e30)

    def reads(step, slot, units=range(UNIT)):
        row = lax.broadcasted_iota(jnp.int32, (ROWS, HEAD), 0)
        lane = lax.broadcasted_iota(jnp.int32, (ROWS, HEAD), 1)
        results = []
        for u in units:
            b = step * UNIT + u
            logit = logits[slot, u]
            top = jnp.max(logit, axis=1, keepdims=True)
            part = jnp.exp2((logit - top) * TO_EXP2)
            total = jnp.sum(part, axis=1, keepdims=True)
            high = part.astype(jnp.bfloat16)
            low = (part - high.astype(jnp.float32)).astype(jnp.bfloat16)
            v = jnp.concatenate([vbuf[b, 0], vbuf[b, 1]], axis=1)
            both = jnp.dot(
                jnp.concatenate([high, low], axis=0), v, preferred_element_type=jnp.float32
            )
            results.append((both[:ROWS] + both[ROWS:], top, total))
        for n, u in enumerate(units[::PAIR]):
            for head in range(HEADS):
                own = slice(head * GROUP, (head + 1) * GROUP)
                here = slice(head * HEAD, (head + 1) * HEAD)
                two = results[n * PAIR : (n + 1) * PAIR]
                top = jnp.concatenate([r[1][own] for r in two], axis=0)
                total = jnp.concatenate([r[2][own] for r in two], axis=0)
                psend[step * UNIT + u + head] = jnp.concatenate([r[0][own, here] for r in two], axis=0)
                pair = jnp.where(lane == row, top, jnp.where(lane == row + ROWS, total, 0.0))
                ssend[pl.ds(step * UNIT + u + head, 1)] = jnp.sum(pair, axis=0, keepdims=True)

    def p_remote(b):
        return pltpu.make_async_remote_copy(
            src_ref=psend.at[b], dst_ref=parts.at[me], send_sem=p_send, recv_sem=p_recv,
            device_id={"seq": b}, device_id_type=MESH,
        )

    def s_remote(b):
        return pltpu.make_async_remote_copy(
            src_ref=ssend.at[pl.ds(b, 1)], dst_ref=stats.at[pl.ds(me, 1)], send_sem=s_send, recv_sem=s_recv,
            device_id={"seq": b}, device_id_type=MESH,
        )

    def send(step, units=range(UNIT)):
        for u in units:
            b = step * UNIT + u

            @pl.when(b != me)
            def _():
                s_remote(b).start()
                p_remote(b).start()

    head, tail = range(PAIR), range(PAIR, UNIT)
    arrived(0)
    loaded(0)
    scores(0, 0, head)
    reads(0, 0, head)
    send(0, head)
    arrived(1)
    arrived(2 * nth(1))
    arrived(2 * nth(1) + 1)
    loaded(1)
    scores(0, 0, tail)
    scores(nth(1), 1)
    reads(0, 0, tail)
    send(0, tail)

    @pl.loop(0, STEPS // 2 - 1)
    def _(i):
        n = 2 * i + 1
        now, second, third = nth(n), nth(n + 1), nth(n + 2)
        for step in (second, third):
            arrived(2 * step)
            arrived(2 * step + 1)
        loaded(n + 1)
        loaded(n + 2)
        scores(second, 0)
        reads(now, 1)
        send(now)
        scores(third, 1)
        reads(second, 0)
        send(second)

    pltpu.make_async_copy(wbuf, wbuf, w_sem.at[0]).wait()
    reads(nth(STEPS - 1), 1)
    send(nth(STEPS - 1))
    parts[me] = psend[me]
    stats[pl.ds(me, 1)] = ssend[pl.ds(me, 1)]

    def all_but_one(ref, send_sem, recv_sem):
        most = ref.at[pl.ds(0, SEQ - 1)]
        return pltpu.make_async_remote_copy(
            src_ref=most, dst_ref=most, send_sem=send_sem, recv_sem=recv_sem,
            device_id={"seq": me}, device_id_type=MESH,
        )

    all_but_one(stats, s_send, s_recv).wait_recv()
    stat = stats[...]
    best = jnp.max(stat, axis=0, keepdims=True)
    scale = jnp.exp2((stat - best) * TO_EXP2)
    sums = pltpu.roll(stat, HEAD - ROWS, axis=1)
    weight = scale / jnp.sum(sums * scale, axis=0, keepdims=True)
    weight = weight.T[:ROWS]

    all_but_one(parts, p_send, p_recv).wait_recv()
    read = jnp.zeros((ROWS, HEAD), jnp.float32)
    for i in range(SEQ):
        read = read + parts[i] * weight[:, i : i + 1]
    rows[...] = read.astype(jnp.bfloat16).astype(jnp.float32)
    even = lax.broadcasted_iota(jnp.int32, (GROUP, HEAD), 0) == 0
    wide = jnp.concatenate(
        [jnp.where(even, rows[r : r + 1, :], rows[GROUP + r : GROUP + r + 1, :]) for r in range(GROUP)],
        axis=1,
    )
    spread = wide.astype(jnp.bfloat16)
    deep = GROUP * HEAD // 2
    folded = jnp.concatenate([wide[:, :deep], wide[:, deep:]], axis=0).astype(jnp.bfloat16)

    mine = grp * PAIR + core

    def y_remote(quarter, token, peer):
        return pltpu.make_async_remote_copy(
            src_ref=ysend.at[quarter, token], dst_ref=ybuf.at[mine], send_sem=y_send, recv_sem=y_recv,
            device_id={"seq": chip + token, "group": peer}, device_id_type=MESH,
        )

    def pair(quarter, start):
        w = wbuf[quarter, :, :, start : start + 512].reshape(GROUP * HEAD, 512)
        return jnp.dot(spread, w, preferred_element_type=jnp.float32)

    def single(quarter):
        w = wbuf[quarter, :, :, 1024:COLS]
        w = jnp.concatenate(
            [w[: GROUP // 2].reshape(deep, 256), w[GROUP // 2 :].reshape(deep, 256)], axis=1
        )
        both = jnp.dot(folded, w, preferred_element_type=jnp.float32)
        return both[:GROUP, :256] + both[GROUP:, 256:]

    def ship(quarter, terms):
        line = jnp.concatenate(terms, axis=1)
        for token in range(PAIR):
            for n in range(COLS // 128):
                ysend[quarter, token, n : n + 1, :] = line[token : token + 1, n * 128 : (n + 1) * 128]
        if quarter < GRP - 1:
            for token in range(PAIR):
                y_remote(quarter, token, owner_of(quarter)).start()

    ahead = pair(0, 0)
    for quarter in range(GRP):
        terms = [ahead, pair(quarter, 512), single(quarter)]
        if quarter < GRP - 1:
            ahead = pair(quarter + 1, 0)
        ship(quarter, terms)
    y_remote(GRP - 1, 1 - core, grp).start()
    ybuf[mine] = ysend[GRP - 1, core]

    def others(ref):
        most = ref.at[pl.ds(0, GRP * PAIR - 1)]
        return pltpu.make_async_remote_copy(
            src_ref=most, dst_ref=most, send_sem=y_send, recv_sem=y_recv,
            device_id={"seq": me}, device_id_type=MESH,
        )

    all_but_one(qbuf, q_send, q_recv.at[0]).wait_send()
    all_but_one(stats, s_send, s_recv).wait_send()
    all_but_one(parts, p_send, p_recv).wait_send()
    others(ybuf).wait_send()
    others(ybuf).wait_recv()
    token = ybuf[0]
    for i in range(1, GRP * PAIR):
        token = token + ybuf[i]
    for n in range(COLS // 128):
        out_ref[0:1, n * 128 : (n + 1) * 128] = token[n : n + 1, :].astype(out_ref.dtype)


def per_device(new_queries, stored_keys, stored_values, used_length, out_weight):
    hbm = pl.BlockSpec(memory_space=pl.ANY)
    dma = pltpu.SemaphoreType.DMA
    return pl.pallas_call(
        kernel,
        out_shape=pltpu.VMEM((1, COLS), jnp.bfloat16),
        in_specs=[hbm] * 5,
        out_specs=pl.BlockSpec(memory_space=pltpu.VMEM),
        scratch_shapes=[
            pltpu.VMEM((SEQ, HEADS, STRETCH, HEAD), jnp.bfloat16),
            pltpu.VMEM((SEQ, HEADS, STRETCH, HEAD), jnp.bfloat16),
            pltpu.VMEM((GRP, GROUP, HEAD, COLS), jnp.bfloat16),
            pltpu.VMEM((SEQ, HEADS, GROUP, HEAD), jnp.bfloat16),
            pltpu.SMEM((SEQ,), jnp.int32),
            pltpu.VMEM((2, UNIT, ROWS, STRETCH), jnp.float32),
            pltpu.VMEM((SEQ, ROWS, HEAD), jnp.float32),
            pltpu.VMEM((SEQ, 128), jnp.float32),
            pltpu.VMEM((SEQ, ROWS, HEAD), jnp.float32),
            pltpu.VMEM((SEQ, 128), jnp.float32),
            pltpu.VMEM((ROWS, HEAD), jnp.float32),
            pltpu.VMEM((GRP, PAIR, COLS // 128, 128), jnp.float32),
            pltpu.VMEM((GRP * PAIR, COLS // 128, 128), jnp.float32),
            dma((2,)), dma((STEPS,)), dma((1,)),
            dma(()), dma((SEQ // PAIR,)), dma(()), dma(()), dma(()), dma(()),
            dma(()), dma(()),
        ],
        compiler_params=pltpu.CompilerParams(
            collective_id=0, has_side_effects=True, vmem_limit_bytes=60 * 1024 * 1024
        ),
        name="decode",
    )(new_queries, stored_keys, stored_values, used_length, out_weight)


def solution(mesh):
    in_specs = (
        P("seq", "group", None, None),
        P(None, "group", "seq", None),
        P(None, "group", "seq", None),
        P(),
        P("group", None, None, None),
    )
    return jax.shard_map(
        per_device, mesh=mesh, in_specs=in_specs, out_specs=P("seq", "group"), check_vma=False
    )
```
